32 devices in a mesh: lon: 8 (over y, x, core), lat: 4 (over z).
Axes of the slice: x: 2, y: 2, z: 4, core: 2. Of those that a mesh axis runs over, the one named last changes fastest.
Arguments:
- normed: bfloat16 [8, 96, 192, 192], P(None, 'lat', 'lon'), may hold values from -6 to 6
- cotangent: bfloat16 [8, 96, 192, 192], P(None, 'lat', 'lon'), may hold values from -6 to 6
- weight_qkv: bfloat16 [192, 576], replicated, may hold values from -0.4375 to 0.4375
- weight_proj: bfloat16 [192, 192], replicated, may hold values from -0.4375 to 0.4375
- bias_table: bfloat16 [64, 6, 20736], P('lat'), may hold values from -6 to 390
Outputs:
- input_grad: bfloat16 [8, 96, 192, 192], P(None, 'lat', 'lon')
- qkv_grad: float32 [192, 576], replicated
- proj_grad: float32 [192, 192], replicated
- bias_grad: float32 [64, 6, 20736], P('lat')
The draws below stay inside these ranges and needn't reach their ends.
All inputs are finite; a program needn't handle non-finite values.
Results may differ from the reference program's by a relative error of at most 0.019.
Values may be sent and summed in bfloat16 or wider, within the bound.
A program may use at most 192 MiB of HBM per device.

```python
import jax
import jax.numpy as jnp
from jax import lax

C = 192
HEADS = 6
WIN_Z = 2
WIN_LAT = 6
WIN_LON = 12
WTOK = 144
NZ = 8
TYPES = 64
NLAT = 96
NLON = 192


def draw_bias_table(key, part):
    keys_list = jax.random.split(jax.random.fold_in(key, 17), 1)
    shape = (TYPES, HEADS, WTOK, WTOK)
    baseline = jnp.clip(jax.random.normal(keys_list[0], shape, jnp.float32), -6.0, 6.0)
    return baseline.reshape(TYPES, HEADS, WTOK * WTOK).astype(jnp.bfloat16)


def block_levels(stream_key, shape, shards, least, largest):
    factor_of, own = 1.0, jax.random.fold_in(stream_key, 6)
    for position, blocks in shards:
        heights = jnp.exp(jax.random.uniform(jax.random.fold_in(own, position), (blocks,), jnp.float32, least / len(shards), largest / len(shards)))
        factor_of = factor_of * jnp.repeat(heights, shape[position] // blocks).reshape([-1 if axis == position else 1 for axis in range(len(shape))])
    return factor_of


def gaussian(rng, dims, width, most, cuts=(), kind=jnp.bfloat16):
    level = block_levels(rng, dims, cuts, -0.22, 0.18) if cuts else 1.0
    entries = jax.random.normal(rng, dims, jnp.float32) * width * level
    return jnp.minimum(jnp.maximum(entries, -most), most).astype(kind)


def setup_inputs(seed: int = 0) -> dict:
    keys = jax.random.split(jax.random.key(seed), 6)
    return {
        "normed": gaussian(keys[0], (NZ, NLAT, NLON, C), 1.0, 6.0, ((1, 4), (2, 8))),
        "cotangent": gaussian(keys[1], (NZ, NLAT, NLON, C), 1.0, 6.0, ((1, 4), (2, 8))),
        "weight_qkv": gaussian(keys[2], (C, 3 * C), C ** -0.5, 0.4375),
        "weight_proj": gaussian(keys[3], (C, C), C ** -0.5, 0.4375),
        "bias_table": draw_bias_table(jax.random.fold_in(keys[5], 71), 0),
    }


def window_split(grid_field):
    levels, height, breadth = grid_field.shape[:3]
    trailing_dims = grid_field.shape[3:]
    shaped = grid_field.reshape((levels // WIN_Z, WIN_Z, height // WIN_LAT, WIN_LAT, breadth // WIN_LON, WIN_LON) + trailing_dims)
    axes_order = (0, 2, 4, 1, 3, 5) + tuple(range(6, 6 + len(trailing_dims)))
    return shaped.transpose(axes_order).reshape((-1, WTOK) + trailing_dims)


def window_merge(windowed, levels, height, breadth):
    channels = windowed.shape[-1]
    shaped = windowed.reshape(levels // WIN_Z, height // WIN_LAT, breadth // WIN_LON, WIN_Z, WIN_LAT, WIN_LON, channels)
    return shaped.transpose(0, 3, 1, 4, 2, 5, 6).reshape(levels, height, breadth, channels)


def window_backward(block_in, block_cot, block_region, block_live, block_types, bias_rows, weight_qkv, weight_proj):
    windows = block_in.shape[0]
    channels = block_in.shape[2]
    head_dim = channels // HEADS
    softmax_scale = head_dim ** -0.5
    high = lax.Precision.HIGHEST
    f32 = jnp.float32
    projected = jnp.einsum('bnc,cf->bnf', block_in.astype(f32), weight_qkv.astype(f32), precision=high).astype(jnp.bfloat16)
    projected = projected.reshape(windows, WTOK, 3, HEADS, head_dim)
    queries = projected[:, :, 0]
    key_rows = projected[:, :, 1]
    values = projected[:, :, 2]
    bias_add = jnp.dot(block_types, bias_rows.astype(f32), precision=high).reshape(windows, HEADS, WTOK, WTOK)
    scores = jnp.einsum('bqhd,bkhd->bhqk', queries.astype(f32), key_rows.astype(f32), precision=high) * softmax_scale + bias_add
    allowed = (block_region[:, :, None] == block_region[:, None, :]) & (block_live[:, :, None] == block_live[:, None, :])
    allowed = allowed[:, None]
    peak_score = jnp.max(jnp.where(allowed, scores, -1e30), axis=-1, keepdims=True)
    exp_terms = jnp.where(allowed, jnp.exp(scores - peak_score), 0.0)
    attn_probs = exp_terms / jnp.sum(exp_terms, axis=-1, keepdims=True)
    probs_b = attn_probs.astype(jnp.bfloat16)
    mixed = jnp.einsum('bhqk,bkhd->bqhd', probs_b.astype(f32), values.astype(f32), precision=high).astype(jnp.bfloat16)
    mixed = mixed.reshape(windows, WTOK, channels)
    grad_proj = jnp.einsum('bnc,bnf->cf', mixed.astype(f32), block_cot.astype(f32), precision=high)
    mixed_grad = jnp.einsum('bnf,cf->bnc', block_cot.astype(f32), weight_proj.astype(f32), precision=high).astype(jnp.bfloat16)
    mixed_grad = mixed_grad.reshape(windows, WTOK, HEADS, head_dim)
    prob_grad = jnp.einsum('bqhd,bkhd->bhqk', mixed_grad.astype(f32), values.astype(f32), precision=high)
    row_delta = jnp.sum(attn_probs * prob_grad, axis=-1, keepdims=True)
    score_grad = attn_probs * (prob_grad - row_delta)
    grad_bias = jnp.dot(block_types.T, score_grad.reshape(windows, -1), precision=high)
    score_grad_b = score_grad.astype(jnp.bfloat16).astype(f32)
    query_grad = (jnp.einsum('bhqk,bkhd->bqhd', score_grad_b, key_rows.astype(f32), precision=high) * softmax_scale).astype(jnp.bfloat16)
    key_grad = (jnp.einsum('bhqk,bqhd->bkhd', score_grad_b, queries.astype(f32), precision=high) * softmax_scale).astype(jnp.bfloat16)
    value_grad = jnp.einsum('bhqk,bqhd->bkhd', probs_b.astype(f32), mixed_grad.astype(f32), precision=high).astype(jnp.bfloat16)
    cols_grad = jnp.stack([query_grad, key_grad, value_grad], axis=2).reshape(windows, WTOK, 3 * channels)
    grad_qkv = jnp.einsum('bnc,bnf->cf', block_in.astype(f32), cols_grad.astype(f32), precision=high)
    grad_in = jnp.einsum('bnf,cf->bnc', cols_grad.astype(f32), weight_qkv.astype(f32), precision=high).astype(jnp.bfloat16)
    return grad_in, grad_qkv, grad_proj, grad_bias


def reference(normed, cotangent, weight_qkv, weight_proj, bias_table):
    levels, height, breadth, channels = normed.shape
    level_shift = WIN_Z // 2
    lat_shift = WIN_LAT // 2
    lon_shift = WIN_LON // 2

    def to_frame(grid_field):
        rolled = jnp.roll(jnp.roll(grid_field, -lon_shift, axis=2), -level_shift, axis=0)
        padding = jnp.zeros((levels, lat_shift, breadth, channels), grid_field.dtype)
        return jnp.concatenate([rolled[:, lat_shift:], padding], axis=1)

    framed_in = window_split(to_frame(normed))
    framed_cot = window_split(to_frame(cotangent))
    level_index = jnp.arange(levels, dtype=jnp.int32)
    wrapped_levels = (level_index >= levels - level_shift).astype(jnp.int32)
    wrapped_field = jnp.broadcast_to(wrapped_levels[:, None, None], (levels, height, breadth))
    region_win = window_split(wrapped_field)
    row_index = jnp.arange(height, dtype=jnp.int32)
    live_rows = row_index < height - lat_shift
    live_field = jnp.broadcast_to(live_rows[None, :, None], (levels, height, breadth))
    live_win = window_split(live_field)
    level_windows = levels // WIN_Z
    lat_windows = height // WIN_LAT
    lon_windows = breadth // WIN_LON
    level_part = jnp.arange(level_windows, dtype=jnp.int32)[:, None, None]
    lat_part = jnp.arange(lat_windows, dtype=jnp.int32)[None, :, None]
    kinds = jnp.broadcast_to(lat_part * level_windows + level_part, (level_windows, lat_windows, lon_windows))
    onehot = (kinds.reshape(-1)[:, None] == jnp.arange(TYPES, dtype=jnp.int32)[None, :]).astype(jnp.float32)
    bias_rows = bias_table.reshape(TYPES, -1)
    window_total = framed_in.shape[0]
    block_size = max(divisor for divisor in range(1, 65) if window_total % divisor == 0)
    blocks = window_total // block_size

    def regroup(array):
        return array.reshape((blocks, block_size) + array.shape[1:])

    def step_block(totals, pieces):
        grad_in, grad_qkv, grad_proj, grad_bias = window_backward(pieces[0], pieces[1], pieces[2], pieces[3], pieces[4], bias_rows, weight_qkv, weight_proj)
        return (totals[0] + grad_qkv, totals[1] + grad_proj, totals[2] + grad_bias), grad_in

    start = (jnp.zeros((channels, 3 * channels), jnp.float32), jnp.zeros((channels, channels), jnp.float32), jnp.zeros((TYPES, HEADS * WTOK * WTOK), jnp.float32))
    totals, grads = lax.scan(step_block, start, (regroup(framed_in), regroup(framed_cot), regroup(region_win), regroup(live_win), regroup(onehot)))
    framed_grad = window_merge(grads.reshape(window_total, WTOK, channels), levels, height, breadth)
    zeros_rows = jnp.zeros((levels, lat_shift, breadth, channels), jnp.bfloat16)
    unshifted = jnp.concatenate([zeros_rows, framed_grad[:, :height - lat_shift]], axis=1)
    input_grad = jnp.roll(jnp.roll(unshifted, lon_shift, axis=2), level_shift, axis=0)
    return input_grad, totals[0], totals[1], totals[2].reshape(TYPES, HEADS, WTOK * WTOK)
```

```python
import functools
import math

import jax
import jax.numpy as jnp
from jax import lax
from jax.experimental import pallas as pl
from jax.experimental.pallas import tpu as pltpu
from jax.sharding import PartitionSpec as P

HEADS = 6
WIN_Z = 2
WIN_LAT = 6
WIN_LON = 12
WTOK = 144
LANES = 128
TAIL = WTOK - LANES
HALO = 8
PACKED = 1024
UNROLL = 6
LOG2E = math.log2(math.e)
F32 = jnp.float32
BF16 = jnp.bfloat16


def ring_permute(block, axis, distance):
    size = lax.axis_size(axis)
    return lax.ppermute(block, axis, [((i - distance) % size, i) for i in range(size)])


def line_permute(block, axis, distance):
    size = lax.axis_size(axis)
    route = [(i - distance, i) for i in range(size) if 0 <= i - distance < size]
    return lax.ppermute(block, axis, route)


def mm(a, b, ca=1, cb=0):
    return lax.dot_general(a, b, (((ca,), (cb,)), ((), ())), preferred_element_type=F32)


class Exchange:
    def __init__(self, n, kinds, bufs, sems):
        self.n, self.kinds = n, kinds
        self.chips = n // 2
        self.gb, self.pair, self.sum, self.cross, self.out, self.hbm = bufs
        self.pair_sem, self.cross_sem, self.back_sem, self.fwd_sem, self.store_sem = sems
        me = lax.axis_index("lon")
        self.me = me
        self.core = lax.rem(me, 2)
        self.chip = me // 2
        self.other = 1 - self.core
        self.partner = self.chip * 2 + self.other
        self.half = PACKED // 2
        self.part = self.half // self.chips

    def remote(self, src, dst, send, recv, device):
        return pltpu.make_async_remote_copy(
            src_ref=src, dst_ref=dst, send_sem=send, recv_sem=recv,
            device_id={"lon": device}, device_id_type=pl.DeviceIdType.MESH,
        )

    def peer(self, o):
        return lax.rem(self.chip + o, self.chips)

    def rows(self, core, chip):
        return pl.ds(core * self.half + chip * self.part, self.part)

    def pair_copy(self, t):
        src = self.gb.at[t, pl.ds(self.other * self.half, self.half)]
        return self.remote(
            src, self.pair.at[t], self.pair_sem.at[0, t], self.pair_sem.at[1, t], self.partner
        )

    def cross_copy(self, t, o, arriving):
        j = self.peer(o)
        src = self.sum.at[t, pl.ds(j * self.part, self.part)]
        slot = j if arriving else self.chip
        return self.remote(
            src, self.cross.at[t, slot], self.cross_sem.at[0, t, j],
            self.cross_sem.at[1, t, slot], j * 2 + self.core,
        )

    def back_copy(self, t, o, arriving):
        j = self.peer(o)
        slot = j if arriving else self.chip
        part = self.out.at[t, self.rows(self.core, slot)]
        return self.remote(
            part, part, self.back_sem.at[0, t, j], self.back_sem.at[1, t, slot],
            j * 2 + self.core,
        )

    def fwd_copy(self, t, j, arriving):
        part = self.out.at[t, self.rows(self.other if arriving else self.core, j)]
        return self.remote(
            part, part, self.fwd_sem.at[0, t, j], self.fwd_sem.at[1, t, j], self.partner
        )

    def store(self, t):
        return pltpu.make_async_copy(self.out.at[t], self.hbm.at[t], self.store_sem.at[t])

    def stage_pair(self, t):
        self.pair_copy(t).wait_recv()
        mine = self.gb[t, pl.ds(self.core * self.half, self.half)].astype(F32)
        total = (mine + self.pair[t].astype(F32)).astype(BF16)
        self.sum[t] = total
        for o in range(1, self.chips):
            self.cross_copy(t, o, False).start()

    def stage_cross(self, t):
        for o in range(1, self.chips):
            self.cross_copy(t, o, True).wait_recv()
        acc = self.sum[t, pl.ds(self.chip * self.part, self.part)].astype(F32)
        for o in range(1, self.chips):
            acc = acc + self.cross[t, self.peer(o)].astype(F32)
        self.out[t, self.rows(self.core, self.chip)] = acc.astype(BF16)
        for o in range(1, self.chips):
            self.back_copy(t, o, False).start()
        self.fwd_copy(t, self.chip, False).start()

    def stage_back(self, t):
        for o in range(1, self.chips):
            self.back_copy(t, o, True).wait_recv()
            self.fwd_copy(t, self.peer(o), False).start()

    def stage_fwd(self, t):
        for j in range(self.chips):
            self.fwd_copy(t, j, True).wait_recv()
        self.store(t).start()

    def stages(self):
        return [self.stage_pair, self.stage_cross, self.stage_back, self.stage_fwd]

    def behind(self, step):
        for d, stage in enumerate(self.stages()):
            t = step - 1 - d
            if isinstance(t, int):
                if 0 <= t < self.kinds:
                    stage(t)
            else:
                pl.when(t >= 0)(functools.partial(stage, t))

    def drain(self):
        def body(t, _):
            self.pair_copy(t).wait_send()
            for o in range(1, self.chips):
                self.cross_copy(t, o, False).wait_send()
                self.back_copy(t, o, False).wait_send()
            for j in range(self.chips):
                self.fwd_copy(t, j, False).wait_send()
            self.store(t).wait()
            return 0

        lax.fori_loop(0, self.kinds, body, 0)


def enter(n, lats):
    me, lat = lax.axis_index("lon"), lax.axis_index("lat")
    barrier = pltpu.get_barrier_semaphore()
    for o in range(1, n):
        pl.semaphore_signal(
            barrier, inc=1, device_id={"lon": lax.rem(me + o, n)},
            device_id_type=pl.DeviceIdType.MESH,
        )
    for o in range(1, lats):
        pl.semaphore_signal(
            barrier, inc=1, device_id={"lat": lax.rem(lat + o, lats)},
            device_id_type=pl.DeviceIdType.MESH,
        )
    pl.semaphore_wait(barrier, n + lats - 2)


class WeightSum:
    def __init__(self, n, lats, wg, w1, w2, wout, sems):
        self.n, self.lats = n, lats
        self.wg, self.w1, self.w2, self.wout = wg, w1, w2, wout
        self.s1, self.s2, self.s3 = sems
        self.me, self.lat = lax.axis_index("lon"), lax.axis_index("lat")

    def remote(self, src, dst, sems, out_at, in_at, device):
        return pltpu.make_async_remote_copy(
            src_ref=src, dst_ref=dst, send_sem=sems.at[0, out_at], recv_sem=sems.at[1, in_at],
            device_id=device, device_id_type=pl.DeviceIdType.MESH,
        )

    def first(self, o, arriving):
        p = lax.rem(self.me + o, self.n)
        slot = p if arriving else self.me
        return self.remote(self.wg.at[p], self.w1.at[slot], self.s1, p, slot, {"lon": p})

    def second(self, o, arriving):
        p = lax.rem(self.lat + o, self.lats)
        slot = p if arriving else self.lat
        return self.remote(self.w2.at[slot], self.w2.at[slot], self.s2, p, slot, {"lat": p})

    def third(self, o, arriving):
        p = lax.rem(self.me + o, self.n)
        slot = p if arriving else self.me
        return self.remote(self.wout.at[slot], self.wout.at[slot], self.s3, p, slot, {"lon": p})

    def start(self):
        for o in range(1, self.n):
            self.first(o, False).start()
        self.w1[pl.ds(self.me, 1)] = self.wg[pl.ds(self.me, 1)]

    def step_one(self):
        for o in range(1, self.n):
            self.first(o, True).wait_recv()
        total = jnp.sum(self.w1[...].astype(F32), axis=0, keepdims=True)
        self.w2[pl.ds(self.lat, 1)] = total.astype(BF16)
        for o in range(1, self.lats):
            self.second(o, False).start()

    def step_two(self):
        for o in range(1, self.lats):
            self.second(o, True).wait_recv()
        total = jnp.sum(self.w2[...].astype(F32), axis=0, keepdims=True)
        self.wout[pl.ds(self.me, 1)] = total.astype(BF16)
        for o in range(1, self.n):
            self.third(o, False).start()

    def finish(self):
        for o in range(1, self.n):
            self.third(o, True).wait_recv()
        for o in range(1, self.n):
            self.first(o, False).wait_send()
            self.third(o, False).wait_send()
        for o in range(1, self.lats):
            self.second(o, False).wait_send()


def kernel(
    n,
    lats,
    kinds,
    lat_windows,
    level_windows,
    lon_windows,
    last_ref,
    perm_ref,
    xa_ref,
    xb_ref,
    ca_ref,
    cb_ref,
    wqkv_ref,
    wproj_ref,
    bias_ref,
    gframe_ref,
    wout_ref,
    gbias_hbm,
    qm_s,
    mm_s,
    p_s,
    ds_s,
    gqkv_ref,
    gproj_ref,
    gbias_ref,
    pair_s,
    sum_s,
    cross_s,
    red_s,
    wg_s,
    w1_s,
    w2_s,
    w3_s,
    pair_sem,
    cross_sem,
    back_sem,
    fwd_sem,
    store_sem,
    w1_sem,
    w2_sem,
    w3_sem,
):
    step = pl.program_id(0)
    a = lax.rem(step, level_windows)
    b = step // level_windows
    channels = wqkv_ref.shape[0]
    head_dim = channels // HEADS
    scale = head_dim ** -0.5
    half = WIN_LAT * xa_ref.shape[2]

    @pl.when(step == 0)
    def _():
        gqkv_ref[...] = jnp.zeros_like(gqkv_ref)
        gproj_ref[...] = jnp.zeros_like(gproj_ref)
        gbias_ref[:, HEADS * WTOK :, :] = jnp.zeros((kinds, PACKED - HEADS * WTOK, LANES), BF16)
        enter(n, lats)

    ex = Exchange(
        n, kinds,
        (gbias_ref, pair_s, sum_s, cross_s, red_s, gbias_hbm),
        (pair_sem, cross_sem, back_sem, fwd_sem, store_sem),
    )
    ex.behind(step)

    perm = perm_ref[...]
    x_raw = jnp.concatenate(
        [xa_ref[...].reshape(half, channels), xb_ref[...].reshape(half, channels)], axis=0
    )
    c_raw = jnp.concatenate(
        [ca_ref[...].reshape(half, channels), cb_ref[...].reshape(half, channels)], axis=0
    )
    x = mm(perm, x_raw).astype(BF16)
    c = mm(perm, c_raw).astype(BF16)
    proj = mm(x, wqkv_ref[...]).astype(BF16)
    mgrad = mm(c, wproj_ref[...], 1, 1).astype(BF16)

    wrap_here = a == level_windows - 1
    dead_here = (b == lat_windows - 1) & (last_ref[0] == 1)
    per_level = WTOK // WIN_Z

    def classes(shape, dim):
        token = lax.broadcasted_iota(jnp.int32, shape, dim)
        upper = token >= per_level
        inner = jnp.where(upper, token - per_level, token)
        wrapped = jnp.where(upper & wrap_here, 2, 0)
        dead = jnp.where((inner >= per_level // 2) & dead_here, 1, 0)
        return wrapped + dead

    same = classes((WTOK, WTOK), 0) == classes((WTOK, WTOK), 1)
    mask_add = jnp.where(same, 0.0, -1e30)
    lane_head = lax.broadcasted_iota(jnp.int32, (1, channels), 1) // head_dim
    zero = jnp.zeros((), BF16)

    parts = []
    for w in range(lon_windows):
        rows = slice(w * WTOK, (w + 1) * WTOK)
        parts.append(
            (
                proj[rows, :channels],
                proj[rows, channels : 2 * channels],
                proj[rows, 2 * channels :],
                mgrad[rows],
            )
        )
    mixed = [jnp.zeros((WTOK, channels), F32) for _ in range(lon_windows)]
    dq = [jnp.zeros((WTOK, channels), F32) for _ in range(lon_windows)]
    for h in range(HEADS):
        hot = (lane_head == h).astype(BF16)
        hrows = slice(h * WTOK, (h + 1) * WTOK)
        shift = bias_ref[0, hrows, :].astype(F32) * LOG2E + mask_add
        gb = None
        for w in range(lon_windows):
            q, k, v, m = parts[w]
            qm = q * hot
            mg = m * hot
            qm_s[w, hrows, :] = qm
            mm_s[w, hrows, :] = mg
            s = mm(qm, k, 1, 1) * (scale * LOG2E) + shift
            dp = mm(mg, v, 1, 1)
            e = jnp.exp2(s - jnp.max(s, axis=1, keepdims=True))
            p = e * (1.0 / jnp.sum(e, axis=1, keepdims=True))
            delta = jnp.sum(p * dp, axis=1, keepdims=True)
            ds = p * (dp - delta)
            pb = p.astype(BF16)
            dsb = ds.astype(BF16)
            p_s[w, hrows, :] = pb
            ds_s[w, hrows, :] = dsb
            gb = ds if gb is None else gb + ds
            mixed[w] = mixed[w] + mm(pb, v * hot)
            dq[w] = dq[w] + mm(dsb, k * hot)
        gb = gb.astype(BF16)
        gbias_ref[step, hrows, :] = gb[:, :LANES]
        gbias_ref[step, HEADS * WTOK : HEADS * WTOK + WTOK, h * TAIL : (h + 1) * TAIL] = gb[:, LANES:]
    cols = []
    for w in range(lon_windows):
        dk = mm(ds_s[w], qm_s[w], 0, 0) * scale
        dv = mm(p_s[w], mm_s[w], 0, 0)
        cols.append(
            jnp.concatenate(
                [(dq[w] * scale).astype(BF16), dk.astype(BF16), dv.astype(BF16)], axis=1
            )
        )
    cols = jnp.concatenate(cols, axis=0)
    mixed_b = jnp.concatenate([t.astype(BF16) for t in mixed], axis=0)
    gproj_ref[...] += mm(mixed_b, c, 0, 0)
    gqkv_ref[...] += mm(x, cols, 0, 0)
    gin = mm(cols, wqkv_ref[...], 1, 1).astype(BF16)
    gout = mm(perm, gin, 0, 0).astype(BF16)
    gframe_ref[...] = gout.reshape(gframe_ref.shape)
    ex.pair_copy(step).start()

    @pl.when(step == kinds - 1)
    def _():
        share = channels // n
        for i in range(n):
            rows = slice(i * share, (i + 1) * share)
            wg_s[i, :, : 3 * channels] = gqkv_ref[rows].astype(BF16)
            wg_s[i, :, 3 * channels :] = gproj_ref[rows].astype(BF16)
        ws = WeightSum(n, lats, wg_s, w1_s, w2_s, w3_s, (w1_sem, w2_sem, w3_sem))
        ws.start()
        ex.behind(kinds)
        ws.step_one()
        ex.behind(kinds + 1)
        ws.step_two()
        ex.behind(kinds + 2)
        ex.behind(kinds + 3)
        ws.finish()
        wout_ref[...] = w3_s[...]
        ex.drain()


def unpack_kernel(packed_ref, out_ref, main_s, tail_s):
    stack = HEADS * WTOK
    main_s[...] = packed_ref[0, :stack].astype(F32)
    tails = packed_ref[0, stack : stack + WTOK].astype(F32)
    for h in range(HEADS):
        turned = tails if h == 0 else pltpu.roll(tails, LANES - h * TAIL, 1)
        tail_s[h * WTOK : (h + 1) * WTOK] = turned
    group = LANES // TAIL
    lane = lax.broadcasted_iota(jnp.int32, (HEADS, LANES), 1)

    def body(m, _):
        before_main = before_tail = None
        for r in range(group + 1):
            tile = None
            if r < group:
                at = pl.ds(m * group + r, HEADS, stride=WTOK)
                here_main, here_tail = main_s[at, :], tail_s[at, :]
                if r:
                    here_main = pltpu.roll(here_main, TAIL * r, 1)
                    here_tail = pltpu.roll(here_tail, TAIL * r, 1)
                tile = here_main
            if r:
                ended = before_tail
                if r > 1:
                    ended = jnp.where(lane < TAIL * (r - 1), before_main, before_tail)
                tile = ended if r == group else jnp.where(lane < TAIL * r, ended, tile)
            start = pl.multiple_of(m * (group * WTOK) + r * LANES, LANES)
            out_ref[0, :, pl.ds(start, LANES)] = tile
            if r < group:
                before_main, before_tail = here_main, here_tail
        return 0

    def several(i, _):
        for u in range(UNROLL):
            body(i * UNROLL + u, 0)
        return 0

    lax.fori_loop(0, WTOK // group // UNROLL, several, 0)


def unpack(packed):
    kinds, rows, lanes = packed.shape
    stack = HEADS * WTOK
    return pl.pallas_call(
        unpack_kernel,
        grid=(kinds,),
        in_specs=[pl.BlockSpec((1, rows, lanes), lambda i: (i, 0, 0))],
        out_specs=pl.BlockSpec((1, HEADS, WTOK * WTOK), lambda i: (i, 0, 0)),
        out_shape=jax.ShapeDtypeStruct((kinds, HEADS, WTOK * WTOK), F32),
        scratch_shapes=[pltpu.VMEM((stack, LANES), F32), pltpu.VMEM((stack, LANES), F32)],
        cost_estimate=pl.CostEstimate(
            flops=10_000_000_000, bytes_accessed=15_000_000, transcendentals=0
        ),
    )(packed)


def window_call(last, perm, frame_in, frame_cot, weight_qkv, weight_proj, bias):
    levels, height, wide, channels = frame_in.shape
    level_windows = levels // WIN_Z
    lat_windows = height // WIN_LAT
    lon_windows = perm.shape[0] // WTOK
    kinds = lat_windows * level_windows
    n, lats = lax.axis_size("lon"), lax.axis_size("lat")
    chips = n // 2

    def at(step, up):
        z = lax.rem(WIN_Z * lax.rem(step, level_windows) + up, levels)
        return z, step // level_windows, 0, 0

    tok = (1, WIN_LAT, wide, channels)
    low = pl.BlockSpec(tok, lambda i: at(i, 1))
    high = pl.BlockSpec(tok, lambda i: at(i, 2))
    whole = lambda arr: pl.BlockSpec(arr.shape, lambda i: (0,) * arr.ndim)
    const = lambda shape: pl.BlockSpec(shape, lambda i: (0,) * len(shape))
    stack = HEADS * WTOK
    share = channels // n
    sem = lambda *k: pltpu.SemaphoreType.DMA((2,) + k)
    return pl.pallas_call(
        functools.partial(kernel, n, lats, kinds, lat_windows, level_windows, lon_windows),
        grid=(kinds,),
        in_specs=[
            pl.BlockSpec(memory_space=pltpu.SMEM),
            whole(perm),
            low,
            high,
            low,
            high,
            whole(weight_qkv),
            whole(weight_proj),
            pl.BlockSpec((1, stack, WTOK), lambda i: (i, 0, 0)),
        ],
        out_specs=[
            pl.BlockSpec(
                (WIN_Z, WIN_LAT, wide, channels),
                lambda i: (lax.rem(i, level_windows), i // level_windows, 0, 0),
            ),
            const((n, share, 4 * channels)),
            pl.BlockSpec(memory_space=pl.ANY),
        ],
        out_shape=[
            jax.ShapeDtypeStruct((levels, height, wide, channels), BF16),
            jax.ShapeDtypeStruct((n, share, 4 * channels), BF16),
            jax.ShapeDtypeStruct((kinds, PACKED, LANES), BF16),
        ],
        scratch_shapes=[
            pltpu.VMEM((lon_windows, stack, channels), BF16),
            pltpu.VMEM((lon_windows, stack, channels), BF16),
            pltpu.VMEM((lon_windows, stack, WTOK), BF16),
            pltpu.VMEM((lon_windows, stack, WTOK), BF16),
            pltpu.VMEM((channels, 3 * channels), F32),
            pltpu.VMEM((channels, channels), F32),
            pltpu.VMEM((kinds, PACKED, LANES), BF16),
            pltpu.VMEM((kinds, PACKED // 2, LANES), BF16),
            pltpu.VMEM((kinds, PACKED // 2, LANES), BF16),
            pltpu.VMEM((kinds, chips, PACKED // n, LANES), BF16),
            pltpu.VMEM((kinds, PACKED, LANES), BF16),
            pltpu.VMEM((n, share, 4 * channels), BF16),
            pltpu.VMEM((n, share, 4 * channels), BF16),
            pltpu.VMEM((lats, share, 4 * channels), BF16),
            pltpu.VMEM((n, share, 4 * channels), BF16),
            sem(kinds),
            sem(kinds, chips),
            sem(kinds, chips),
            sem(kinds, chips),
            pltpu.SemaphoreType.DMA((kinds,)),
            sem(n),
            sem(lats),
            sem(n),
        ],
        compiler_params=pltpu.CompilerParams(
            dimension_semantics=("arbitrary",),
            vmem_limit_bytes=56 * 2**20,
            collective_id=0,
            has_side_effects=True,
        ),
        cost_estimate=pl.CostEstimate(
            flops=kinds * 1_500_000_000, bytes_accessed=kinds * 2_000_000, transcendentals=0
        ),
    )(
        last, perm, frame_in, frame_in, frame_cot, frame_cot, weight_qkv, weight_proj, bias
    )


def local(normed, cotangent, weight_qkv, weight_proj, bias_table):
    levels, height, breadth, channels = normed.shape
    lat_shift = WIN_LAT // 2
    lon_shift = WIN_LON // 2
    lon_windows = breadth // WIN_LON
    wide = breadth + HALO
    across = ring_permute((normed[:, :, :HALO], cotangent[:, :, :HALO]), "lon", -1)
    wide_in = jnp.concatenate([normed, across[0]], axis=2)
    wide_cot = jnp.concatenate([cotangent, across[1]], axis=2)
    upward = line_permute((wide_in[:, :lat_shift], wide_cot[:, :lat_shift]), "lat", -1)
    frame_in = jnp.concatenate([wide_in[:, lat_shift:], upward[0]], axis=1)
    frame_cot = jnp.concatenate([wide_cot[:, lat_shift:], upward[1]], axis=1)
    last = (lax.axis_index("lat") == lax.axis_size("lat") - 1).astype(jnp.int32).reshape(1)
    bias = bias_table.reshape(bias_table.shape[0], HEADS * WTOK, WTOK)

    rows = jnp.arange(lon_windows * WTOK, dtype=jnp.int32)
    token = rows % WTOK
    per_level = WIN_LAT * WIN_LON
    source = (
        token // per_level * (WIN_LAT * wide)
        + token % per_level // WIN_LON * wide
        + rows // WTOK * WIN_LON
        + token % WIN_LON
        + lon_shift
    )
    columns = jnp.arange(WIN_Z * WIN_LAT * wide, dtype=jnp.int32)
    perm = (source[:, None] == columns[None, :]).astype(BF16)

    gframe, weights, packed = window_call(
        last, perm, frame_in, frame_cot, weight_qkv, weight_proj, bias
    )
    weights = weights.reshape(channels, 4 * channels).astype(F32)

    gwide = jnp.roll(gframe, WIN_Z // 2, axis=0)
    side = ring_permute(gwide[:, :, breadth:], "lon", 1)
    seam = jnp.concatenate(
        [gwide[:, :, :HALO] + side, gwide[:, :, HALO:breadth]], axis=2
    )
    down = line_permute(seam[:, height - lat_shift :], "lat", 1)
    input_grad = jnp.concatenate([down, seam[:, : height - lat_shift]], axis=1)

    bias_grad = unpack(packed)
    return input_grad, weights[:, : 3 * channels], weights[:, 3 * channels :], bias_grad


def solution(mesh):
    in_specs = (
        P(None, "lat", "lon", None),
        P(None, "lat", "lon", None),
        P(),
        P(),
        P("lat", None, None),
    )
    out_specs = (P(None, "lat", "lon", None), P(), P(), P("lat", None, None))
    return jax.shard_map(local, mesh=mesh, in_specs=in_specs, out_specs=out_specs, check_vma=False)
```

```python
import functools
import math

import jax
import jax.numpy as jnp
from jax import lax
from jax.experimental import pallas as pl
from jax.experimental.pallas import tpu as pltpu
from jax.sharding import PartitionSpec as P

HEADS = 6
WIN_Z = 2
WIN_LAT = 6
WIN_LON = 12
WTOK = 144
LANES = 128
TAIL = WTOK - LANES
HALO = 8
PACKED = 1024
LAGS = (1, 3, 5, 6)
GRAD_LAG = 2
UNROLL = 6
LOG2E = math.log2(math.e)
F32 = jnp.float32
BF16 = jnp.bfloat16


def mm(a, b, ca=1, cb=0):
    return lax.dot_general(a, b, (((ca,), (cb,)), ((), ())), preferred_element_type=F32)


class Exchange:
    def __init__(self, n, kinds, bufs, sems):
        self.n, self.kinds = n, kinds
        self.chips = n // 2
        self.gb, self.pair, self.sum, self.cross, self.out, self.hbm = bufs
        self.pair_sem, self.cross_sem, self.back_sem, self.fwd_sem, self.store_sem = sems
        me = lax.axis_index("lon")
        self.me = me
        self.core = lax.rem(me, 2)
        self.chip = me // 2
        self.other = 1 - self.core
        self.partner = self.chip * 2 + self.other
        self.half = PACKED // 2
        self.part = self.half // self.chips

    def remote(self, src, dst, send, recv, device):
        return pltpu.make_async_remote_copy(
            src_ref=src, dst_ref=dst, send_sem=send, recv_sem=recv,
            device_id={"lon": device}, device_id_type=pl.DeviceIdType.MESH,
        )

    def peer(self, o):
        return lax.rem(self.chip + o, self.chips)

    def rows(self, core, chip):
        return pl.ds(core * self.half + chip * self.part, self.part)

    def pair_copy(self, t):
        src = self.gb.at[t, pl.ds(self.other * self.half, self.half)]
        return self.remote(
            src, self.pair.at[t], self.pair_sem.at[0, t], self.pair_sem.at[1, t], self.partner
        )

    def cross_copy(self, t, o, arriving):
        j = self.peer(o)
        src = self.sum.at[t, pl.ds(j * self.part, self.part)]
        slot = j if arriving else self.chip
        return self.remote(
            src, self.cross.at[t, slot], self.cross_sem.at[0, t, j],
            self.cross_sem.at[1, t, slot], j * 2 + self.core,
        )

    def back_copy(self, t, o, arriving):
        j = self.peer(o)
        slot = j if arriving else self.chip
        part = self.out.at[t, self.rows(self.core, slot)]
        return self.remote(
            part, part, self.back_sem.at[0, t, j], self.back_sem.at[1, t, slot],
            j * 2 + self.core,
        )

    def fwd_copy(self, t, j, arriving):
        part = self.out.at[t, self.rows(self.other if arriving else self.core, j)]
        return self.remote(
            part, part, self.fwd_sem.at[0, t, j], self.fwd_sem.at[1, t, j], self.partner
        )

    def store(self, t):
        return pltpu.make_async_copy(self.out.at[t], self.hbm.at[t], self.store_sem.at[t])

    def stage_pair(self, t):
        self.pair_copy(t).wait_recv()
        mine = self.gb[t, pl.ds(self.core * self.half, self.half)].astype(F32)
        total = (mine + self.pair[t].astype(F32)).astype(BF16)
        self.sum[t] = total
        for o in range(1, self.chips):
            self.cross_copy(t, o, False).start()

    def stage_cross(self, t):
        for o in range(1, self.chips):
            self.cross_copy(t, o, True).wait_recv()
        acc = self.sum[t, pl.ds(self.chip * self.part, self.part)].astype(F32)
        for o in range(1, self.chips):
            acc = acc + self.cross[t, self.peer(o)].astype(F32)
        self.out[t, self.rows(self.core, self.chip)] = acc.astype(BF16)
        for o in range(1, self.chips):
            self.back_copy(t, o, False).start()
        self.fwd_copy(t, self.chip, False).start()

    def stage_back(self, t):
        for o in range(1, self.chips):
            self.back_copy(t, o, True).wait_recv()
            self.fwd_copy(t, self.peer(o), False).start()

    def stage_fwd(self, t):
        for j in range(self.chips):
            self.fwd_copy(t, j, True).wait_recv()
        self.store(t).start()

    def stages(self):
        return [self.stage_pair, self.stage_cross, self.stage_back, self.stage_fwd]

    def behind(self, step):
        for lag, stage in zip(LAGS, self.stages()):
            t = step - lag
            if isinstance(t, int):
                if 0 <= t < self.kinds:
                    stage(t)
            else:
                pl.when(t >= 0)(functools.partial(stage, t))

    def drain(self):
        def body(t, _):
            self.pair_copy(t).wait_send()
            for o in range(1, self.chips):
                self.cross_copy(t, o, False).wait_send()
                self.back_copy(t, o, False).wait_send()
            for j in range(self.chips):
                self.fwd_copy(t, j, False).wait_send()
            self.store(t).wait()
            return 0

        lax.fori_loop(0, self.kinds, body, 0)


class Halo:
    def __init__(self, n, lats, levels, level_windows, lat_windows, refs, sems):
        self.n, self.lats = n, lats
        self.levels, self.level_windows, self.lat_windows = levels, level_windows, lat_windows
        self.given, self.east, self.south, self.gl, self.gh, self.wh, self.nh, self.out = refs
        self.east_sem, self.south_sem, self.wh_sem, self.nh_sem, self.out_sem = sems
        self.me, self.lat = lax.axis_index("lon"), lax.axis_index("lat")
        self.shift = WIN_LAT // 2
        self.height = lat_windows * WIN_LAT

    def remote(self, src, dst, sems, at, lat, lon):
        device = {"lat": self.lat + lat, "lon": lax.rem(self.me + lon + self.n, self.n)}
        return pltpu.make_async_remote_copy(
            src_ref=src, dst_ref=dst, send_sem=sems.at[(0,) + at], recv_sem=sems.at[(1,) + at],
            device_id=device, device_id_type=pl.DeviceIdType.MESH,
        )

    def east_copy(self, i, z, piece):
        short = piece >= self.lat_windows - 1
        count = self.shift if short else WIN_LAT
        corner = piece == self.lat_windows
        src_row = 0 if corner else self.shift + piece * WIN_LAT
        dst_row = self.height - self.shift if corner else piece * WIN_LAT
        src = self.given[i].at[z, pl.ds(src_row, count), pl.ds(0, HALO), :]
        dst = self.east.at[i, z, pl.ds(dst_row, count)]
        return self.remote(src, dst, self.east_sem, (i, piece, z), -1 if corner else 0, -1)

    def south_copy(self, i, z):
        src = self.given[i].at[z, pl.ds(0, self.shift)]
        return self.remote(src, self.south.at[i, z], self.south_sem, (i, z), -1, 0)

    def send(self):
        def level(piece, y, _):
            z = lax.rem(y + 1, self.levels)
            for i in range(2):
                self.east_copy(i, z, piece).start()
            return 0

        def below(y, _):
            z = lax.rem(y + 1, self.levels)
            for i in range(2):
                self.south_copy(i, z).start()
                self.east_copy(i, z, self.lat_windows).start()
            return 0

        for piece in range(self.lat_windows):
            lax.fori_loop(0, self.levels, functools.partial(level, piece), 0)

        @pl.when(self.lat > 0)
        def _():
            lax.fori_loop(0, self.levels, below, 0)

        @pl.when(self.lat == self.lats - 1)
        def _():
            self.south[...] = jnp.zeros_like(self.south)
            shape = self.east.shape
            rows = pl.ds(self.height - self.shift, self.shift)
            self.east[:, :, rows] = jnp.zeros(shape[:2] + (self.shift,) + shape[3:], BF16)

        @pl.when(self.lat == 0)
        def _():
            self.nh[...] = jnp.zeros_like(self.nh)
            shape = self.wh.shape
            self.wh[:, : self.shift] = jnp.zeros((shape[0], self.shift) + shape[2:], BF16)

    def pair(self, a):
        return [lax.rem(WIN_Z * a + 1 + u, self.levels) for u in range(WIN_Z)]

    def arrive(self, a, b):
        last = self.lat_windows - 1
        for z in self.pair(a):
            for i in range(2):
                for piece in range(self.lat_windows):
                    @pl.when(b == piece)
                    def _(i=i, z=z, piece=piece):
                        self.east_copy(i, z, piece).wait_recv()

                @pl.when((b == last) & (self.lat < self.lats - 1))
                def _(i=i, z=z):
                    self.south_copy(i, z).wait_recv()
                    self.east_copy(i, z, self.lat_windows).wait_recv()

    def back_copy(self, z, piece):
        short = piece >= self.lat_windows - 1
        count = self.shift if short else WIN_LAT
        corner = piece == self.lat_windows
        src_row = self.height - self.shift if corner else piece * WIN_LAT
        dst_row = 0 if corner else self.shift + piece * WIN_LAT
        return self.remote(
            self.gh.at[z, pl.ds(src_row, count)], self.wh.at[z, pl.ds(dst_row, count)],
            self.wh_sem, (piece, z), 1 if corner else 0, 1,
        )

    def down_copy(self, z):
        src = self.gl.at[z, pl.ds(self.height, self.shift)]
        return self.remote(src, self.nh.at[z], self.nh_sem, (z,), 1, 0)

    def give(self, a, b):
        last = self.lat_windows - 1
        for z in self.pair(a):
            for piece in range(self.lat_windows):
                @pl.when(b == piece)
                def _(z=z, piece=piece):
                    self.back_copy(z, piece).start()

            @pl.when((b == last) & (self.lat < self.lats - 1))
            def _(z=z):
                self.back_copy(z, self.lat_windows).start()
                self.down_copy(z).start()

    def store(self, z, piece):
        short = piece >= self.lat_windows - 1
        count = self.shift if short else WIN_LAT
        if piece == self.lat_windows:
            return pltpu.make_async_copy(
                self.nh.at[z], self.out.at[z, pl.ds(0, count)], self.out_sem.at[piece, z]
            )
        rows = pl.ds(self.shift + piece * WIN_LAT, count)
        return pltpu.make_async_copy(
            self.gl.at[z, rows], self.out.at[z, rows], self.out_sem.at[piece, z]
        )

    def finish_piece(self, z, piece):
        short = piece >= self.lat_windows - 1
        count = self.shift if short else WIN_LAT
        if piece == self.lat_windows:
            @pl.when(self.lat > 0)
            def _():
                self.back_copy(z, piece).wait_recv()
                self.down_copy(z).wait_recv()

            seam = self.nh[z, :, :HALO].astype(F32) + self.wh[z, :count].astype(F32)
            self.nh[z, :, :HALO] = seam.astype(BF16)
        else:
            self.back_copy(z, piece).wait_recv()
            rows = pl.ds(self.shift + piece * WIN_LAT, count)
            seam = self.gl[z, rows, :HALO].astype(F32) + self.wh[z, rows].astype(F32)
            self.gl[z, rows, :HALO] = seam.astype(BF16)
        self.store(z, piece).start()

    def finish(self, a, b):
        for z in self.pair(a):
            for piece in range(self.lat_windows):
                @pl.when(b == piece)
                def _(z=z, piece=piece):
                    self.finish_piece(z, piece)

    def end(self):
        def top(z, _):
            self.finish_piece(z, self.lat_windows)
            return 0

        def level(piece, z, _):
            for i in range(2):
                self.east_copy(i, z, piece).wait_send()
            self.back_copy(z, piece).wait_send()
            self.store(z, piece).wait()
            return 0

        def near(z, _):
            self.store(z, self.lat_windows).wait()
            return 0

        def up(z, _):
            for i in range(2):
                self.south_copy(i, z).wait_send()
                self.east_copy(i, z, self.lat_windows).wait_send()
            return 0

        def down(z, _):
            self.back_copy(z, self.lat_windows).wait_send()
            self.down_copy(z).wait_send()
            return 0

        lax.fori_loop(0, self.levels, top, 0)
        for piece in range(self.lat_windows):
            lax.fori_loop(0, self.levels, functools.partial(level, piece), 0)
        lax.fori_loop(0, self.levels, near, 0)

        @pl.when(self.lat > 0)
        def _():
            lax.fori_loop(0, self.levels, up, 0)

        @pl.when(self.lat < self.lats - 1)
        def _():
            lax.fori_loop(0, self.levels, down, 0)


def enter(n, lats):
    me, lat = lax.axis_index("lon"), lax.axis_index("lat")
    barrier = pltpu.get_barrier_semaphore()
    for o in range(1, n):
        pl.semaphore_signal(
            barrier, inc=1, device_id={"lon": lax.rem(me + o, n)},
            device_id_type=pl.DeviceIdType.MESH,
        )
    for o in range(1, lats):
        pl.semaphore_signal(
            barrier, inc=1, device_id={"lat": lax.rem(lat + o, lats)},
            device_id_type=pl.DeviceIdType.MESH,
        )
    for o in (-1, 1):
        pl.semaphore_signal(
            barrier, inc=1,
            device_id={"lat": lax.rem(lat + o + lats, lats), "lon": lax.rem(me + o + n, n)},
            device_id_type=pl.DeviceIdType.MESH,
        )
    pl.semaphore_wait(barrier, n + lats)


class WeightSum:
    def __init__(self, n, lats, wg, w1, w2, wout, sems):
        self.n, self.lats = n, lats
        self.wg, self.w1, self.w2, self.wout = wg, w1, w2, wout
        self.s1, self.s2, self.s3 = sems
        self.me, self.lat = lax.axis_index("lon"), lax.axis_index("lat")

    def remote(self, src, dst, sems, out_at, in_at, device):
        return pltpu.make_async_remote_copy(
            src_ref=src, dst_ref=dst, send_sem=sems.at[0, out_at], recv_sem=sems.at[1, in_at],
            device_id=device, device_id_type=pl.DeviceIdType.MESH,
        )

    def first(self, o, arriving):
        p = lax.rem(self.me + o, self.n)
        slot = p if arriving else self.me
        return self.remote(self.wg.at[p], self.w1.at[slot], self.s1, p, slot, {"lon": p})

    def second(self, o, arriving):
        p = lax.rem(self.lat + o, self.lats)
        slot = p if arriving else self.lat
        return self.remote(self.w2.at[slot], self.w2.at[slot], self.s2, p, slot, {"lat": p})

    def third(self, o, arriving):
        p = lax.rem(self.me + o, self.n)
        slot = p if arriving else self.me
        return self.remote(self.wout.at[slot], self.wout.at[slot], self.s3, p, slot, {"lon": p})

    def start(self):
        for o in range(1, self.n):
            self.first(o, False).start()
        self.w1[pl.ds(self.me, 1)] = self.wg[pl.ds(self.me, 1)]

    def step_one(self):
        for o in range(1, self.n):
            self.first(o, True).wait_recv()
        total = jnp.sum(self.w1[...].astype(F32), axis=0, keepdims=True)
        self.w2[pl.ds(self.lat, 1)] = total.astype(BF16)
        for o in range(1, self.lats):
            self.second(o, False).start()

    def step_two(self):
        for o in range(1, self.lats):
            self.second(o, True).wait_recv()
        total = jnp.sum(self.w2[...].astype(F32), axis=0, keepdims=True)
        self.wout[pl.ds(self.me, 1)] = total.astype(BF16)
        for o in range(1, self.n):
            self.third(o, False).start()

    def finish(self):
        for o in range(1, self.n):
            self.third(o, True).wait_recv()
        for o in range(1, self.n):
            self.first(o, False).wait_send()
            self.third(o, False).wait_send()
        for o in range(1, self.lats):
            self.second(o, False).wait_send()


def flip(mains, under, right, corner):
    lane = lax.broadcasted_iota(jnp.int32, (TAIL, LANES), 1) // TAIL
    spare = jnp.zeros((LANES - HEADS * TAIL, LANES), F32)
    mains_t = [block.T for block in mains]
    right_t = jnp.concatenate(under + [spare], axis=0).T
    turned = right.T
    under_t = [turned[h * TAIL : (h + 1) * TAIL] for h in range(HEADS)]
    pad = jnp.zeros((LANES - TAIL, LANES), F32)
    turned = jnp.concatenate([corner, pad], axis=0).T
    corner_t = jnp.zeros((TAIL, LANES), F32)
    for h in range(HEADS):
        piece = turned[h * TAIL : (h + 1) * TAIL]
        if h:
            piece = pltpu.roll(piece, h * TAIL, 1)
        corner_t = jnp.where(lane == h, piece, corner_t)
    return mains_t, under_t, right_t, corner_t


def kernel(
    n,
    lats,
    kinds,
    lat_windows,
    level_windows,
    lon_windows,
    perm_ref,
    back_ref,
    x0_ref,
    x1_ref,
    x2_ref,
    x3_ref,
    c0_ref,
    c1_ref,
    c2_ref,
    c3_ref,
    x_hbm,
    c_hbm,
    wqkv_ref,
    wback_ref,
    wproj_ref,
    bias_ref,
    side_ref,
    wout_ref,
    gbias_hbm,
    grad_hbm,
    q_s,
    m_s,
    qt_s,
    mt_s,
    kt_s,
    vt_s,
    p_s,
    ds_s,
    shift_s,
    mix_s,
    dqt_s,
    gqkv_s,
    gproj_s,
    gbias_s,
    pair_s,
    sum_s,
    cross_s,
    red_s,
    wg_s,
    w1_s,
    w2_s,
    w3_s,
    east_s,
    south_s,
    gl_s,
    gh_s,
    wh_s,
    nh_s,
    below_s,
    pair_sem,
    cross_sem,
    back_sem,
    fwd_sem,
    store_sem,
    w1_sem,
    w2_sem,
    w3_sem,
    east_sem,
    south_sem,
    wh_sem,
    nh_sem,
    out_sem,
):
    step = pl.program_id(0)
    a = lax.rem(step, level_windows)
    b = step // level_windows
    channels = wqkv_ref.shape[1]
    head_dim = channels // HEADS
    scale = head_dim ** -0.5
    levels = x_hbm.shape[0]
    shift = WIN_LAT // 2
    breadth = x0_ref.shape[2]
    tails = HEADS * LANES
    stack = HEADS * WTOK

    @pl.when(step == 0)
    def _():
        for ref in (gqkv_s, gproj_s, q_s, m_s, qt_s, mt_s):
            ref[...] = jnp.zeros_like(ref)
        gbias_s[:, stack + WTOK :, :] = jnp.zeros((kinds, PACKED - stack - WTOK, LANES), BF16)
        enter(n, lats)

    halo = Halo(
        n, lats, levels, level_windows, lat_windows,
        ((x_hbm, c_hbm), east_s, south_s, gl_s, gh_s, wh_s, nh_s, grad_hbm),
        (east_sem, south_sem, wh_sem, nh_sem, out_sem),
    )
    pl.when(step == 0)(halo.send)
    halo.arrive(a, b)

    perm = perm_ref[...]
    bottom = b == lat_windows - 1

    def raw(which, refs):
        flat = lambda t: t.reshape(-1, channels)
        parts = []
        for u, z in enumerate(halo.pair(a)):
            @pl.when(bottom)
            def _(u=u, z=z):
                below_s[which, u] = south_s[which, z]

            @pl.when(jnp.logical_not(bottom))
            def _(u=u):
                below_s[which, u] = refs[2 * u + 1][0]

            parts += [flat(refs[2 * u][0]), flat(below_s[which, u])]
        for z in halo.pair(a):
            parts.append(flat(east_s[which, z, pl.ds(b * WIN_LAT, WIN_LAT)]))
        return jnp.concatenate(parts, axis=0)

    x_raw = raw(0, (x0_ref, x1_ref, x2_ref, x3_ref))
    c_raw = raw(1, (c0_ref, c1_ref, c2_ref, c3_ref))
    x = mm(perm, x_raw).astype(BF16)
    c = mm(perm, c_raw).astype(BF16)
    q = (mm(x, wqkv_ref[0]) * (scale * LOG2E)).astype(BF16)
    k = mm(x, wqkv_ref[1]).astype(BF16)
    v = mm(x, wqkv_ref[2]).astype(BF16)
    m = mm(c, wproj_ref[...]).astype(BF16)

    wrap_here = a == level_windows - 1
    dead_here = bottom & (lax.axis_index("lat") == lats - 1)
    per_level = WTOK // WIN_Z

    def classes(token):
        upper = token >= per_level
        inner = jnp.where(upper, token - per_level, token)
        wrapped = jnp.where(upper & wrap_here, 2, 0)
        dead = jnp.where((inner >= per_level // 2) & dead_here, 1, 0)
        return wrapped + dead

    lane = lax.broadcasted_iota(jnp.int32, (1, LANES), 1)
    key_class = classes(lax.broadcasted_iota(jnp.int32, (WTOK, LANES), 0))
    mask_main = jnp.where(key_class == classes(lane), 0.0, -1e30)
    mask_tail = jnp.where(key_class == classes(LANES + lax.rem(lane, TAIL)), 0.0, -1e30)

    table = lambda lo, rows: bias_ref[0, lo : lo + rows, :].astype(F32) * LOG2E
    mains_t, under_t, right_t, corner_t = flip(
        [table(h * WTOK, LANES) for h in range(HEADS)],
        [table(h * WTOK + LANES, TAIL) for h in range(HEADS)],
        side_ref[0, :LANES, :].astype(F32) * LOG2E,
        side_ref[0, LANES:, :].astype(F32) * LOG2E,
    )
    for h in range(HEADS):
        cols = slice(h * LANES, (h + 1) * LANES)
        shift_s[:LANES, cols] = mains_t[h] + mask_main[:LANES]
        shift_s[LANES:, cols] = under_t[h] + mask_main[LANES:]
    shift_s[:LANES, tails:] = right_t + mask_tail[:LANES]
    shift_s[LANES:, tails:] = corner_t + mask_tail[LANES:]

    whole = lon_windows * LANES
    main = lambda w: slice(w * LANES, (w + 1) * LANES)
    tail = lambda w: slice(whole + w * TAIL, whole + (w + 1) * TAIL)
    window = lambda t, w: jnp.concatenate([t[main(w)], t[tail(w)]], axis=0)
    keys = [window(k, w) for w in range(lon_windows)]
    values = [window(v, w) for w in range(lon_windows)]
    for w in range(lon_windows):
        for flat, wide_s, turned_s in ((q, q_s, qt_s), (m, m_s, mt_s)):
            turned = flat[main(w)].T
            for h in range(HEADS):
                cs = slice(h * head_dim, (h + 1) * head_dim)
                wide_s[w, h * LANES : (h + 1) * LANES, cs] = flat[main(w), cs]
                wide_s[w, tails + h * TAIL : tails + (h + 1) * TAIL, cs] = flat[tail(w), cs]
                turned_s[w, cs, h * LANES : (h + 1) * LANES] = turned[cs]
            turned_s[w, :, tails:] = wide_s[w, tails:, :].T
        kt_s[w] = keys[w].T
        vt_s[w] = values[w].T

    tiles = HEADS + 1
    gb = []
    for j in range(0, tiles, 2):
        cols = slice(j * LANES, min(j + 2, tiles) * LANES)
        total = [None, None]
        for w in range(lon_windows):
            s2 = mm(keys[w], qt_s[w, :, cols])
            dp2 = mm(values[w], mt_s[w, :, cols])
            for i in range(min(2, tiles - j)):
                here = slice(i * LANES, (i + 1) * LANES)
                at = slice((j + i) * LANES, (j + i + 1) * LANES)
                s = s2[:, here] + shift_s[:, at]
                dp = dp2[:, here]
                e = jnp.exp2(s - jnp.max(s, axis=0, keepdims=True))
                r = 1.0 / jnp.sum(e, axis=0, keepdims=True)
                p = e * r
                delta = jnp.sum(p * dp, axis=0, keepdims=True)
                ds = p * (dp - delta)
                p_s[w, :, at] = p.astype(BF16)
                ds_s[w, :, at] = ds.astype(BF16)
                total[i] = ds if total[i] is None else total[i] + ds
        gb += total[: min(2, tiles - j)]

    tail_lane = lax.broadcasted_iota(jnp.int32, (head_dim, LANES), 1) // TAIL
    for turned_s, from_s, to_s, factor in ((vt_s, p_s, mix_s, None), (kt_s, ds_s, dqt_s, scale)):
        far = [None] * HEADS
        for w in range(lon_windows):
            for j in range(0, HEADS, 2):
                rows = slice(j * head_dim, (j + 2) * head_dim)
                out = mm(turned_s[w, rows, :], from_s[w, :, j * LANES : (j + 2) * LANES])
                if factor is not None:
                    out = out * factor
                for i in range(2):
                    cs = slice((j + i) * head_dim, (j + i + 1) * head_dim)
                    piece = out[i * head_dim : (i + 1) * head_dim, i * LANES : (i + 1) * LANES]
                    to_s[cs, main(w)] = piece.astype(BF16)
            out = mm(turned_s[w], from_s[w, :, tails:])
            if factor is not None:
                out = out * factor
            for h in range(HEADS):
                piece = out[h * head_dim : (h + 1) * head_dim]
                turn = (w - h) * TAIL % LANES
                if turn:
                    piece = pltpu.roll(piece, turn, 1)
                far[h] = jnp.where(tail_lane == w, piece, 0.0 if far[h] is None else far[h])
        for h in range(HEADS):
            cs = slice(h * head_dim, (h + 1) * head_dim)
            to_s[cs, whole:] = far[h].astype(BF16)

    dk, dv = [], []
    for w in range(lon_windows):
        dk.append((mm(ds_s[w], q_s[w]) * (1.0 / LOG2E)).astype(BF16))
        dv.append(mm(p_s[w], m_s[w]).astype(BF16))
    order = lambda ts: jnp.concatenate([t[:LANES] for t in ts] + [t[LANES:] for t in ts], axis=0)
    tokens = lon_windows * WTOK
    dq = dqt_s[...].T[:tokens]
    cols = [dq, order(dk), order(dv)]
    xt = x.T
    for i in range(3):
        gqkv_s[i] += mm(xt, cols[i])
    gproj_s[...] += mm(mix_s[:, :tokens], c)
    gin = mm(cols[0], wback_ref[0]) + mm(cols[1], wback_ref[1]) + mm(cols[2], wback_ref[2])
    gout = mm(back_ref[...], gin.astype(BF16)).astype(BF16)
    near, far = WIN_LAT * breadth, WIN_LAT * HALO
    for u, z in enumerate(halo.pair(a)):
        rows = pl.ds(shift + b * WIN_LAT, WIN_LAT)
        own = gout[u * near : (u + 1) * near]
        gl_s[z, rows] = own.reshape(WIN_LAT, breadth, channels)
        strip = gout[WIN_Z * near + u * far : WIN_Z * near + (u + 1) * far]
        gh_s[z, pl.ds(b * WIN_LAT, WIN_LAT)] = strip.reshape(WIN_LAT, HALO, channels)
    halo.give(a, b)
    late = step - GRAD_LAG

    @pl.when(late >= 0)
    def _():
        halo.finish(lax.rem(late, level_windows), late // level_windows)


    mains_t, under_t, right_t, corner_t = flip(
        [gb[h][:LANES] for h in range(HEADS)],
        [gb[h][LANES:] for h in range(HEADS)],
        gb[HEADS][:LANES],
        gb[HEADS][LANES:],
    )
    for h in range(HEADS):
        gbias_s[step, h * WTOK : h * WTOK + LANES, :] = mains_t[h].astype(BF16)
        gbias_s[step, h * WTOK + LANES : (h + 1) * WTOK, :] = under_t[h].astype(BF16)
    gbias_s[step, stack : stack + LANES, :] = right_t.astype(BF16)
    gbias_s[step, stack + LANES : stack + WTOK, :] = corner_t.astype(BF16)

    ex = Exchange(
        n, kinds,
        (gbias_s, pair_s, sum_s, cross_s, red_s, gbias_hbm),
        (pair_sem, cross_sem, back_sem, fwd_sem, store_sem),
    )
    ex.behind(step)
    ex.pair_copy(step).start()

    @pl.when(step == kinds - 1)
    def _():
        share = channels // n
        for i in range(n):
            rows = slice(i * share, (i + 1) * share)
            for j in range(3):
                wg_s[i, j * share : (j + 1) * share, :] = gqkv_s[j, rows].astype(BF16)
            wg_s[i, 3 * share :, :] = gproj_s[rows].astype(BF16)
        ws = WeightSum(n, lats, wg_s, w1_s, w2_s, w3_s, (w1_sem, w2_sem, w3_sem))
        ws.start()
        ex.behind(kinds)
        for late in range(kinds - GRAD_LAG, kinds):
            halo.finish(late % level_windows, late // level_windows)
        ex.behind(kinds + 1)
        ws.step_one()
        ex.behind(kinds + 2)
        ex.behind(kinds + 3)
        ws.step_two()
        ex.behind(kinds + 4)
        ex.behind(kinds + 5)
        ws.finish()
        wout_ref[...] = w3_s[...]
        ex.drain()
        halo.end()


def pack_kernel(table_ref, main_ref, tail_ref, main_s, tail_s):
    h = pl.program_id(0)
    kinds = table_ref.shape[1]
    group = LANES // TAIL
    lane = lax.broadcasted_iota(jnp.int32, (kinds, LANES), 1)

    def body(m, _):
        tiles = []
        for r in range(group + 1):
            start = pl.multiple_of(m * (group * WTOK) + r * LANES, LANES)
            tiles.append(table_ref[0, :, pl.ds(start, LANES)].astype(F32))
        for r in range(group):
            turn = (LANES - TAIL * r) % LANES
            left = pltpu.roll(tiles[r], turn, 1) if r else tiles[r]
            right = pltpu.roll(tiles[r + 1], turn, 1) if r else tiles[r + 1]
            whole = jnp.where(lane < LANES - TAIL * r, left, right) if r else left
            at = m * group + r
            main_s[pl.ds(at, kinds, stride=WTOK), :] = whole
            tail_s[pl.ds(at, kinds, stride=WTOK), :] = right
        return 0

    lax.fori_loop(0, WTOK // group, body, 0)
    wide = lax.broadcasted_iota(jnp.int32, (WTOK, LANES), 1) // TAIL

    def out(t, _):
        at = pl.ds(pl.multiple_of(t * WTOK, WTOK), WTOK)
        main_ref[t, 0] = main_s[at, :].astype(BF16)
        turned = pltpu.roll(tail_s[at, :], h * TAIL, 1)
        before = jnp.where(h == 0, 0.0, tail_ref[t].astype(F32))
        tail_ref[t] = jnp.where(wide == h, turned, before).astype(BF16)
        return 0

    lax.fori_loop(0, kinds, out, 0)


def pack(table):
    heads, kinds, flat = table.shape
    main, tail = pl.pallas_call(
        pack_kernel,
        grid=(heads,),
        in_specs=[pl.BlockSpec((1, kinds, flat), lambda i: (i, 0, 0))],
        out_specs=[
            pl.BlockSpec((kinds, 1, WTOK, LANES), lambda i: (0, i, 0, 0)),
            pl.BlockSpec((kinds, WTOK, LANES), lambda i: (0, 0, 0)),
        ],
        out_shape=[
            jax.ShapeDtypeStruct((kinds, heads, WTOK, LANES), BF16),
            jax.ShapeDtypeStruct((kinds, WTOK, LANES), BF16),
        ],
        scratch_shapes=[pltpu.VMEM((kinds * WTOK, LANES), F32)] * 2,
        cost_estimate=pl.CostEstimate(
            flops=10_000_000_000, bytes_accessed=10_000_000, transcendentals=0
        ),
    )(table)
    return main, tail


def unpack_kernel(packed_ref, out_ref, main_s, tail_s):
    stack = HEADS * WTOK
    main_s[...] = packed_ref[0, :stack].astype(F32)
    tails = packed_ref[0, stack : stack + WTOK].astype(F32)
    for h in range(HEADS):
        turned = tails if h == 0 else pltpu.roll(tails, LANES - h * TAIL, 1)
        tail_s[h * WTOK : (h + 1) * WTOK] = turned
    group = LANES // TAIL
    lane = lax.broadcasted_iota(jnp.int32, (HEADS, LANES), 1)

    def body(m, _):
        before_main = before_tail = None
        for r in range(group + 1):
            tile = None
            if r < group:
                at = pl.ds(m * group + r, HEADS, stride=WTOK)
                here_main, here_tail = main_s[at, :], tail_s[at, :]
                if r:
                    here_main = pltpu.roll(here_main, TAIL * r, 1)
                    here_tail = pltpu.roll(here_tail, TAIL * r, 1)
                tile = here_main
            if r:
                ended = before_tail
                if r > 1:
                    ended = jnp.where(lane < TAIL * (r - 1), before_main, before_tail)
                tile = ended if r == group else jnp.where(lane < TAIL * r, ended, tile)
            start = pl.multiple_of(m * (group * WTOK) + r * LANES, LANES)
            out_ref[0, :, pl.ds(start, LANES)] = tile
            if r < group:
                before_main, before_tail = here_main, here_tail
        return 0

    def several(i, _):
        for u in range(UNROLL):
            body(i * UNROLL + u, 0)
        return 0

    lax.fori_loop(0, WTOK // group // UNROLL, several, 0)


def unpack(packed):
    kinds, rows, lanes = packed.shape
    stack = HEADS * WTOK
    return pl.pallas_call(
        unpack_kernel,
        grid=(kinds,),
        in_specs=[pl.BlockSpec((1, rows, lanes), lambda i: (i, 0, 0))],
        out_specs=pl.BlockSpec((1, HEADS, WTOK * WTOK), lambda i: (i, 0, 0)),
        out_shape=jax.ShapeDtypeStruct((kinds, HEADS, WTOK * WTOK), F32),
        scratch_shapes=[pltpu.VMEM((stack, LANES), F32), pltpu.VMEM((stack, LANES), F32)],
        cost_estimate=pl.CostEstimate(
            flops=10_000_000_000, bytes_accessed=15_000_000, transcendentals=0
        ),
    )(packed)


def window_call(perm, back, normed, cotangent, wqkv, wback, wproj, bias, side):
    levels, height, breadth, channels = normed.shape
    level_windows = levels // WIN_Z
    lat_windows = height // WIN_LAT
    lon_windows = perm.shape[0] // WTOK
    kinds = lat_windows * level_windows
    n, lats = lax.axis_size("lon"), lax.axis_size("lat")
    chips = n // 2
    shift = WIN_LAT // 2
    rows = height // shift

    def tokens(up, lower):
        def at(i):
            z = lax.rem(WIN_Z * lax.rem(i, level_windows) + 1 + up, levels)
            row = 1 + 2 * (i // level_windows) + lower
            return z, jnp.minimum(row, rows - 1), 0, 0

        return pl.BlockSpec((1, shift, breadth, channels), at)

    blocks = [tokens(up, lower) for up in range(WIN_Z) for lower in range(2)]
    whole = lambda arr: pl.BlockSpec(arr.shape, lambda i: (0,) * arr.ndim)
    const = lambda shape: pl.BlockSpec(shape, lambda i: (0,) * len(shape))
    anywhere = pl.BlockSpec(memory_space=pl.ANY)
    stack = HEADS * WTOK
    padded = (HEADS + 1) * LANES
    turned = (lon_windows + 1) * LANES
    wgrad = (4 * channels // n, channels)
    sem = lambda *k: pltpu.SemaphoreType.DMA((2,) + k)
    return pl.pallas_call(
        functools.partial(kernel, n, lats, kinds, lat_windows, level_windows, lon_windows),
        grid=(kinds,),
        in_specs=[
            whole(perm),
            whole(back),
            *blocks,
            *blocks,
            anywhere,
            anywhere,
            whole(wqkv),
            whole(wback),
            whole(wproj),
            pl.BlockSpec((1, stack, LANES), lambda i: (i, 0, 0)),
            pl.BlockSpec((1, WTOK, LANES), lambda i: (i, 0, 0)),
        ],
        out_specs=[const((n,) + wgrad), anywhere, anywhere],
        out_shape=[
            jax.ShapeDtypeStruct((n,) + wgrad, BF16),
            jax.ShapeDtypeStruct((kinds, PACKED, LANES), BF16),
            jax.ShapeDtypeStruct(normed.shape, BF16),
        ],
        scratch_shapes=[
            pltpu.VMEM((lon_windows, padded, channels), BF16),
            pltpu.VMEM((lon_windows, padded, channels), BF16),
            pltpu.VMEM((lon_windows, channels, padded), BF16),
            pltpu.VMEM((lon_windows, channels, padded), BF16),
            pltpu.VMEM((lon_windows, channels, WTOK), BF16),
            pltpu.VMEM((lon_windows, channels, WTOK), BF16),
            pltpu.VMEM((lon_windows, WTOK, padded), BF16),
            pltpu.VMEM((lon_windows, WTOK, padded), BF16),
            pltpu.VMEM((WTOK, padded), F32),
            pltpu.VMEM((channels, turned), BF16),
            pltpu.VMEM((channels, turned), BF16),
            pltpu.VMEM((3, channels, channels), F32),
            pltpu.VMEM((channels, channels), F32),
            pltpu.VMEM((kinds, PACKED, LANES), BF16),
            pltpu.VMEM((kinds, PACKED // 2, LANES), BF16),
            pltpu.VMEM((kinds, PACKED // 2, LANES), BF16),
            pltpu.VMEM((kinds, chips, PACKED // n, LANES), BF16),
            pltpu.VMEM((kinds, PACKED, LANES), BF16),
            pltpu.VMEM((n,) + wgrad, BF16),
            pltpu.VMEM((n,) + wgrad, BF16),
            pltpu.VMEM((lats,) + wgrad, BF16),
            pltpu.VMEM((n,) + wgrad, BF16),
            pltpu.VMEM((2, levels, height, HALO, channels), BF16),
            pltpu.VMEM((2, levels, shift, breadth, channels), BF16),
            pltpu.VMEM((levels, height + shift, breadth, channels), BF16),
            pltpu.VMEM((levels, height, HALO, channels), BF16),
            pltpu.VMEM((levels, height, HALO, channels), BF16),
            pltpu.VMEM((levels, shift, breadth, channels), BF16),
            pltpu.VMEM((2, WIN_Z, shift, breadth, channels), BF16),
            sem(kinds),
            sem(kinds, chips),
            sem(kinds, chips),
            sem(kinds, chips),
            pltpu.SemaphoreType.DMA((kinds,)),
            sem(n),
            sem(lats),
            sem(n),
            sem(2, lat_windows + 1, levels),
            sem(2, levels),
            sem(lat_windows + 1, levels),
            sem(levels),
            pltpu.SemaphoreType.DMA((lat_windows + 1, levels)),
        ],
        compiler_params=pltpu.CompilerParams(
            dimension_semantics=("arbitrary",),
            vmem_limit_bytes=56 * 2**20,
            collective_id=0,
            has_side_effects=True,
        ),
        cost_estimate=pl.CostEstimate(
            flops=kinds * 1_500_000_000, bytes_accessed=kinds * 2_000_000, transcendentals=0
        ),
    )(
        perm, back, *[normed] * 4, *[cotangent] * 4, normed, cotangent,
        wqkv, wback, wproj, bias, side,
    )


def local(normed, cotangent, weight_qkv, weight_proj, bias_table):
    levels, height, breadth, channels = normed.shape
    lon_shift = WIN_LON // 2
    lon_windows = breadth // WIN_LON
    bias, side = pack(jnp.swapaxes(bias_table, 0, 1))
    bias = bias.reshape(bias.shape[0], HEADS * WTOK, LANES)
    wqkv = jnp.stack(jnp.split(weight_qkv, 3, axis=1))
    wback = jnp.swapaxes(wqkv, 1, 2)
    wproj = weight_proj.T

    rows = jnp.arange(lon_windows * WTOK, dtype=jnp.int32)
    mains = lon_windows * LANES
    is_main = rows < mains
    window = jnp.where(is_main, rows // LANES, (rows - mains) // TAIL)
    token = jnp.where(is_main, rows % LANES, LANES + (rows - mains) % TAIL)
    per_level = WIN_LAT * WIN_LON
    level = token // per_level
    row = token % per_level // WIN_LON
    place = window * WIN_LON + token % WIN_LON + lon_shift
    near, far = WIN_LAT * breadth, WIN_LAT * HALO
    source = jnp.where(
        place < breadth,
        level * near + row * breadth + place,
        WIN_Z * near + level * far + row * HALO + place - breadth,
    )
    columns = jnp.arange(WIN_Z * (near + far), dtype=jnp.int32)
    perm = (source[:, None] == columns[None, :]).astype(BF16)

    weights, packed, input_grad = window_call(
        perm, perm.T, normed, cotangent, wqkv, wback, wproj, bias, side
    )
    n = lax.axis_size("lon")
    weights = weights.reshape(n, 4, channels // n, channels).astype(F32)
    weights = weights.transpose(0, 2, 1, 3).reshape(channels, 4 * channels)

    bias_grad = unpack(packed)
    return input_grad, weights[:, : 3 * channels], weights[:, 3 * channels :], bias_grad


def solution(mesh):
    in_specs = (
        P(None, "lat", "lon", None),
        P(None, "lat", "lon", None),
        P(),
        P(),
        P("lat", None, None),
    )
    out_specs = (P(None, "lat", "lon", None), P(), P(), P("lat", None, None))
    return jax.shard_map(local, mesh=mesh, in_specs=in_specs, out_specs=out_specs, check_vma=False)
```

```python
import functools
import math

import jax
import jax.numpy as jnp
import numpy as np
from jax import lax
from jax.experimental import pallas as pl
from jax.experimental.pallas import tpu as pltpu
from jax.sharding import PartitionSpec as P

HEADS = 6
WIN_Z = 2
WIN_LAT = 6
WIN_LON = 12
WTOK = 144
LANES = 128
TAIL = WTOK - LANES
HALO = 8
PACKED = 1024
GRAD_LAG = 2
LAGS = (1, 3, 5, 7, 9, 10)
UNROLL = 3
ODD = WTOK + 1
LOG2E = math.log2(math.e)
F32 = jnp.float32
BF16 = jnp.bfloat16


def mm(a, b, ca=1, cb=0):
    return lax.dot_general(a, b, (((ca,), (cb,)), ((), ())), preferred_element_type=F32)


class Exchange:
    def __init__(self, n, kinds, bufs, sems):
        self.n, self.kinds = n, kinds
        self.chips = n // 2
        self.gb, self.pair, self.sum, self.cross, self.out, self.hbm = bufs
        self.pair_sem, self.cross_sem, self.back_sem, self.fwd_sem, self.store_sem = sems
        me = lax.axis_index("lon")
        self.me = me
        self.core = lax.rem(me, 2)
        self.chip = me // 2
        self.other = 1 - self.core
        self.partner = self.chip * 2 + self.other
        self.half = PACKED // 2
        self.part = self.half // self.chips

    def remote(self, src, dst, send, recv, device):
        return pltpu.make_async_remote_copy(
            src_ref=src, dst_ref=dst, send_sem=send, recv_sem=recv,
            device_id={"lon": device}, device_id_type=pl.DeviceIdType.MESH,
        )

    def peer(self, o):
        return lax.rem(self.chip + o, self.chips)

    def rows(self, core, chip):
        return pl.ds(core * self.half + chip * self.part, self.part)

    def pair_copy(self, t):
        src = self.gb.at[t, pl.ds(self.other * self.half, self.half)]
        return self.remote(
            src, self.pair.at[t], self.pair_sem.at[0, t], self.pair_sem.at[1, t], self.partner
        )

    def cross_copy(self, t, o, arriving):
        j = self.peer(o)
        src = self.sum.at[t, pl.ds(j * self.part, self.part)]
        slot = j if arriving else self.chip
        return self.remote(
            src, self.cross.at[t, slot], self.cross_sem.at[0, t, j],
            self.cross_sem.at[1, t, slot], j * 2 + self.core,
        )

    def back_copy(self, t, o, arriving):
        j = self.peer(o)
        slot = j if arriving else self.chip
        part = self.out.at[t, self.rows(self.core, slot)]
        return self.remote(
            part, part, self.back_sem.at[0, t, j], self.back_sem.at[1, t, slot],
            j * 2 + self.core,
        )

    def fwd_copy(self, t, arriving):
        core = self.other if arriving else self.core
        part = self.out.at[t, pl.ds(core * self.half, self.half)]
        return self.remote(
            part, part, self.fwd_sem.at[0, t], self.fwd_sem.at[1, t], self.partner
        )

    def store(self, t):
        return pltpu.make_async_copy(self.out.at[t], self.hbm.at[t], self.store_sem.at[t])

    def stage_pair(self, t):
        self.pair_copy(t).wait_recv()
        mine = self.gb[t, pl.ds(self.core * self.half, self.half)].astype(F32)
        total = (mine + self.pair[t].astype(F32)).astype(BF16)
        self.sum[t] = total
        for o in range(1, self.chips):
            self.cross_copy(t, o, False).start()

    def stage_cross(self, t):
        for o in range(1, self.chips):
            self.cross_copy(t, o, True).wait_recv()
        acc = self.sum[t, pl.ds(self.chip * self.part, self.part)].astype(F32)
        for o in range(1, self.chips):
            acc = acc + self.cross[t, self.peer(o)].astype(F32)
        self.out[t, self.rows(self.core, self.chip)] = acc.astype(BF16)
        for o in range(1, self.chips):
            self.back_copy(t, o, False).start()

    def stage_back(self, t):
        for o in range(1, self.chips):
            self.back_copy(t, o, True).wait_recv()
        self.fwd_copy(t, False).start()

    def stage_fwd(self, t):
        self.fwd_copy(t, True).wait_recv()
        self.store(t).start()

    def stages(self):
        return [self.stage_pair, self.stage_cross, self.stage_back, self.stage_fwd]

    def behind(self, step):
        for lag, stage in zip(LAGS, self.stages()):
            t = step - lag
            if isinstance(t, int):
                if 0 <= t < self.kinds:
                    stage(t)
            else:
                pl.when(t >= 0)(functools.partial(stage, t))

    def rest(self):
        stages = self.stages()
        done = [self.kinds - lag for lag in LAGS[: len(stages)]]
        while done[-1] < self.kinds:
            limit = [self.kinds] + done[:-1]
            for k, stage in enumerate(stages):
                for t in range(done[k], min(done[k] + 2, limit[k])):
                    stage(t)
                done[k] = max(done[k], min(done[k] + 2, limit[k]))
            yield

    def drain(self):
        def body(t, _):
            self.pair_copy(t).wait_send()
            for o in range(1, self.chips):
                self.cross_copy(t, o, False).wait_send()
                self.back_copy(t, o, False).wait_send()
            self.fwd_copy(t, False).wait_send()
            self.store(t).wait()
            return 0

        lax.fori_loop(0, self.kinds, body, 0)


class Square(Exchange):
    def __init__(self, n, kinds, bufs, sems):
        pair_bufs, one, sums, two = bufs[:3] + bufs[4:], bufs[3][0], bufs[3][1], bufs[3][2]
        gb, pair, total, out, hbm = pair_bufs
        super().__init__(n, kinds, (gb, pair, total, None, out, hbm), sems)
        self.one, self.sums, self.two = one, sums, two
        bits = (lax.rem(self.chip, 2), self.chip // 2)
        flip_x = self.chip + 1 - 2 * bits[0]
        flip_y = lax.rem(self.chip + 2, self.chips)
        self.first = (flip_x * 2 + self.core, flip_y * 2 + self.core)
        self.second = self.first[::-1]
        self.bit = bits
        self.other_bit = bits[::-1]
        self.plane = self.half // 2
        self.send_sem, self.step_sem = sems[0], sems[1]

    def coarse(self, p, bit):
        return pl.ds(p * self.plane + bit * (self.plane // 2), self.plane // 2)

    def fine(self, bit):
        return pl.ds(bit * (self.plane // 4), self.plane // 4)

    def placed(self, t, p, start, rows):
        at = self.core * self.half + p * self.plane + start
        return self.out.at[t, pl.ds(at, rows)]

    def pair_copy(self, t):
        src = self.gb.at[t, pl.ds(self.other * self.half, self.half)]
        return self.remote(
            src, self.pair.at[t], self.send_sem.at[0], self.step_sem.at[0, t], self.partner
        )

    def fwd_copy(self, t, arriving):
        core = self.other if arriving else self.core
        part = self.out.at[t, pl.ds(core * self.half, self.half)]
        return self.remote(
            part, part, self.send_sem.at[5], self.step_sem.at[5, t], self.partner
        )

    def copy(self, src, dst, k, t, device):
        return self.remote(src, dst, self.send_sem.at[k], self.step_sem.at[k, t], device)

    def one_copy(self, t, p):
        src = self.sum.at[t, self.coarse(p, 1 - self.bit[p])]
        return self.copy(src, self.one.at[t, p], 1, t, self.first[p])

    def two_copy(self, t, p):
        src = self.sums.at[t, p, self.fine(1 - self.other_bit[p])]
        return self.copy(src, self.two.at[t, p], 2, t, self.second[p])

    def three_copy(self, t, p):
        start = self.bit[p] * (self.plane // 2) + self.other_bit[p] * (self.plane // 4)
        part = self.placed(t, p, start, self.plane // 4)
        return self.copy(part, part, 3, t, self.second[p])

    def four_copy(self, t, p):
        part = self.placed(t, p, self.bit[p] * (self.plane // 2), self.plane // 2)
        return self.copy(part, part, 4, t, self.first[p])

    def both(self, buf, k, t):
        return self.copy(buf.at[t], buf.at[t], k, t, self.partner)

    def stage_pair(self, t):
        self.pair_copy(t).wait_recv()
        mine = self.gb[t, pl.ds(self.core * self.half, self.half)].astype(F32)
        self.sum[t] = (mine + self.pair[t].astype(F32)).astype(BF16)
        for p in range(2):
            self.one_copy(t, p).start()

    def stage_one(self, t):
        self.both(self.one, 1, t).wait_recv()
        for p in range(2):
            mine = self.sum[t, self.coarse(p, self.bit[p])].astype(F32)
            self.sums[t, p] = (mine + self.one[t, p].astype(F32)).astype(BF16)
        for p in range(2):
            self.two_copy(t, p).start()

    def stage_two(self, t):
        self.both(self.two, 2, t).wait_recv()
        for p in range(2):
            mine = self.sums[t, p, self.fine(self.other_bit[p])].astype(F32)
            total = (mine + self.two[t, p].astype(F32)).astype(BF16)
            start = self.bit[p] * (self.plane // 2) + self.other_bit[p] * (self.plane // 4)
            at = self.core * self.half + p * self.plane + start
            self.out[t, pl.ds(at, self.plane // 4)] = total
        for p in range(2):
            self.three_copy(t, p).start()

    def stage_three(self, t):
        self.both(self.two, 3, t).wait_recv()
        for p in range(2):
            self.four_copy(t, p).start()

    def stage_four(self, t):
        self.both(self.one, 4, t).wait_recv()
        self.fwd_copy(t, False).start()

    def store(self, t):
        return pltpu.make_async_copy(self.out.at[t], self.hbm.at[t], self.store_sem.at[0])

    def stages(self):
        return [
            self.stage_pair, self.stage_one, self.stage_two, self.stage_three,
            self.stage_four, self.stage_fwd,
        ]

    def drain(self):
        for k, buf in enumerate((self.pair, self.one, self.two, self.two, self.one, self.pair)):
            self.remote(
                buf, buf, self.send_sem.at[k], self.step_sem.at[k, 0], self.partner
            ).wait_send()
        pltpu.make_async_copy(self.out, self.hbm, self.store_sem.at[0]).wait()


class Halo:
    def __init__(self, n, lats, levels, level_windows, lat_windows, refs, sems):
        self.n, self.lats = n, lats
        self.levels, self.level_windows, self.lat_windows = levels, level_windows, lat_windows
        self.given, self.body, self.east, self.gl, self.gh, self.wh, self.nh, self.out = refs
        self.load_sem, self.east_sem, self.south_sem, self.wh_sem, self.nh_sem, self.out_sem = sems
        self.me, self.lat = lax.axis_index("lon"), lax.axis_index("lat")
        self.shift = WIN_LAT // 2
        self.height = lat_windows * WIN_LAT
        self.last = lat_windows - 1
        self.last_lat = self.lat == lats - 1
        self.strip = pl.ds(0, WIN_LON // 2)
        self.parts = ((1, WIN_Z), (1 + WIN_Z, levels - 1 - WIN_Z), (0, 1))

    def remote(self, src, dst, sems, at, lat, lon, send_at=None):
        device = {"lat": self.lat + lat, "lon": lax.rem(self.me + lon + self.n, self.n)}
        send = (0,) + (at if send_at is None else send_at)
        return pltpu.make_async_remote_copy(
            src_ref=src, dst_ref=dst, send_sem=sems.at[send], recv_sem=sems.at[(1,) + at],
            device_id=device, device_id_type=pl.DeviceIdType.MESH,
        )

    def count(self, bottom):
        return self.shift if bottom else WIN_LAT

    def load(self, i, b, bottom):
        rows = pl.ds(self.shift + b * WIN_LAT, self.count(bottom))
        return pltpu.make_async_copy(
            self.given[i].at[:, rows], self.body.at[i, :, rows], self.load_sem.at[i, b]
        )

    def east_copy(self, i, part, b, bottom):
        level = pl.ds(*self.parts[part])
        src = pl.ds(self.shift + b * WIN_LAT, self.count(bottom))
        dst = pl.ds(b * WIN_LAT, self.count(bottom))
        return self.remote(
            self.given[i].at[level, src, self.strip, :], self.east.at[i, level, dst, self.strip, :],
            self.east_sem, (i, b, part), 0, -1, (i, 0, 0),
        )

    def east_all(self, i):
        rows = pl.ds(self.shift, self.height - self.shift)
        src = self.given[i].at[:, rows, self.strip, :]
        dst = self.east.at[i, :, rows, self.strip, :]
        return self.remote(src, dst, self.east_sem, (i, 0, 0), 0, -1)

    def corner_copy(self, i):
        src, dst = pl.ds(0, self.shift), pl.ds(self.height - self.shift, self.shift)
        return self.remote(
            self.given[i].at[:, src, self.strip, :], self.east.at[i, :, dst, self.strip, :],
            self.east_sem, (i, self.lat_windows, 0), -1, -1,
        )

    def south_copy(self, i):
        src = self.given[i].at[:, pl.ds(0, self.shift)]
        dst = self.body.at[i, :, pl.ds(self.height, self.shift)]
        return self.remote(src, dst, self.south_sem, (i,), -1, 0)

    def begin(self):
        for b in range(self.lat_windows):
            for i in range(2):
                self.load(i, b, b == self.last).start()
        self.east[...] = jnp.zeros_like(self.east)
        self.wh[...] = jnp.zeros_like(self.wh)

        @pl.when(self.last_lat)
        def _():
            shape = self.body.shape
            blank = jnp.zeros(shape[:2] + (self.shift,) + shape[3:], BF16)
            self.body[:, :, pl.ds(self.height, self.shift)] = blank

        @pl.when(self.lat == 0)
        def _():
            self.nh[...] = jnp.zeros_like(self.nh)

    def send(self, b, bottom):
        for part in range(3):
            for i in range(2):
                self.east_copy(i, part, b, bottom).start()
        if bottom:
            @pl.when(self.lat > 0)
            def _():
                for i in range(2):
                    self.south_copy(i).start()
                    self.corner_copy(i).start()

    def send_next(self, b):
        pl.when(b + 1 < self.last)(lambda: self.send(b + 1, False))
        pl.when(b + 1 == self.last)(lambda: self.send(self.last, True))

    def pair(self, a):
        return [lax.rem(WIN_Z * a + 1 + u, self.levels) for u in range(WIN_Z)]

    def arrive_part(self, part, b, bottom):
        for i in range(2):
            if part == 0:
                self.load(i, b, bottom).wait()
            self.east_copy(i, part, b, bottom).wait_recv()
        if bottom and part == 0:
            @pl.when(jnp.logical_not(self.last_lat))
            def _():
                for i in range(2):
                    self.corner_copy(i).wait_recv()
                    self.south_copy(i).wait_recv()

    def arrive(self, a, b):
        at = (a == 0, a == 1, a == self.level_windows - 1)
        for part in range(3):
            pl.when(at[part] & (b < self.last))(
                functools.partial(self.arrive_part, part, b, False)
            )
            pl.when(at[part] & (b == self.last))(
                functools.partial(self.arrive_part, part, self.last, True)
            )

    def back_copy(self, b, bottom):
        src = pl.ds(b * WIN_LAT, self.count(bottom))
        dst = pl.ds(self.shift + b * WIN_LAT, self.count(bottom))
        return self.remote(
            self.gh.at[:, src, self.strip, :], self.wh.at[:, dst, self.strip, :],
            self.wh_sem, (b,), 0, 1,
        )

    def back_corner(self):
        src, dst = pl.ds(self.height - self.shift, self.shift), pl.ds(0, self.shift)
        return self.remote(
            self.gh.at[:, src, self.strip, :], self.wh.at[:, dst, self.strip, :],
            self.wh_sem, (self.lat_windows,), 1, 1,
        )

    def down_copy(self):
        src = self.gl.at[:, pl.ds(self.height, self.shift)]
        return self.remote(src, self.nh, self.nh_sem, (), 1, 0)

    def give_last(self):
        @pl.when(jnp.logical_not(self.last_lat))
        def _():
            self.back_corner().start()
            self.down_copy().start()

        self.back_copy(self.last, True).start()

    def store(self, b, bottom):
        rows = pl.ds(self.shift + b * WIN_LAT, self.count(bottom))
        return pltpu.make_async_copy(
            self.gl.at[:, rows], self.out.at[:, rows], self.out_sem.at[b]
        )

    def store_top(self):
        rows = pl.ds(0, self.shift)
        return pltpu.make_async_copy(
            self.nh, self.out.at[:, rows], self.out_sem.at[self.lat_windows]
        )

    def finish(self, b, bottom):
        self.back_copy(b, bottom).wait_recv()
        rows = pl.ds(self.shift + b * WIN_LAT, self.count(bottom))
        seam = self.gl[:, rows, :HALO].astype(F32) + self.wh[:, rows].astype(F32)
        self.gl[:, rows, :HALO] = seam.astype(BF16)
        self.store(b, bottom).start()

    def finish_top(self):
        @pl.when(self.lat > 0)
        def _():
            self.back_corner().wait_recv()
            self.down_copy().wait_recv()

        seam = self.nh[:, :, :HALO].astype(F32) + self.wh[:, : self.shift].astype(F32)
        self.nh[:, :, :HALO] = seam.astype(BF16)
        self.store_top().start()

    def end(self):
        for b in range(self.lat_windows):
            bottom = b == self.last
            self.back_copy(b, bottom).wait_send()
            self.store(b, bottom).wait()
        self.store_top().wait()
        for i in range(2):
            self.east_all(i).wait_send()

        @pl.when(self.lat > 0)
        def _():
            for i in range(2):
                self.south_copy(i).wait_send()
                self.corner_copy(i).wait_send()

        @pl.when(jnp.logical_not(self.last_lat))
        def _():
            self.back_corner().wait_send()
            self.down_copy().wait_send()


def enter(n, lats):
    me, lat = lax.axis_index("lon"), lax.axis_index("lat")
    barrier = pltpu.get_barrier_semaphore()
    for o in range(1, n):
        pl.semaphore_signal(
            barrier, inc=1, device_id={"lon": lax.rem(me + o, n)},
            device_id_type=pl.DeviceIdType.MESH,
        )
    for o in range(1, lats):
        pl.semaphore_signal(
            barrier, inc=1, device_id={"lat": lax.rem(lat + o, lats)},
            device_id_type=pl.DeviceIdType.MESH,
        )
    for o in (-1, 1):
        pl.semaphore_signal(
            barrier, inc=1,
            device_id={"lat": lax.rem(lat + o + lats, lats), "lon": lax.rem(me + o + n, n)},
            device_id_type=pl.DeviceIdType.MESH,
        )
    pl.semaphore_wait(barrier, n + lats)


class WeightSum:
    def __init__(self, n, lats, wg, w1, w2, wout, sems):
        self.n, self.lats = n, lats
        self.wg, self.w1, self.w2, self.wout = wg, w1, w2, wout
        self.sems = sems
        self.me, self.lat = lax.axis_index("lon"), lax.axis_index("lat")

    def remote(self, src, dst, k, device):
        return pltpu.make_async_remote_copy(
            src_ref=src, dst_ref=dst, send_sem=self.sems.at[0, k], recv_sem=self.sems.at[1, k],
            device_id=device, device_id_type=pl.DeviceIdType.MESH,
        )

    def every(self, buf, count, k):
        part = buf.at[pl.ds(0, count - 1)]
        return self.remote(part, part, k, {"lon": lax.rem(self.me + 1, self.n)})

    def start(self):
        for o in range(1, self.n):
            p = lax.rem(self.me + o, self.n)
            self.remote(self.wg.at[p], self.w1.at[self.me], 0, {"lon": p}).start()
        self.w1[pl.ds(self.me, 1)] = self.wg[pl.ds(self.me, 1)]

    def step_one(self):
        self.every(self.w1, self.n, 0).wait_recv()
        total = jnp.sum(self.w1[...].astype(F32), axis=0, keepdims=True)
        self.w2[pl.ds(self.lat, 1)] = total.astype(BF16)
        for o in range(1, self.lats):
            p = lax.rem(self.lat + o, self.lats)
            part = self.w2.at[self.lat]
            self.remote(part, part, 1, {"lat": p}).start()

    def step_two(self):
        self.every(self.w2, self.lats, 1).wait_recv()
        total = jnp.sum(self.w2[...].astype(F32), axis=0, keepdims=True)
        self.wout[pl.ds(self.me, 1)] = total.astype(BF16)
        for o in range(1, self.n):
            p = lax.rem(self.me + o, self.n)
            part = self.wout.at[self.me]
            self.remote(part, part, 2, {"lon": p}).start()

    def finish(self):
        self.every(self.wout, self.n, 2).wait_recv()
        self.every(self.w1, self.n, 0).wait_send()
        self.every(self.w2, self.lats, 1).wait_send()
        self.every(self.wout, self.n, 2).wait_send()


def flip(mains, under, right, corner):
    lane = lax.broadcasted_iota(jnp.int32, (TAIL, LANES), 1) // TAIL
    spare = jnp.zeros((LANES - HEADS * TAIL, LANES), F32)
    mains_t = [block.T for block in mains]
    right_t = jnp.concatenate(under + [spare], axis=0).T
    turned = right.T
    under_t = [turned[h * TAIL : (h + 1) * TAIL] for h in range(HEADS)]
    pad = jnp.zeros((LANES - TAIL, LANES), F32)
    turned = jnp.concatenate([corner, pad], axis=0).T
    corner_t = jnp.zeros((TAIL, LANES), F32)
    for h in range(HEADS):
        piece = turned[h * TAIL : (h + 1) * TAIL]
        if h:
            piece = pltpu.roll(piece, h * TAIL, 1)
        corner_t = jnp.where(lane == h, piece, corner_t)
    return mains_t, under_t, right_t, corner_t


def kernel(
    n,
    lats,
    kinds,
    lat_windows,
    level_windows,
    lon_windows,
    perm_ref,
    back_ref,
    x_hbm,
    c_hbm,
    wqkv_ref,
    wback_ref,
    wproj_ref,
    bias_ref,
    side_ref,
    gqkv_ref,
    gproj_ref,
    gbias_hbm,
    grad_hbm,
    q_s,
    m_s,
    qt_s,
    mt_s,
    kt_s,
    vt_s,
    p_s,
    ds_s,
    shift_s,
    mix_s,
    dqt_s,
    gqkv_s,
    gproj_s,
    gbias_s,
    pair_s,
    sum_s,
    cross_s,
    step_s,
    half_s,
    red_s,
    wg_s,
    w1_s,
    w2_s,
    w3_s,
    body_s,
    east_s,
    gl_s,
    gh_s,
    wh_s,
    nh_s,
    pair_sem,
    cross_sem,
    back_sem,
    fwd_sem,
    store_sem,
    w_sem,
    load_sem,
    east_sem,
    south_sem,
    wh_sem,
    nh_sem,
    out_sem,
):
    step = pl.program_id(0)
    a = lax.rem(step, level_windows)
    b = step // level_windows
    channels = wqkv_ref.shape[1]
    head_dim = channels // HEADS
    scale = head_dim ** -0.5
    levels = x_hbm.shape[0]
    shift = WIN_LAT // 2
    breadth = x_hbm.shape[2]
    tails = HEADS * LANES
    stack = HEADS * WTOK

    @pl.when(step == 0)
    def _():
        for ref in (gqkv_s, gproj_s, q_s, m_s, qt_s, mt_s):
            ref[...] = jnp.zeros_like(ref)
        gbias_s[:, stack + WTOK :, :] = jnp.zeros((kinds, PACKED - stack - WTOK, LANES), BF16)

    halo = Halo(
        n, lats, levels, level_windows, lat_windows,
        ((x_hbm, c_hbm), body_s, east_s, gl_s, gh_s, wh_s, nh_s, grad_hbm),
        (load_sem, east_sem, south_sem, wh_sem, nh_sem, out_sem),
    )

    @pl.when(step == 0)
    def _():
        halo.begin()
        enter(n, lats)
        halo.send(0, lat_windows == 1)

    halo.arrive(a, b)

    perm = perm_ref[...]
    bottom = b == lat_windows - 1

    def raw(which):
        flat = lambda t: t.reshape(-1, channels)
        zs = halo.pair(a)
        parts = [flat(body_s[which, z, pl.ds(shift + b * WIN_LAT, WIN_LAT)]) for z in zs]
        parts += [flat(east_s[which, z, pl.ds(b * WIN_LAT, WIN_LAT)]) for z in zs]
        return jnp.concatenate(parts, axis=0)

    x_raw, c_raw = raw(0), raw(1)
    x = mm(perm, x_raw).astype(BF16)
    c = mm(perm, c_raw).astype(BF16)
    q = (mm(x, wqkv_ref[0]) * (scale * LOG2E)).astype(BF16)
    k = mm(x, wqkv_ref[1]).astype(BF16)
    v = mm(x, wqkv_ref[2]).astype(BF16)
    m = mm(c, wproj_ref[...]).astype(BF16)

    wrap_here = a == level_windows - 1
    dead_here = bottom & (lax.axis_index("lat") == lats - 1)
    per_level = WTOK // WIN_Z

    def classes(token):
        upper = token >= per_level
        inner = jnp.where(upper, token - per_level, token)
        wrapped = jnp.where(upper & wrap_here, 2, 0)
        dead = jnp.where((inner >= per_level // 2) & dead_here, 1, 0)
        return wrapped + dead

    lane = lax.broadcasted_iota(jnp.int32, (1, LANES), 1)
    key_class = classes(lax.broadcasted_iota(jnp.int32, (WTOK, LANES), 0))
    mask_main = jnp.where(key_class == classes(lane), 0.0, -1e30)
    mask_tail = jnp.where(key_class == classes(LANES + lax.rem(lane, TAIL)), 0.0, -1e30)

    table = lambda lo, rows: bias_ref[0, lo : lo + rows, :].astype(F32) * LOG2E
    mains_t, under_t, right_t, corner_t = flip(
        [table(h * WTOK, LANES) for h in range(HEADS)],
        [table(h * WTOK + LANES, TAIL) for h in range(HEADS)],
        side_ref[0, :LANES, :].astype(F32) * LOG2E,
        side_ref[0, LANES:, :].astype(F32) * LOG2E,
    )
    for h in range(HEADS):
        cols = slice(h * LANES, (h + 1) * LANES)
        shift_s[:LANES, cols] = mains_t[h] + mask_main[:LANES]
        shift_s[LANES:, cols] = under_t[h] + mask_main[LANES:]
    shift_s[:LANES, tails:] = right_t + mask_tail[:LANES]
    shift_s[LANES:, tails:] = corner_t + mask_tail[LANES:]

    whole = lon_windows * LANES
    main = lambda w: slice(w * LANES, (w + 1) * LANES)
    tail = lambda w: slice(whole + w * TAIL, whole + (w + 1) * TAIL)
    window = lambda t, w: jnp.concatenate([t[main(w)], t[tail(w)]], axis=0)
    keys = [window(k, w) for w in range(lon_windows)]
    values = [window(v, w) for w in range(lon_windows)]
    for w in range(lon_windows):
        for flat, wide_s, turned_s in ((q, q_s, qt_s), (m, m_s, mt_s)):
            turned = flat[main(w)].T
            for h in range(HEADS):
                cs = slice(h * head_dim, (h + 1) * head_dim)
                wide_s[w, h * LANES : (h + 1) * LANES, cs] = flat[main(w), cs]
                wide_s[w, tails + h * TAIL : tails + (h + 1) * TAIL, cs] = flat[tail(w), cs]
                turned_s[w, cs, h * LANES : (h + 1) * LANES] = turned[cs]
            turned_s[w, :, tails:] = wide_s[w, tails:, :].T
        kt_s[w] = keys[w].T
        vt_s[w] = values[w].T

    tiles = HEADS + 1
    gb = []
    for j in range(0, tiles, 2):
        cols = slice(j * LANES, min(j + 2, tiles) * LANES)
        total = [None, None]
        for w in range(lon_windows):
            s2 = mm(keys[w], qt_s[w, :, cols])
            dp2 = mm(values[w], mt_s[w, :, cols])
            for i in range(min(2, tiles - j)):
                here = slice(i * LANES, (i + 1) * LANES)
                at = slice((j + i) * LANES, (j + i + 1) * LANES)
                s = s2[:, here] + shift_s[:, at]
                dp = dp2[:, here]
                e = jnp.exp2(s - jnp.max(s, axis=0, keepdims=True))
                r = 1.0 / jnp.sum(e, axis=0, keepdims=True)
                p = e * r
                delta = jnp.sum(p * dp, axis=0, keepdims=True)
                ds = p * (dp - delta)
                p_s[w, :, at] = p.astype(BF16)
                ds_s[w, :, at] = ds.astype(BF16)
                total[i] = ds if total[i] is None else total[i] + ds
        gb += total[: min(2, tiles - j)]

    tail_lane = lax.broadcasted_iota(jnp.int32, (head_dim, LANES), 1) // TAIL
    for turned_s, from_s, to_s, factor in ((vt_s, p_s, mix_s, None), (kt_s, ds_s, dqt_s, scale)):
        far = [None] * HEADS
        for w in range(lon_windows):
            for j in range(0, HEADS, 2):
                rows = slice(j * head_dim, (j + 2) * head_dim)
                out = mm(turned_s[w, rows, :], from_s[w, :, j * LANES : (j + 2) * LANES])
                if factor is not None:
                    out = out * factor
                for i in range(2):
                    cs = slice((j + i) * head_dim, (j + i + 1) * head_dim)
                    piece = out[i * head_dim : (i + 1) * head_dim, i * LANES : (i + 1) * LANES]
                    to_s[cs, main(w)] = piece.astype(BF16)
            out = mm(turned_s[w], from_s[w, :, tails:])
            if factor is not None:
                out = out * factor
            for h in range(HEADS):
                piece = out[h * head_dim : (h + 1) * head_dim]
                turn = (w - h) * TAIL % LANES
                if turn:
                    piece = pltpu.roll(piece, turn, 1)
                far[h] = jnp.where(tail_lane == w, piece, 0.0 if far[h] is None else far[h])
        for h in range(HEADS):
            cs = slice(h * head_dim, (h + 1) * head_dim)
            to_s[cs, whole:] = far[h].astype(BF16)

    dk, dv = [], []
    for w in range(lon_windows):
        dk.append((mm(ds_s[w], q_s[w]) * (1.0 / LOG2E)).astype(BF16))
        dv.append(mm(p_s[w], m_s[w]).astype(BF16))
    order = lambda ts: jnp.concatenate([t[:LANES] for t in ts] + [t[LANES:] for t in ts], axis=0)
    tokens = lon_windows * WTOK
    dq = dqt_s[...].T[:tokens]
    cols = [dq, order(dk), order(dv)]
    xt = x.T
    for i in range(3):
        gqkv_s[i] += mm(xt, cols[i])
    gproj_s[...] += mm(mix_s[:, :tokens], c)
    gin = mm(cols[0], wback_ref[0]) + mm(cols[1], wback_ref[1]) + mm(cols[2], wback_ref[2])
    gout = mm(back_ref[...], gin.astype(BF16)).astype(BF16)
    near, far = WIN_LAT * breadth, WIN_LAT * HALO
    for u, z in enumerate(halo.pair(a)):
        rows = pl.ds(shift + b * WIN_LAT, WIN_LAT)
        own = gout[u * near : (u + 1) * near]
        gl_s[z, rows] = own.reshape(WIN_LAT, breadth, channels)
        strip = gout[WIN_Z * near + u * far : WIN_Z * near + (u + 1) * far]
        gh_s[z, pl.ds(b * WIN_LAT, WIN_LAT)] = strip.reshape(WIN_LAT, HALO, channels)

    @pl.when((a == level_windows - 1) & (b < lat_windows - 1))
    def _():
        halo.back_copy(b, False).start()

    @pl.when(a == 0)
    def _():
        halo.send_next(b)

    @pl.when((a == GRAD_LAG - 1) & (b > 0))
    def _():
        halo.finish(b - 1, False)

    mains_t, under_t, right_t, corner_t = flip(
        [gb[h][:LANES] for h in range(HEADS)],
        [gb[h][LANES:] for h in range(HEADS)],
        gb[HEADS][:LANES],
        gb[HEADS][LANES:],
    )
    for h in range(HEADS):
        gbias_s[step, h * WTOK : h * WTOK + LANES, :] = mains_t[h].astype(BF16)
        gbias_s[step, h * WTOK + LANES : (h + 1) * WTOK, :] = under_t[h].astype(BF16)
    gbias_s[step, stack : stack + LANES, :] = right_t.astype(BF16)
    gbias_s[step, stack + LANES : stack + WTOK, :] = corner_t.astype(BF16)

    ex = (Square if n == 8 else Exchange)(
        n, kinds,
        (gbias_s, pair_s, sum_s, (cross_s, step_s, half_s) if n == 8 else cross_s, red_s, gbias_hbm),
        (pair_sem, cross_sem, back_sem, fwd_sem, store_sem),
    )
    ex.behind(step)
    ex.pair_copy(step).start()

    @pl.when(step == kinds - 1)
    def _():
        share = channels // n
        for i in range(n):
            rows = slice(i * share, (i + 1) * share)
            for j in range(3):
                wg_s[i, j * share : (j + 1) * share, :] = gqkv_s[j, rows].astype(BF16)
            wg_s[i, 3 * share :, :] = gproj_s[rows].astype(BF16)
        ws = WeightSum(n, lats, wg_s, w1_s, w2_s, w3_s, w_sem)
        ws.start()
        halo.give_last()
        for turn, _ in enumerate(ex.rest()):
            if turn == 1:
                ws.step_one()
            if turn == 2:
                halo.finish(lat_windows - 1, True)
                halo.finish_top()
            if turn == 3:
                ws.step_two()
        ws.finish()
        for p in range(n):
            rows = slice(p * share, (p + 1) * share)
            for j in range(3):
                cs = slice(j * channels, (j + 1) * channels)
                gqkv_ref[rows, cs] = w3_s[p, j * share : (j + 1) * share, :].astype(F32)
            gproj_ref[rows, :] = w3_s[p, 3 * share :, :].astype(F32)
        ex.drain()
        halo.end()


def pack_kernel(table_ref, main_ref, tail_ref, main_s, tail_s):
    h = pl.program_id(0)
    kinds = table_ref.shape[1]
    group = LANES // TAIL
    lane = lax.broadcasted_iota(jnp.int32, (kinds, LANES), 1)

    def body(m):
        tiles = []
        for r in range(group + 1):
            start = pl.multiple_of(m * (group * WTOK) + r * LANES, LANES)
            tiles.append(table_ref[0, :, pl.ds(start, LANES)].astype(F32))
        for r in range(group):
            turn = (LANES - TAIL * r) % LANES
            left = pltpu.roll(tiles[r], turn, 1) if r else tiles[r]
            right = pltpu.roll(tiles[r + 1], turn, 1) if r else tiles[r + 1]
            whole = jnp.where(lane < LANES - TAIL * r, left, right) if r else left
            at = pl.ds(m * group + r, kinds, stride=ODD)
            main_s[at, :] = whole
            tail_s[at, :] = right

    def several(i, _):
        for u in range(UNROLL):
            body(i * UNROLL + u)
        return 0

    lax.fori_loop(0, WTOK // group // UNROLL, several, 0)
    wide = lax.broadcasted_iota(jnp.int32, (WTOK, LANES), 1) // TAIL
    for t in range(kinds):
        at = slice(t * ODD, t * ODD + WTOK)
        main_ref[t, 0] = main_s[at, :].astype(BF16)
        turned = pltpu.roll(tail_s[at, :], h * TAIL, 1)
        before = jnp.where(h == 0, 0.0, tail_ref[t].astype(F32))
        tail_ref[t] = jnp.where(wide == h, turned, before).astype(BF16)


def pack(table):
    heads, kinds, flat = table.shape
    main, tail = pl.pallas_call(
        pack_kernel,
        grid=(heads,),
        in_specs=[pl.BlockSpec((1, kinds, flat), lambda i: (i, 0, 0))],
        out_specs=[
            pl.BlockSpec((kinds, 1, WTOK, LANES), lambda i: (0, i, 0, 0)),
            pl.BlockSpec((kinds, WTOK, LANES), lambda i: (0, 0, 0)),
        ],
        out_shape=[
            jax.ShapeDtypeStruct((kinds, heads, WTOK, LANES), BF16),
            jax.ShapeDtypeStruct((kinds, WTOK, LANES), BF16),
        ],
        scratch_shapes=[pltpu.VMEM((kinds * ODD, LANES), F32)] * 2,
        cost_estimate=pl.CostEstimate(
            flops=10_000_000_000, bytes_accessed=10_000_000, transcendentals=0
        ),
    )(table)
    return main, tail


def unpack_kernel(main_ref, tail_ref, out_ref, main_s, tail_s):
    h = pl.program_id(0)
    kinds = main_ref.shape[0]
    for t in range(kinds):
        at = slice(t * ODD, t * ODD + WTOK)
        main_s[at, :] = main_ref[t].astype(F32)
        tail_s[at, :] = pltpu.roll(tail_ref[t].astype(F32), (HEADS - h) * TAIL + LANES - HEADS * TAIL, 1)
    group = LANES // TAIL
    lane = lax.broadcasted_iota(jnp.int32, (kinds, LANES), 1)

    def body(m):
        before_main = before_tail = None
        for r in range(group + 1):
            tile = None
            if r < group:
                at = pl.ds(m * group + r, kinds, stride=ODD)
                here_main, here_tail = main_s[at, :], tail_s[at, :]
                if r:
                    here_main = pltpu.roll(here_main, TAIL * r, 1)
                    here_tail = pltpu.roll(here_tail, TAIL * r, 1)
                tile = here_main
            if r:
                ended = before_tail
                if r > 1:
                    ended = jnp.where(lane < TAIL * (r - 1), before_main, before_tail)
                tile = ended if r == group else jnp.where(lane < TAIL * r, ended, tile)
            start = pl.multiple_of(m * (group * WTOK) + r * LANES, LANES)
            out_ref[0, :, pl.ds(start, LANES)] = tile
            if r < group:
                before_main, before_tail = here_main, here_tail

    def several(i, _):
        for u in range(UNROLL):
            body(i * UNROLL + u)
        return 0

    lax.fori_loop(0, WTOK // group // UNROLL, several, 0)


def unpack(packed):
    kinds, _, lanes = packed.shape
    return pl.pallas_call(
        unpack_kernel,
        grid=(HEADS,),
        in_specs=[
            pl.BlockSpec((kinds, WTOK, lanes), lambda i: (0, i, 0)),
            pl.BlockSpec((kinds, WTOK, lanes), lambda i: (0, HEADS, 0)),
        ],
        out_specs=pl.BlockSpec((1, kinds, WTOK * WTOK), lambda i: (i, 0, 0)),
        out_shape=jax.ShapeDtypeStruct((HEADS, kinds, WTOK * WTOK), F32),
        scratch_shapes=[pltpu.VMEM((kinds * ODD, LANES), F32)] * 2,
        cost_estimate=pl.CostEstimate(
            flops=10_000_000_000, bytes_accessed=15_000_000, transcendentals=0
        ),
    )(packed, packed)


def window_call(perm, back, normed, cotangent, wqkv, wback, wproj, bias, side):
    levels, height, breadth, channels = normed.shape
    level_windows = levels // WIN_Z
    lat_windows = height // WIN_LAT
    lon_windows = perm.shape[0] // WTOK
    kinds = lat_windows * level_windows
    n, lats = lax.axis_size("lon"), lax.axis_size("lat")
    chips = n // 2
    shift = WIN_LAT // 2
    whole = lambda arr: pl.BlockSpec(arr.shape, lambda i: (0,) * arr.ndim)
    const = lambda shape: pl.BlockSpec(shape, lambda i: (0,) * len(shape))
    anywhere = pl.BlockSpec(memory_space=pl.ANY)
    stack = HEADS * WTOK
    padded = (HEADS + 1) * LANES
    turned = (lon_windows + 1) * LANES
    wgrad = (4 * channels // n, channels)
    sem = lambda *k: pltpu.SemaphoreType.DMA((2,) + k)
    dma = pltpu.SemaphoreType.DMA
    if n == 8:
        exchange_sems = [dma((6,)), dma((6, kinds)), dma((1,)), dma((1,)), dma((1,))]
    else:
        exchange_sems = [
            sem(kinds), sem(kinds, chips), sem(kinds, chips), sem(kinds), dma((kinds,))
        ]
    arriving = (2, PACKED // 8, LANES) if n == 8 else (chips, PACKED // n, LANES)
    return pl.pallas_call(
        functools.partial(kernel, n, lats, kinds, lat_windows, level_windows, lon_windows),
        grid=(kinds,),
        in_specs=[
            whole(perm),
            whole(back),
            anywhere,
            anywhere,
            whole(wqkv),
            whole(wback),
            whole(wproj),
            pl.BlockSpec((1, stack, LANES), lambda i: (i, 0, 0)),
            pl.BlockSpec((1, WTOK, LANES), lambda i: (i, 0, 0)),
        ],
        out_specs=[
            const((channels, 3 * channels)),
            const((channels, channels)),
            anywhere,
            anywhere,
        ],
        out_shape=[
            jax.ShapeDtypeStruct((channels, 3 * channels), F32),
            jax.ShapeDtypeStruct((channels, channels), F32),
            jax.ShapeDtypeStruct((kinds, PACKED, LANES), BF16),
            jax.ShapeDtypeStruct(normed.shape, BF16),
        ],
        scratch_shapes=[
            pltpu.VMEM((lon_windows, padded, channels), BF16),
            pltpu.VMEM((lon_windows, padded, channels), BF16),
            pltpu.VMEM((lon_windows, channels, padded), BF16),
            pltpu.VMEM((lon_windows, channels, padded), BF16),
            pltpu.VMEM((lon_windows, channels, WTOK), BF16),
            pltpu.VMEM((lon_windows, channels, WTOK), BF16),
            pltpu.VMEM((lon_windows, WTOK, padded), BF16),
            pltpu.VMEM((lon_windows, WTOK, padded), BF16),
            pltpu.VMEM((WTOK, padded), F32),
            pltpu.VMEM((channels, turned), BF16),
            pltpu.VMEM((channels, turned), BF16),
            pltpu.VMEM((3, channels, channels), F32),
            pltpu.VMEM((channels, channels), F32),
            pltpu.VMEM((kinds, PACKED, LANES), BF16),
            pltpu.VMEM((kinds, PACKED // 2, LANES), BF16),
            pltpu.VMEM((kinds, PACKED // 2, LANES), BF16),
            pltpu.VMEM((kinds,) + arriving, BF16),
            pltpu.VMEM((kinds, 2, PACKED // 8, LANES), BF16),
            pltpu.VMEM((kinds, 2, PACKED // 16, LANES), BF16),
            pltpu.VMEM((kinds, PACKED, LANES), BF16),
            pltpu.VMEM((n,) + wgrad, BF16),
            pltpu.VMEM((n,) + wgrad, BF16),
            pltpu.VMEM((lats,) + wgrad, BF16),
            pltpu.VMEM((n,) + wgrad, BF16),
            pltpu.VMEM((2, levels, height + shift, breadth, channels), BF16),
            pltpu.VMEM((2, levels, height, HALO, channels), BF16),
            pltpu.VMEM((levels, height + shift, breadth, channels), BF16),
            pltpu.VMEM((levels, height, HALO, channels), BF16),
            pltpu.VMEM((levels, height, HALO, channels), BF16),
            pltpu.VMEM((levels, shift, breadth, channels), BF16),
            *exchange_sems,
            sem(3),
            pltpu.SemaphoreType.DMA((2, lat_windows)),
            sem(2, lat_windows + 1, 3),
            sem(2),
            sem(lat_windows + 1),
            sem(),
            pltpu.SemaphoreType.DMA((lat_windows + 1,)),
        ],
        compiler_params=pltpu.CompilerParams(
            dimension_semantics=("arbitrary",),
            vmem_limit_bytes=56 * 2**20,
            collective_id=0,
            has_side_effects=True,
        ),
        cost_estimate=pl.CostEstimate(
            flops=kinds * 1_500_000_000, bytes_accessed=kinds * 2_000_000, transcendentals=0
        ),
    )(
        perm, back, normed, cotangent, wqkv, wback, wproj, bias, side
    )


def frame_order(breadth, lon_windows):
    rows = np.arange(lon_windows * WTOK)
    mains = lon_windows * LANES
    is_main = rows < mains
    window = np.where(is_main, rows // LANES, (rows - mains) // TAIL)
    token = np.where(is_main, rows % LANES, LANES + (rows - mains) % TAIL)
    per_level = WIN_LAT * WIN_LON
    level = token // per_level
    row = token % per_level // WIN_LON
    place = window * WIN_LON + token % WIN_LON + WIN_LON // 2
    near, far = WIN_LAT * breadth, WIN_LAT * HALO
    source = np.where(
        place < breadth,
        level * near + row * breadth + place,
        WIN_Z * near + level * far + row * HALO + place - breadth,
    )
    columns = np.arange(WIN_Z * (near + far))
    return (source[:, None] == columns[None, :]).astype(np.float32)


def local(normed, cotangent, weight_qkv, weight_proj, bias_table):
    breadth = normed.shape[2]
    lon_windows = breadth // WIN_LON
    bias, side = pack(jnp.swapaxes(bias_table, 0, 1))
    bias = bias.reshape(bias.shape[0], HEADS * WTOK, LANES)
    wqkv = jnp.stack(jnp.split(weight_qkv, 3, axis=1))
    wback = jnp.swapaxes(wqkv, 1, 2)
    wproj = weight_proj.T

    perm = frame_order(breadth, lon_windows)
    gqkv, gproj, packed, input_grad = window_call(
        jnp.asarray(perm, BF16), jnp.asarray(perm.T, BF16),
        normed, cotangent, wqkv, wback, wproj, bias, side,
    )
    bias_grad = jnp.swapaxes(unpack(packed), 0, 1)
    return input_grad, gqkv, gproj, bias_grad


def solution(mesh):
    in_specs = (
        P(None, "lat", "lon", None),
        P(None, "lat", "lon", None),
        P(),
        P(),
        P("lat", None, None),
    )
    out_specs = (P(None, "lat", "lon", None), P(), P(), P("lat", None, None))
    return jax.shard_map(local, mesh=mesh, in_specs=in_specs, out_specs=out_specs, check_vma=False)
```

```python
import functools
import math

import jax
import jax.numpy as jnp
import numpy as np
from jax import lax
from jax.experimental import pallas as pl
from jax.experimental.pallas import tpu as pltpu
from jax.sharding import PartitionSpec as P

HEADS = 6
WIN_Z = 2
WIN_LAT = 6
WIN_LON = 12
WTOK = 144
LANES = 128
TAIL = WTOK - LANES
HALO = 8
PACKED = 1024
GRAD_LAG = 2
LAGS = (1, 3, 5, 7, 9, 10)
UNROLL = 6
ODD = WTOK + 1
LOG2E = math.log2(math.e)
F32 = jnp.float32
BF16 = jnp.bfloat16


def mm(a, b, ca=1, cb=0):
    return lax.dot_general(a, b, (((ca,), (cb,)), ((), ())), preferred_element_type=F32)


class Exchange:
    def __init__(self, n, kinds, bufs, sems):
        self.n, self.kinds = n, kinds
        self.chips = n // 2
        self.gb, self.pair, self.sum, self.cross, self.out, self.hbm = bufs
        self.pair_sem, self.cross_sem, self.back_sem, self.fwd_sem, self.store_sem = sems
        me = lax.axis_index("lon")
        self.me = me
        self.core = lax.rem(me, 2)
        self.chip = me // 2
        self.other = 1 - self.core
        self.partner = self.chip * 2 + self.other
        self.half = PACKED // 2
        self.part = self.half // self.chips

    def remote(self, src, dst, send, recv, device):
        return pltpu.make_async_remote_copy(
            src_ref=src, dst_ref=dst, send_sem=send, recv_sem=recv,
            device_id={"lon": device}, device_id_type=pl.DeviceIdType.MESH,
        )

    def peer(self, o):
        return lax.rem(self.chip + o, self.chips)

    def rows(self, core, chip):
        return pl.ds(core * self.half + chip * self.part, self.part)

    def pair_copy(self, t):
        src = self.gb.at[t, pl.ds(self.other * self.half, self.half)]
        return self.remote(
            src, self.pair.at[t], self.pair_sem.at[0, t], self.pair_sem.at[1, t], self.partner
        )

    def cross_copy(self, t, o, arriving):
        j = self.peer(o)
        src = self.sum.at[t, pl.ds(j * self.part, self.part)]
        slot = j if arriving else self.chip
        return self.remote(
            src, self.cross.at[t, slot], self.cross_sem.at[0, t, j],
            self.cross_sem.at[1, t, slot], j * 2 + self.core,
        )

    def back_copy(self, t, o, arriving):
        j = self.peer(o)
        slot = j if arriving else self.chip
        part = self.out.at[t, self.rows(self.core, slot)]
        return self.remote(
            part, part, self.back_sem.at[0, t, j], self.back_sem.at[1, t, slot],
            j * 2 + self.core,
        )

    def fwd_copy(self, t, arriving):
        core = self.other if arriving else self.core
        part = self.out.at[t, pl.ds(core * self.half, self.half)]
        return self.remote(
            part, part, self.fwd_sem.at[0, t], self.fwd_sem.at[1, t], self.partner
        )

    def store(self, t):
        return pltpu.make_async_copy(self.out.at[t], self.hbm.at[t], self.store_sem.at[t])

    def stage_pair(self, t):
        self.pair_copy(t).wait_recv()
        mine = self.gb[t, pl.ds(self.core * self.half, self.half)].astype(F32)
        total = (mine + self.pair[t].astype(F32)).astype(BF16)
        self.sum[t] = total
        for o in range(1, self.chips):
            self.cross_copy(t, o, False).start()

    def stage_cross(self, t):
        for o in range(1, self.chips):
            self.cross_copy(t, o, True).wait_recv()
        acc = self.sum[t, pl.ds(self.chip * self.part, self.part)].astype(F32)
        for o in range(1, self.chips):
            acc = acc + self.cross[t, self.peer(o)].astype(F32)
        self.out[t, self.rows(self.core, self.chip)] = acc.astype(BF16)
        for o in range(1, self.chips):
            self.back_copy(t, o, False).start()

    def stage_back(self, t):
        for o in range(1, self.chips):
            self.back_copy(t, o, True).wait_recv()
        self.fwd_copy(t, False).start()

    def stage_fwd(self, t):
        self.fwd_copy(t, True).wait_recv()
        self.store(t).start()

    def stages(self):
        return [self.stage_pair, self.stage_cross, self.stage_back, self.stage_fwd]

    def behind(self, step):
        for lag, stage in zip(LAGS, self.stages()):
            t = step - lag
            if isinstance(t, int):
                if 0 <= t < self.kinds:
                    stage(t)
            else:
                pl.when(t >= 0)(functools.partial(stage, t))

    def rest(self):
        stages = self.stages()
        done = [self.kinds - lag for lag in LAGS[: len(stages)]]
        while done[-1] < self.kinds:
            limit = [self.kinds] + done[:-1]
            for k, stage in enumerate(stages):
                for t in range(done[k], min(done[k] + 2, limit[k])):
                    stage(t)
                done[k] = max(done[k], min(done[k] + 2, limit[k]))
            yield

    def drain(self):
        def body(t, _):
            self.pair_copy(t).wait_send()
            for o in range(1, self.chips):
                self.cross_copy(t, o, False).wait_send()
                self.back_copy(t, o, False).wait_send()
            self.fwd_copy(t, False).wait_send()
            self.store(t).wait()
            return 0

        lax.fori_loop(0, self.kinds, body, 0)


class Square(Exchange):
    def __init__(self, n, kinds, bufs, sems):
        pair_bufs, one, sums, two = bufs[:3] + bufs[4:], bufs[3][0], bufs[3][1], bufs[3][2]
        gb, pair, total, out, hbm = pair_bufs
        super().__init__(n, kinds, (gb, pair, total, None, out, hbm), sems)
        self.one, self.sums, self.two = one, sums, two
        bits = (lax.rem(self.chip, 2), self.chip // 2)
        flip_x = self.chip + 1 - 2 * bits[0]
        flip_y = lax.rem(self.chip + 2, self.chips)
        self.first = (flip_x * 2 + self.core, flip_y * 2 + self.core)
        self.second = self.first[::-1]
        self.bit = bits
        self.other_bit = bits[::-1]
        self.plane = self.half // 2
        self.send_sem, self.step_sem = sems[0], sems[1]

    def coarse(self, p, bit):
        return pl.ds(p * self.plane + bit * (self.plane // 2), self.plane // 2)

    def fine(self, bit):
        return pl.ds(bit * (self.plane // 4), self.plane // 4)

    def placed(self, t, p, start, rows):
        at = self.core * self.half + p * self.plane + start
        return self.out.at[t, pl.ds(at, rows)]

    def pair_copy(self, t):
        src = self.gb.at[t, pl.ds(self.other * self.half, self.half)]
        return self.remote(
            src, self.pair.at[t], self.send_sem.at[0], self.step_sem.at[0, t], self.partner
        )

    def fwd_copy(self, t, arriving):
        core = self.other if arriving else self.core
        part = self.out.at[t, pl.ds(core * self.half, self.half)]
        return self.remote(
            part, part, self.send_sem.at[5], self.step_sem.at[5, t], self.partner
        )

    def copy(self, src, dst, k, t, device):
        return self.remote(src, dst, self.send_sem.at[k], self.step_sem.at[k, t], device)

    def one_copy(self, t, p):
        src = self.sum.at[t, self.coarse(p, 1 - self.bit[p])]
        return self.copy(src, self.one.at[t, p], 1, t, self.first[p])

    def two_copy(self, t, p):
        src = self.sums.at[t, p, self.fine(1 - self.other_bit[p])]
        return self.copy(src, self.two.at[t, p], 2, t, self.second[p])

    def three_copy(self, t, p):
        start = self.bit[p] * (self.plane // 2) + self.other_bit[p] * (self.plane // 4)
        part = self.placed(t, p, start, self.plane // 4)
        return self.copy(part, part, 3, t, self.second[p])

    def four_copy(self, t, p):
        part = self.placed(t, p, self.bit[p] * (self.plane // 2), self.plane // 2)
        return self.copy(part, part, 4, t, self.first[p])

    def both(self, buf, k, t):
        return self.copy(buf.at[t], buf.at[t], k, t, self.partner)

    def stage_pair(self, t):
        self.pair_copy(t).wait_recv()
        mine = self.gb[t, pl.ds(self.core * self.half, self.half)].astype(F32)
        self.sum[t] = (mine + self.pair[t].astype(F32)).astype(BF16)
        for p in range(2):
            self.one_copy(t, p).start()

    def stage_one(self, t):
        self.both(self.one, 1, t).wait_recv()
        for p in range(2):
            mine = self.sum[t, self.coarse(p, self.bit[p])].astype(F32)
            self.sums[t, p] = (mine + self.one[t, p].astype(F32)).astype(BF16)
        for p in range(2):
            self.two_copy(t, p).start()

    def stage_two(self, t):
        self.both(self.two, 2, t).wait_recv()
        for p in range(2):
            mine = self.sums[t, p, self.fine(self.other_bit[p])].astype(F32)
            total = (mine + self.two[t, p].astype(F32)).astype(BF16)
            start = self.bit[p] * (self.plane // 2) + self.other_bit[p] * (self.plane // 4)
            at = self.core * self.half + p * self.plane + start
            self.out[t, pl.ds(at, self.plane // 4)] = total
        for p in range(2):
            self.three_copy(t, p).start()

    def stage_three(self, t):
        self.both(self.two, 3, t).wait_recv()
        for p in range(2):
            self.four_copy(t, p).start()

    def stage_four(self, t):
        self.both(self.one, 4, t).wait_recv()
        self.fwd_copy(t, False).start()

    def store(self, t):
        return pltpu.make_async_copy(self.out.at[t], self.hbm.at[t], self.store_sem.at[0])

    def stages(self):
        return [
            self.stage_pair, self.stage_one, self.stage_two, self.stage_three,
            self.stage_four, self.stage_fwd,
        ]

    def drain(self):
        for k, buf in enumerate((self.pair, self.one, self.two, self.two, self.one, self.pair)):
            self.remote(
                buf, buf, self.send_sem.at[k], self.step_sem.at[k, 0], self.partner
            ).wait_send()
        pltpu.make_async_copy(self.out, self.hbm, self.store_sem.at[0]).wait()


class Halo:
    def __init__(self, n, lats, levels, level_windows, lat_windows, refs, sems):
        self.n, self.lats = n, lats
        self.levels, self.level_windows, self.lat_windows = levels, level_windows, lat_windows
        self.given, self.body, self.east, self.gl, self.gh, self.wh, self.nh, self.out = refs
        self.load_sem, self.east_sem, self.south_sem, self.wh_sem, self.nh_sem, self.out_sem = sems
        self.me, self.lat = lax.axis_index("lon"), lax.axis_index("lat")
        self.shift = WIN_LAT // 2
        self.height = lat_windows * WIN_LAT
        self.last = lat_windows - 1
        self.last_lat = self.lat == lats - 1
        self.strip = pl.ds(0, WIN_LON // 2)
        self.parts = ((1, WIN_Z), (1 + WIN_Z, levels - 1 - WIN_Z), (0, 1))

    def remote(self, src, dst, sems, at, lat, lon, send_at=None):
        device = {"lat": self.lat + lat, "lon": lax.rem(self.me + lon + self.n, self.n)}
        send = (0,) + (at if send_at is None else send_at)
        return pltpu.make_async_remote_copy(
            src_ref=src, dst_ref=dst, send_sem=sems.at[send], recv_sem=sems.at[(1,) + at],
            device_id=device, device_id_type=pl.DeviceIdType.MESH,
        )

    def count(self, bottom):
        return self.shift if bottom else WIN_LAT

    def load(self, i, b, bottom):
        rows = pl.ds(self.shift + b * WIN_LAT, self.count(bottom))
        return pltpu.make_async_copy(
            self.given[i].at[:, rows], self.body.at[i, :, rows], self.load_sem.at[i, b]
        )

    def east_copy(self, i, part, b, bottom):
        level = pl.ds(*self.parts[part])
        src = pl.ds(self.shift + b * WIN_LAT, self.count(bottom))
        dst = pl.ds(b * WIN_LAT, self.count(bottom))
        return self.remote(
            self.given[i].at[level, src, self.strip, :], self.east.at[i, level, dst, self.strip, :],
            self.east_sem, (i, b, part), 0, -1, (i, 0, 0),
        )

    def east_all(self, i):
        rows = pl.ds(self.shift, self.height - self.shift)
        src = self.given[i].at[:, rows, self.strip, :]
        dst = self.east.at[i, :, rows, self.strip, :]
        return self.remote(src, dst, self.east_sem, (i, 0, 0), 0, -1)

    def corner_copy(self, i):
        src, dst = pl.ds(0, self.shift), pl.ds(self.height - self.shift, self.shift)
        return self.remote(
            self.given[i].at[:, src, self.strip, :], self.east.at[i, :, dst, self.strip, :],
            self.east_sem, (i, self.lat_windows, 0), -1, -1,
        )

    def south_copy(self, i):
        src = self.given[i].at[:, pl.ds(0, self.shift)]
        dst = self.body.at[i, :, pl.ds(self.height, self.shift)]
        return self.remote(src, dst, self.south_sem, (i,), -1, 0)

    def begin(self):
        for b in range(self.lat_windows):
            for i in range(2):
                self.load(i, b, b == self.last).start()
        self.east[...] = jnp.zeros_like(self.east)
        self.wh[...] = jnp.zeros_like(self.wh)

        @pl.when(self.last_lat)
        def _():
            shape = self.body.shape
            blank = jnp.zeros(shape[:2] + (self.shift,) + shape[3:], BF16)
            self.body[:, :, pl.ds(self.height, self.shift)] = blank

        @pl.when(self.lat == 0)
        def _():
            self.nh[...] = jnp.zeros_like(self.nh)

    def send(self, b, bottom):
        for part in range(3):
            for i in range(2):
                self.east_copy(i, part, b, bottom).start()
        if bottom:
            @pl.when(self.lat > 0)
            def _():
                for i in range(2):
                    self.south_copy(i).start()
                    self.corner_copy(i).start()

    def send_next(self, b):
        pl.when(b + 1 < self.last)(lambda: self.send(b + 1, False))
        pl.when(b + 1 == self.last)(lambda: self.send(self.last, True))

    def pair(self, a):
        return [lax.rem(WIN_Z * a + 1 + u, self.levels) for u in range(WIN_Z)]

    def arrive_part(self, part, b, bottom):
        for i in range(2):
            if part == 0:
                self.load(i, b, bottom).wait()
            self.east_copy(i, part, b, bottom).wait_recv()
        if bottom and part == 0:
            @pl.when(jnp.logical_not(self.last_lat))
            def _():
                for i in range(2):
                    self.corner_copy(i).wait_recv()
                    self.south_copy(i).wait_recv()

    def arrive(self, a, b):
        at = (a == 0, a == 1, a == self.level_windows - 1)
        for part in range(3):
            pl.when(at[part] & (b < self.last))(
                functools.partial(self.arrive_part, part, b, False)
            )
            pl.when(at[part] & (b == self.last))(
                functools.partial(self.arrive_part, part, self.last, True)
            )

    def back_copy(self, b, bottom):
        src = pl.ds(b * WIN_LAT, self.count(bottom))
        dst = pl.ds(self.shift + b * WIN_LAT, self.count(bottom))
        return self.remote(
            self.gh.at[:, src, self.strip, :], self.wh.at[:, dst, self.strip, :],
            self.wh_sem, (b,), 0, 1,
        )

    def back_corner(self):
        src, dst = pl.ds(self.height - self.shift, self.shift), pl.ds(0, self.shift)
        return self.remote(
            self.gh.at[:, src, self.strip, :], self.wh.at[:, dst, self.strip, :],
            self.wh_sem, (self.lat_windows,), 1, 1,
        )

    def down_copy(self):
        src = self.gl.at[:, pl.ds(self.height, self.shift)]
        return self.remote(src, self.nh, self.nh_sem, (), 1, 0)

    def give_last(self):
        @pl.when(jnp.logical_not(self.last_lat))
        def _():
            self.back_corner().start()
            self.down_copy().start()

        self.back_copy(self.last, True).start()

    def store(self, b, bottom):
        rows = pl.ds(self.shift + b * WIN_LAT, self.count(bottom))
        return pltpu.make_async_copy(
            self.gl.at[:, rows], self.out.at[:, rows], self.out_sem.at[b]
        )

    def store_top(self):
        rows = pl.ds(0, self.shift)
        return pltpu.make_async_copy(
            self.nh, self.out.at[:, rows], self.out_sem.at[self.lat_windows]
        )

    def finish(self, b, bottom):
        self.back_copy(b, bottom).wait_recv()
        rows = pl.ds(self.shift + b * WIN_LAT, self.count(bottom))
        seam = self.gl[:, rows, :HALO].astype(F32) + self.wh[:, rows].astype(F32)
        self.gl[:, rows, :HALO] = seam.astype(BF16)
        self.store(b, bottom).start()

    def finish_top(self):
        @pl.when(self.lat > 0)
        def _():
            self.back_corner().wait_recv()
            self.down_copy().wait_recv()

        seam = self.nh[:, :, :HALO].astype(F32) + self.wh[:, : self.shift].astype(F32)
        self.nh[:, :, :HALO] = seam.astype(BF16)
        self.store_top().start()

    def end(self):
        for b in range(self.lat_windows):
            bottom = b == self.last
            self.back_copy(b, bottom).wait_send()
            self.store(b, bottom).wait()
        self.store_top().wait()
        for i in range(2):
            self.east_all(i).wait_send()

        @pl.when(self.lat > 0)
        def _():
            for i in range(2):
                self.south_copy(i).wait_send()
                self.corner_copy(i).wait_send()

        @pl.when(jnp.logical_not(self.last_lat))
        def _():
            self.back_corner().wait_send()
            self.down_copy().wait_send()


def enter(n, lats):
    me, lat = lax.axis_index("lon"), lax.axis_index("lat")
    barrier = pltpu.get_barrier_semaphore()
    for o in range(1, n):
        pl.semaphore_signal(
            barrier, inc=1, device_id={"lon": lax.rem(me + o, n)},
            device_id_type=pl.DeviceIdType.MESH,
        )
    for o in range(1, lats):
        pl.semaphore_signal(
            barrier, inc=1, device_id={"lat": lax.rem(lat + o, lats)},
            device_id_type=pl.DeviceIdType.MESH,
        )
    for o in (-1, 1):
        pl.semaphore_signal(
            barrier, inc=1,
            device_id={"lat": lax.rem(lat + o + lats, lats), "lon": lax.rem(me + o + n, n)},
            device_id_type=pl.DeviceIdType.MESH,
        )
    return lambda: pl.semaphore_wait(barrier, n + lats)


class WeightSum:
    def __init__(self, n, lats, wg, w1, w2, wout, sems):
        self.n, self.lats = n, lats
        self.wg, self.w1, self.w2, self.wout = wg, w1, w2, wout
        self.sems = sems
        self.me, self.lat = lax.axis_index("lon"), lax.axis_index("lat")

    def remote(self, src, dst, k, device):
        return pltpu.make_async_remote_copy(
            src_ref=src, dst_ref=dst, send_sem=self.sems.at[0, k], recv_sem=self.sems.at[1, k],
            device_id=device, device_id_type=pl.DeviceIdType.MESH,
        )

    def every(self, buf, count, k):
        part = buf.at[pl.ds(0, count - 1)]
        return self.remote(part, part, k, {"lon": lax.rem(self.me + 1, self.n)})

    def start(self):
        for o in range(1, self.n):
            p = lax.rem(self.me + o, self.n)
            self.remote(self.wg.at[p], self.w1.at[self.me], 0, {"lon": p}).start()
        self.w1[pl.ds(self.me, 1)] = self.wg[pl.ds(self.me, 1)]

    def step_one(self):
        self.every(self.w1, self.n, 0).wait_recv()
        total = jnp.sum(self.w1[...].astype(F32), axis=0, keepdims=True)
        self.w2[pl.ds(self.lat, 1)] = total.astype(BF16)
        for o in range(1, self.lats):
            p = lax.rem(self.lat + o, self.lats)
            part = self.w2.at[self.lat]
            self.remote(part, part, 1, {"lat": p}).start()

    def step_two(self):
        self.every(self.w2, self.lats, 1).wait_recv()
        total = jnp.sum(self.w2[...].astype(F32), axis=0, keepdims=True)
        self.wout[pl.ds(self.me, 1)] = total.astype(BF16)
        for o in range(1, self.n):
            p = lax.rem(self.me + o, self.n)
            part = self.wout.at[self.me]
            self.remote(part, part, 2, {"lon": p}).start()

    def finish(self):
        self.every(self.wout, self.n, 2).wait_recv()
        self.every(self.w1, self.n, 0).wait_send()
        self.every(self.w2, self.lats, 1).wait_send()
        self.every(self.wout, self.n, 2).wait_send()


class Pack:
    def __init__(self, table, rows, sems, bias, side, main, tail):
        self.table, self.rows, self.sems = table, rows, sems
        self.bias, self.side, self.main, self.tail = bias, side, main, tail
        self.kinds = bias.shape[0]

    def load(self, h):
        return pltpu.make_async_copy(self.table.at[h], self.rows.at[h], self.sems.at[h])

    def begin(self):
        for h in range(HEADS):
            self.load(h).start()

    def head(self, h, _):
        self.load(h).wait()
        group = LANES // TAIL
        kinds = self.kinds
        lane = lax.broadcasted_iota(jnp.int32, (kinds, LANES), 1)

        def body(m):
            tiles = []
            for r in range(group + 1):
                start = pl.multiple_of(m * (group * WTOK) + r * LANES, LANES)
                tiles.append(self.rows[h, :, pl.ds(start, LANES)].astype(F32))
            for r in range(group):
                turn = (LANES - TAIL * r) % LANES
                left = pltpu.roll(tiles[r], turn, 1) if r else tiles[r]
                right = pltpu.roll(tiles[r + 1], turn, 1) if r else tiles[r + 1]
                whole = jnp.where(lane < LANES - TAIL * r, left, right) if r else left
                at = pl.ds(m * group + r, kinds, stride=ODD)
                self.main[at, :] = whole
                self.tail[at, :] = right

        def several(i, _):
            for u in range(UNROLL):
                body(i * UNROLL + u)
            return 0

        lax.fori_loop(0, WTOK // group // UNROLL, several, 0)
        wide = lax.broadcasted_iota(jnp.int32, (WTOK, LANES), 1) // TAIL
        for t in range(kinds):
            at = slice(t * ODD, t * ODD + WTOK)
            self.bias[t, pl.ds(pl.multiple_of(h * WTOK, WTOK), WTOK)] = self.main[at, :].astype(BF16)
            turned = pltpu.roll(self.tail[at, :], h * TAIL, 1)
            before = jnp.where(h == 0, 0.0, self.side[t].astype(F32))
            self.side[t] = jnp.where(wide == h, turned, before).astype(BF16)
        return 0

    def heads(self, lo, hi):
        lax.fori_loop(lo, hi, self.head, 0)


def flip(mains, under, right, corner):
    lane = lax.broadcasted_iota(jnp.int32, (TAIL, LANES), 1) // TAIL
    spare = jnp.zeros((LANES - HEADS * TAIL, LANES), F32)
    mains_t = [block.T for block in mains]
    right_t = jnp.concatenate(under + [spare], axis=0).T
    turned = right.T
    under_t = [turned[h * TAIL : (h + 1) * TAIL] for h in range(HEADS)]
    pad = jnp.zeros((LANES - TAIL, LANES), F32)
    turned = jnp.concatenate([corner, pad], axis=0).T
    corner_t = jnp.zeros((TAIL, LANES), F32)
    for h in range(HEADS):
        piece = turned[h * TAIL : (h + 1) * TAIL]
        if h:
            piece = pltpu.roll(piece, h * TAIL, 1)
        corner_t = jnp.where(lane == h, piece, corner_t)
    return mains_t, under_t, right_t, corner_t


def kernel(
    n,
    lats,
    kinds,
    lat_windows,
    level_windows,
    lon_windows,
    perm_ref,
    back_ref,
    x_hbm,
    c_hbm,
    wqkv_ref,
    wproj_ref,
    table_hbm,
    gqkv_ref,
    gproj_ref,
    gbias_hbm,
    grad_hbm,
    q_s,
    m_s,
    qt_s,
    mt_s,
    kt_s,
    vt_s,
    p_s,
    ds_s,
    shift_s,
    mix_s,
    dqt_s,
    gqkv_s,
    gproj_s,
    gbias_s,
    pair_s,
    sum_s,
    cross_s,
    step_s,
    half_s,
    red_s,
    wg_s,
    w1_s,
    w2_s,
    w3_s,
    body_s,
    east_s,
    gl_s,
    gh_s,
    wh_s,
    nh_s,
    rows_s,
    bias_s,
    side_s,
    flat_s,
    flat_tail_s,
    wqkv_s,
    wback_s,
    wproj_s,
    rows_sem,
    pair_sem,
    cross_sem,
    back_sem,
    fwd_sem,
    store_sem,
    w_sem,
    load_sem,
    east_sem,
    south_sem,
    wh_sem,
    nh_sem,
    out_sem,
):
    step = pl.program_id(0)
    a = lax.rem(step, level_windows)
    b = step // level_windows
    channels = wqkv_ref.shape[0]
    head_dim = channels // HEADS
    scale = head_dim ** -0.5
    levels = x_hbm.shape[0]
    shift = WIN_LAT // 2
    breadth = x_hbm.shape[2]
    tails = HEADS * LANES
    stack = HEADS * WTOK

    @pl.when(step == 0)
    def _():
        for ref in (gqkv_s, gproj_s, q_s, m_s, qt_s, mt_s):
            ref[...] = jnp.zeros_like(ref)
        gbias_s[:, stack + WTOK :, :] = jnp.zeros((kinds, PACKED - stack - WTOK, LANES), BF16)

    halo = Halo(
        n, lats, levels, level_windows, lat_windows,
        ((x_hbm, c_hbm), body_s, east_s, gl_s, gh_s, wh_s, nh_s, grad_hbm),
        (load_sem, east_sem, south_sem, wh_sem, nh_sem, out_sem),
    )

    @pl.when(step == 0)
    def _():
        table = Pack(table_hbm, rows_s, rows_sem, bias_s, side_s, flat_s, flat_tail_s)
        table.begin()
        halo.begin()
        entered = enter(n, lats)
        for i in range(3):
            part = wqkv_ref[:, i * channels : (i + 1) * channels]
            wqkv_s[i] = part
            wback_s[i] = part.T
        wproj_s[...] = wproj_ref[...].T
        table.heads(0, HEADS // 3)
        entered()
        halo.send(0, lat_windows == 1)
        table.heads(HEADS // 3, HEADS)

    halo.arrive(a, b)

    perm = perm_ref[...]
    bottom = b == lat_windows - 1

    def raw(which):
        flat = lambda t: t.reshape(-1, channels)
        zs = halo.pair(a)
        parts = [flat(body_s[which, z, pl.ds(shift + b * WIN_LAT, WIN_LAT)]) for z in zs]
        parts += [flat(east_s[which, z, pl.ds(b * WIN_LAT, WIN_LAT)]) for z in zs]
        return jnp.concatenate(parts, axis=0)

    x_raw, c_raw = raw(0), raw(1)
    x = mm(perm, x_raw).astype(BF16)
    c = mm(perm, c_raw).astype(BF16)
    q = (mm(x, wqkv_s[0]) * (scale * LOG2E)).astype(BF16)
    k = mm(x, wqkv_s[1]).astype(BF16)
    v = mm(x, wqkv_s[2]).astype(BF16)
    m = mm(c, wproj_s[...]).astype(BF16)

    wrap_here = a == level_windows - 1
    dead_here = bottom & (lax.axis_index("lat") == lats - 1)
    per_level = WTOK // WIN_Z

    def classes(token):
        upper = token >= per_level
        inner = jnp.where(upper, token - per_level, token)
        wrapped = jnp.where(upper & wrap_here, 2, 0)
        dead = jnp.where((inner >= per_level // 2) & dead_here, 1, 0)
        return wrapped + dead

    lane = lax.broadcasted_iota(jnp.int32, (1, LANES), 1)
    key_class = classes(lax.broadcasted_iota(jnp.int32, (WTOK, LANES), 0))
    mask_main = jnp.where(key_class == classes(lane), 0.0, -1e30)
    mask_tail = jnp.where(key_class == classes(LANES + lax.rem(lane, TAIL)), 0.0, -1e30)

    table = lambda lo, rows: bias_s[step, lo : lo + rows, :].astype(F32) * LOG2E
    mains_t, under_t, right_t, corner_t = flip(
        [table(h * WTOK, LANES) for h in range(HEADS)],
        [table(h * WTOK + LANES, TAIL) for h in range(HEADS)],
        side_s[step, :LANES, :].astype(F32) * LOG2E,
        side_s[step, LANES:, :].astype(F32) * LOG2E,
    )
    for h in range(HEADS):
        cols = slice(h * LANES, (h + 1) * LANES)
        shift_s[:LANES, cols] = mains_t[h] + mask_main[:LANES]
        shift_s[LANES:, cols] = under_t[h] + mask_main[LANES:]
    shift_s[:LANES, tails:] = right_t + mask_tail[:LANES]
    shift_s[LANES:, tails:] = corner_t + mask_tail[LANES:]

    whole = lon_windows * LANES
    main = lambda w: slice(w * LANES, (w + 1) * LANES)
    tail = lambda w: slice(whole + w * TAIL, whole + (w + 1) * TAIL)
    window = lambda t, w: jnp.concatenate([t[main(w)], t[tail(w)]], axis=0)
    keys = [window(k, w) for w in range(lon_windows)]
    values = [window(v, w) for w in range(lon_windows)]
    for w in range(lon_windows):
        for flat, wide_s, turned_s in ((q, q_s, qt_s), (m, m_s, mt_s)):
            turned = flat[main(w)].T
            for h in range(HEADS):
                cs = slice(h * head_dim, (h + 1) * head_dim)
                wide_s[w, h * LANES : (h + 1) * LANES, cs] = flat[main(w), cs]
                wide_s[w, tails + h * TAIL : tails + (h + 1) * TAIL, cs] = flat[tail(w), cs]
                turned_s[w, cs, h * LANES : (h + 1) * LANES] = turned[cs]
            turned_s[w, :, tails:] = wide_s[w, tails:, :].T
        kt_s[w] = keys[w].T
        vt_s[w] = values[w].T

    tiles = HEADS + 1
    gb = []
    for j in range(0, tiles, 2):
        cols = slice(j * LANES, min(j + 2, tiles) * LANES)
        total = [None, None]
        for w in range(lon_windows):
            s2 = mm(keys[w], qt_s[w, :, cols])
            dp2 = mm(values[w], mt_s[w, :, cols])
            for i in range(min(2, tiles - j)):
                here = slice(i * LANES, (i + 1) * LANES)
                at = slice((j + i) * LANES, (j + i + 1) * LANES)
                s = s2[:, here] + shift_s[:, at]
                dp = dp2[:, here]
                e = jnp.exp2(s - jnp.max(s, axis=0, keepdims=True))
                r = 1.0 / jnp.sum(e, axis=0, keepdims=True)
                p = e * r
                delta = jnp.sum(p * dp, axis=0, keepdims=True)
                ds = p * (dp - delta)
                p_s[w, :, at] = p.astype(BF16)
                ds_s[w, :, at] = ds.astype(BF16)
                total[i] = ds if total[i] is None else total[i] + ds
        gb += total[: min(2, tiles - j)]

    tail_lane = lax.broadcasted_iota(jnp.int32, (head_dim, LANES), 1) // TAIL
    for turned_s, from_s, to_s, factor in ((vt_s, p_s, mix_s, None), (kt_s, ds_s, dqt_s, scale)):
        far = [None] * HEADS
        for w in range(lon_windows):
            for j in range(0, HEADS, 2):
                rows = slice(j * head_dim, (j + 2) * head_dim)
                out = mm(turned_s[w, rows, :], from_s[w, :, j * LANES : (j + 2) * LANES])
                if factor is not None:
                    out = out * factor
                for i in range(2):
                    cs = slice((j + i) * head_dim, (j + i + 1) * head_dim)
                    piece = out[i * head_dim : (i + 1) * head_dim, i * LANES : (i + 1) * LANES]
                    to_s[cs, main(w)] = piece.astype(BF16)
            out = mm(turned_s[w], from_s[w, :, tails:])
            if factor is not None:
                out = out * factor
            for h in range(HEADS):
                piece = out[h * head_dim : (h + 1) * head_dim]
                turn = (w - h) * TAIL % LANES
                if turn:
                    piece = pltpu.roll(piece, turn, 1)
                far[h] = jnp.where(tail_lane == w, piece, 0.0 if far[h] is None else far[h])
        for h in range(HEADS):
            cs = slice(h * head_dim, (h + 1) * head_dim)
            to_s[cs, whole:] = far[h].astype(BF16)

    dk, dv = [], []
    for w in range(lon_windows):
        dk.append((mm(ds_s[w], q_s[w]) * (1.0 / LOG2E)).astype(BF16))
        dv.append(mm(p_s[w], m_s[w]).astype(BF16))
    order = lambda ts: jnp.concatenate([t[:LANES] for t in ts] + [t[LANES:] for t in ts], axis=0)
    tokens = lon_windows * WTOK
    dq = dqt_s[...].T[:tokens]
    cols = [dq, order(dk), order(dv)]
    xt = x.T
    for i in range(3):
        gqkv_s[i] += mm(xt, cols[i])
    gproj_s[...] += mm(mix_s[:, :tokens], c)
    gin = mm(cols[0], wback_s[0]) + mm(cols[1], wback_s[1]) + mm(cols[2], wback_s[2])
    gout = mm(back_ref[...], gin.astype(BF16)).astype(BF16)
    near, far = WIN_LAT * breadth, WIN_LAT * HALO
    for u, z in enumerate(halo.pair(a)):
        rows = pl.ds(shift + b * WIN_LAT, WIN_LAT)
        own = gout[u * near : (u + 1) * near]
        gl_s[z, rows] = own.reshape(WIN_LAT, breadth, channels)
        strip = gout[WIN_Z * near + u * far : WIN_Z * near + (u + 1) * far]
        gh_s[z, pl.ds(b * WIN_LAT, WIN_LAT)] = strip.reshape(WIN_LAT, HALO, channels)

    ws = WeightSum(n, lats, wg_s, w1_s, w2_s, w3_s, w_sem)
    share = channels // n

    @pl.when(step == kinds - 1)
    def _():
        for i in range(n):
            rows = slice(i * share, (i + 1) * share)
            for j in range(3):
                wg_s[i, j * share : (j + 1) * share, :] = gqkv_s[j, rows].astype(BF16)
            wg_s[i, 3 * share :, :] = gproj_s[rows].astype(BF16)
        ws.start()

    @pl.when((a == level_windows - 1) & (b < lat_windows - 1))
    def _():
        halo.back_copy(b, False).start()

    @pl.when(a == 0)
    def _():
        halo.send_next(b)

    @pl.when((a == GRAD_LAG - 1) & (b > 0))
    def _():
        halo.finish(b - 1, False)

    mains_t, under_t, right_t, corner_t = flip(
        [gb[h][:LANES] for h in range(HEADS)],
        [gb[h][LANES:] for h in range(HEADS)],
        gb[HEADS][:LANES],
        gb[HEADS][LANES:],
    )
    for h in range(HEADS):
        gbias_s[step, h * WTOK : h * WTOK + LANES, :] = mains_t[h].astype(BF16)
        gbias_s[step, h * WTOK + LANES : (h + 1) * WTOK, :] = under_t[h].astype(BF16)
    gbias_s[step, stack : stack + LANES, :] = right_t.astype(BF16)
    gbias_s[step, stack + LANES : stack + WTOK, :] = corner_t.astype(BF16)

    ex = (Square if n == 8 else Exchange)(
        n, kinds,
        (gbias_s, pair_s, sum_s, (cross_s, step_s, half_s) if n == 8 else cross_s, red_s, gbias_hbm),
        (pair_sem, cross_sem, back_sem, fwd_sem, store_sem),
    )
    ex.behind(step)
    ex.pair_copy(step).start()

    @pl.when(step == kinds - 1)
    def _():
        halo.give_last()
        for turn, _ in enumerate(ex.rest()):
            if turn == 1:
                ws.step_one()
            if turn == 2:
                halo.finish(lat_windows - 1, True)
                halo.finish_top()
            if turn == 3:
                ws.step_two()
        ws.finish()
        for p in range(n):
            rows = slice(p * share, (p + 1) * share)
            for j in range(3):
                cs = slice(j * channels, (j + 1) * channels)
                gqkv_ref[rows, cs] = w3_s[p, j * share : (j + 1) * share, :].astype(F32)
            gproj_ref[rows, :] = w3_s[p, 3 * share :, :].astype(F32)
        ex.drain()
        halo.end()


def unpack_kernel(main_ref, tail_ref, out_ref, main_s, tail_s):
    h = pl.program_id(0)
    kinds = main_ref.shape[0]
    for t in range(kinds):
        at = slice(t * ODD, t * ODD + WTOK)
        main_s[at, :] = main_ref[t].astype(F32)

    @pl.when(h == 0)
    def _():
        for t in range(kinds):
            tail_s[t * ODD : t * ODD + WTOK, :] = tail_ref[t].astype(F32)

    group = LANES // TAIL
    lane = lax.broadcasted_iota(jnp.int32, (kinds, LANES), 1)

    def body(m):
        before_main = before_tail = None
        for r in range(group + 1):
            tile = None
            if r < group:
                at = pl.ds(m * group + r, kinds, stride=ODD)
                here_main, here_tail = main_s[at, :], tail_s[at, :]
                if r:
                    here_main = pltpu.roll(here_main, TAIL * r, 1)
                here_tail = pltpu.roll(here_tail, lax.rem(LANES + TAIL * (r - h), LANES), 1)
                tile = here_main
            if r:
                ended = before_tail
                if r > 1:
                    ended = jnp.where(lane < TAIL * (r - 1), before_main, before_tail)
                tile = ended if r == group else jnp.where(lane < TAIL * r, ended, tile)
            start = pl.multiple_of(m * (group * WTOK) + r * LANES, LANES)
            out_ref[0, :, pl.ds(start, LANES)] = tile
            if r < group:
                before_main, before_tail = here_main, here_tail

    def several(i, _):
        for u in range(UNROLL):
            body(i * UNROLL + u)
        return 0

    lax.fori_loop(0, WTOK // group // UNROLL, several, 0)


def unpack(packed):
    kinds, _, lanes = packed.shape
    return pl.pallas_call(
        unpack_kernel,
        grid=(HEADS,),
        in_specs=[
            pl.BlockSpec((kinds, WTOK, lanes), lambda i: (0, i, 0)),
            pl.BlockSpec((kinds, WTOK, lanes), lambda i: (0, HEADS, 0)),
        ],
        out_specs=pl.BlockSpec((1, kinds, WTOK * WTOK), lambda i: (i, 0, 0)),
        out_shape=jax.ShapeDtypeStruct((HEADS, kinds, WTOK * WTOK), F32),
        scratch_shapes=[pltpu.VMEM((kinds * ODD, LANES), F32)] * 2,
        cost_estimate=pl.CostEstimate(
            flops=10_000_000_000, bytes_accessed=15_000_000, transcendentals=0
        ),
    )(packed, packed)


def window_call(perm, back, normed, cotangent, wqkv, wproj, table):
    levels, height, breadth, channels = normed.shape
    level_windows = levels // WIN_Z
    lat_windows = height // WIN_LAT
    lon_windows = perm.shape[0] // WTOK
    kinds = lat_windows * level_windows
    n, lats = lax.axis_size("lon"), lax.axis_size("lat")
    chips = n // 2
    shift = WIN_LAT // 2
    whole = lambda arr: pl.BlockSpec(arr.shape, lambda i: (0,) * arr.ndim)
    const = lambda shape: pl.BlockSpec(shape, lambda i: (0,) * len(shape))
    anywhere = pl.BlockSpec(memory_space=pl.ANY)
    stack = HEADS * WTOK
    padded = (HEADS + 1) * LANES
    turned = (lon_windows + 1) * LANES
    wgrad = (4 * channels // n, channels)
    sem = lambda *k: pltpu.SemaphoreType.DMA((2,) + k)
    dma = pltpu.SemaphoreType.DMA
    if n == 8:
        exchange_sems = [dma((6,)), dma((6, kinds)), dma((1,)), dma((1,)), dma((1,))]
    else:
        exchange_sems = [
            sem(kinds), sem(kinds, chips), sem(kinds, chips), sem(kinds), dma((kinds,))
        ]
    arriving = (2, PACKED // 8, LANES) if n == 8 else (chips, PACKED // n, LANES)
    return pl.pallas_call(
        functools.partial(kernel, n, lats, kinds, lat_windows, level_windows, lon_windows),
        grid=(kinds,),
        in_specs=[
            whole(perm),
            whole(back),
            anywhere,
            anywhere,
            whole(wqkv),
            whole(wproj),
            anywhere,
        ],
        out_specs=[
            const((channels, 3 * channels)),
            const((channels, channels)),
            anywhere,
            anywhere,
        ],
        out_shape=[
            jax.ShapeDtypeStruct((channels, 3 * channels), F32),
            jax.ShapeDtypeStruct((channels, channels), F32),
            jax.ShapeDtypeStruct((kinds, PACKED, LANES), BF16),
            jax.ShapeDtypeStruct(normed.shape, BF16),
        ],
        scratch_shapes=[
            pltpu.VMEM((lon_windows, padded, channels), BF16),
            pltpu.VMEM((lon_windows, padded, channels), BF16),
            pltpu.VMEM((lon_windows, channels, padded), BF16),
            pltpu.VMEM((lon_windows, channels, padded), BF16),
            pltpu.VMEM((lon_windows, channels, WTOK), BF16),
            pltpu.VMEM((lon_windows, channels, WTOK), BF16),
            pltpu.VMEM((lon_windows, WTOK, padded), BF16),
            pltpu.VMEM((lon_windows, WTOK, padded), BF16),
            pltpu.VMEM((WTOK, padded), F32),
            pltpu.VMEM((channels, turned), BF16),
            pltpu.VMEM((channels, turned), BF16),
            pltpu.VMEM((3, channels, channels), F32),
            pltpu.VMEM((channels, channels), F32),
            pltpu.VMEM((kinds, PACKED, LANES), BF16),
            pltpu.VMEM((kinds, PACKED // 2, LANES), BF16),
            pltpu.VMEM((kinds, PACKED // 2, LANES), BF16),
            pltpu.VMEM((kinds,) + arriving, BF16),
            pltpu.VMEM((kinds, 2, PACKED // 8, LANES), BF16),
            pltpu.VMEM((kinds, 2, PACKED // 16, LANES), BF16),
            pltpu.VMEM((kinds, PACKED, LANES), BF16),
            pltpu.VMEM((n,) + wgrad, BF16),
            pltpu.VMEM((n,) + wgrad, BF16),
            pltpu.VMEM((lats,) + wgrad, BF16),
            pltpu.VMEM((n,) + wgrad, BF16),
            pltpu.VMEM((2, levels, height + shift, breadth, channels), BF16),
            pltpu.VMEM((2, levels, height, HALO, channels), BF16),
            pltpu.VMEM((levels, height + shift, breadth, channels), BF16),
            pltpu.VMEM((levels, height, HALO, channels), BF16),
            pltpu.VMEM((levels, height, HALO, channels), BF16),
            pltpu.VMEM((levels, shift, breadth, channels), BF16),
            pltpu.VMEM(table.shape, BF16),
            pltpu.VMEM((kinds, stack, LANES), BF16),
            pltpu.VMEM((kinds, WTOK, LANES), BF16),
            pltpu.VMEM((kinds * ODD, LANES), F32),
            pltpu.VMEM((kinds * ODD, LANES), F32),
            pltpu.VMEM((3, channels, channels), BF16),
            pltpu.VMEM((3, channels, channels), BF16),
            pltpu.VMEM((channels, channels), BF16),
            dma((HEADS,)),
            *exchange_sems,
            sem(3),
            pltpu.SemaphoreType.DMA((2, lat_windows)),
            sem(2, lat_windows + 1, 3),
            sem(2),
            sem(lat_windows + 1),
            sem(),
            pltpu.SemaphoreType.DMA((lat_windows + 1,)),
        ],
        compiler_params=pltpu.CompilerParams(
            dimension_semantics=("arbitrary",),
            vmem_limit_bytes=62 * 2**20,
            collective_id=0,
            has_side_effects=True,
        ),
        cost_estimate=pl.CostEstimate(
            flops=kinds * 1_500_000_000, bytes_accessed=kinds * 2_000_000, transcendentals=0
        ),
    )(
        perm, back, normed, cotangent, wqkv, wproj, table
    )


def frame_order(breadth, lon_windows):
    rows = np.arange(lon_windows * WTOK)
    mains = lon_windows * LANES
    is_main = rows < mains
    window = np.where(is_main, rows // LANES, (rows - mains) // TAIL)
    token = np.where(is_main, rows % LANES, LANES + (rows - mains) % TAIL)
    per_level = WIN_LAT * WIN_LON
    level = token // per_level
    row = token % per_level // WIN_LON
    place = window * WIN_LON + token % WIN_LON + WIN_LON // 2
    near, far = WIN_LAT * breadth, WIN_LAT * HALO
    source = np.where(
        place < breadth,
        level * near + row * breadth + place,
        WIN_Z * near + level * far + row * HALO + place - breadth,
    )
    columns = np.arange(WIN_Z * (near + far))
    return (source[:, None] == columns[None, :]).astype(np.float32)


def local(normed, cotangent, weight_qkv, weight_proj, bias_table):
    breadth = normed.shape[2]
    lon_windows = breadth // WIN_LON
    perm = frame_order(breadth, lon_windows)
    gqkv, gproj, packed, input_grad = window_call(
        jnp.asarray(perm, BF16), jnp.asarray(perm.T, BF16),
        normed, cotangent, weight_qkv, weight_proj, jnp.swapaxes(bias_table, 0, 1),
    )
    bias_grad = jnp.swapaxes(unpack(packed), 0, 1)
    return input_grad, gqkv, gproj, bias_grad


def solution(mesh):
    in_specs = (
        P(None, "lat", "lon", None),
        P(None, "lat", "lon", None),
        P(),
        P(),
        P("lat", None, None),
    )
    out_specs = (P(None, "lat", "lon", None), P(), P(), P("lat", None, None))
    return jax.shard_map(local, mesh=mesh, in_specs=in_specs, out_specs=out_specs, check_vma=False)
```

```python
import functools
import math

import jax
import jax.numpy as jnp
import numpy as np
from jax import lax
from jax.experimental import pallas as pl
from jax.experimental.pallas import tpu as pltpu
from jax.sharding import PartitionSpec as P

HEADS = 6
WIN_Z = 2
WIN_LAT = 6
WIN_LON = 12
WTOK = 144
LANES = 128
TAIL = WTOK - LANES
HALO = 8
PACKED = 1024
GRAD_LAG = 2
LAGS = (1, 3, 5, 7, 9, 10)
UNROLL = 9
ODD = WTOK + 1
LOG2E = math.log2(math.e)
F32 = jnp.float32
BF16 = jnp.bfloat16


def mm(a, b, ca=1, cb=0):
    return lax.dot_general(a, b, (((ca,), (cb,)), ((), ())), preferred_element_type=F32)


class Exchange:
    def __init__(self, n, kinds, bufs, sems):
        self.n, self.kinds = n, kinds
        self.chips = n // 2
        self.gb, self.pair, self.sum, self.cross, self.out, self.hbm = bufs
        self.pair_sem, self.cross_sem, self.back_sem, self.fwd_sem, self.store_sem = sems
        me = lax.axis_index("lon")
        self.me = me
        self.core = lax.rem(me, 2)
        self.chip = me // 2
        self.other = 1 - self.core
        self.partner = self.chip * 2 + self.other
        self.half = PACKED // 2
        self.part = self.half // self.chips

    def remote(self, src, dst, send, recv, device):
        return pltpu.make_async_remote_copy(
            src_ref=src, dst_ref=dst, send_sem=send, recv_sem=recv,
            device_id={"lon": device}, device_id_type=pl.DeviceIdType.MESH,
        )

    def peer(self, o):
        return lax.rem(self.chip + o, self.chips)

    def rows(self, core, chip):
        return pl.ds(core * self.half + chip * self.part, self.part)

    def pair_copy(self, t):
        src = self.gb.at[t, pl.ds(self.other * self.half, self.half)]
        return self.remote(
            src, self.pair.at[t], self.pair_sem.at[0, t], self.pair_sem.at[1, t], self.partner
        )

    def cross_copy(self, t, o, arriving):
        j = self.peer(o)
        src = self.sum.at[t, pl.ds(j * self.part, self.part)]
        slot = j if arriving else self.chip
        return self.remote(
            src, self.cross.at[t, slot], self.cross_sem.at[0, t, j],
            self.cross_sem.at[1, t, slot], j * 2 + self.core,
        )

    def back_copy(self, t, o, arriving):
        j = self.peer(o)
        slot = j if arriving else self.chip
        part = self.out.at[t, self.rows(self.core, slot)]
        return self.remote(
            part, part, self.back_sem.at[0, t, j], self.back_sem.at[1, t, slot],
            j * 2 + self.core,
        )

    def fwd_copy(self, t, arriving):
        core = self.other if arriving else self.core
        part = self.out.at[t, pl.ds(core * self.half, self.half)]
        return self.remote(
            part, part, self.fwd_sem.at[0, t], self.fwd_sem.at[1, t], self.partner
        )

    def store(self, t):
        return pltpu.make_async_copy(self.out.at[t], self.hbm.at[t], self.store_sem.at[t])

    def stage_pair(self, t):
        self.pair_copy(t).wait_recv()
        mine = self.gb[t, pl.ds(self.core * self.half, self.half)].astype(F32)
        total = (mine + self.pair[t].astype(F32)).astype(BF16)
        self.sum[t] = total
        for o in range(1, self.chips):
            self.cross_copy(t, o, False).start()

    def stage_cross(self, t):
        for o in range(1, self.chips):
            self.cross_copy(t, o, True).wait_recv()
        acc = self.sum[t, pl.ds(self.chip * self.part, self.part)].astype(F32)
        for o in range(1, self.chips):
            acc = acc + self.cross[t, self.peer(o)].astype(F32)
        self.out[t, self.rows(self.core, self.chip)] = acc.astype(BF16)
        for o in range(1, self.chips):
            self.back_copy(t, o, False).start()

    def stage_back(self, t):
        for o in range(1, self.chips):
            self.back_copy(t, o, True).wait_recv()
        self.fwd_copy(t, False).start()

    def stage_fwd(self, t):
        self.fwd_copy(t, True).wait_recv()
        self.store(t).start()

    def stages(self):
        return [self.stage_pair, self.stage_cross, self.stage_back, self.stage_fwd]

    def behind(self, step):
        for lag, stage in reversed(list(zip(LAGS, self.stages()))):
            t = step - lag
            if isinstance(t, int):
                if 0 <= t < self.kinds:
                    stage(t)
            else:
                pl.when(t >= 0)(functools.partial(stage, t))

    def rest(self):
        stages = self.stages()
        done = [self.kinds - lag for lag in LAGS[: len(stages)]]
        while done[-1] < self.kinds:
            limit = [self.kinds] + done[:-1]
            for k, stage in enumerate(stages):
                for t in range(done[k], min(done[k] + 2, limit[k])):
                    stage(t)
                done[k] = max(done[k], min(done[k] + 2, limit[k]))
            yield

    def drain(self):
        def body(t, _):
            self.pair_copy(t).wait_send()
            for o in range(1, self.chips):
                self.cross_copy(t, o, False).wait_send()
                self.back_copy(t, o, False).wait_send()
            self.fwd_copy(t, False).wait_send()
            self.store(t).wait()
            return 0

        lax.fori_loop(0, self.kinds, body, 0)


class Square(Exchange):
    def __init__(self, n, kinds, bufs, sems):
        pair_bufs, one, sums, two = bufs[:3] + bufs[4:], bufs[3][0], bufs[3][1], bufs[3][2]
        gb, pair, total, out, hbm = pair_bufs
        super().__init__(n, kinds, (gb, pair, total, None, out, hbm), sems)
        self.one, self.sums, self.two = one, sums, two
        bits = (lax.rem(self.chip, 2), self.chip // 2)
        flip_x = self.chip + 1 - 2 * bits[0]
        flip_y = lax.rem(self.chip + 2, self.chips)
        self.first = (flip_x * 2 + self.core, flip_y * 2 + self.core)
        self.second = self.first[::-1]
        self.bit = bits
        self.other_bit = bits[::-1]
        self.plane = self.half // 2
        self.send_sem, self.step_sem = sems[0], sems[1]

    def coarse(self, p, bit):
        return pl.ds(p * self.plane + bit * (self.plane // 2), self.plane // 2)

    def fine(self, bit):
        return pl.ds(bit * (self.plane // 4), self.plane // 4)

    def placed(self, t, p, start, rows):
        at = self.core * self.half + p * self.plane + start
        return self.out.at[t, pl.ds(at, rows)]

    def pair_copy(self, t):
        src = self.gb.at[t, pl.ds(self.other * self.half, self.half)]
        return self.remote(
            src, self.pair.at[t], self.send_sem.at[0], self.step_sem.at[0, t], self.partner
        )

    def fwd_copy(self, t, arriving):
        core = self.other if arriving else self.core
        part = self.out.at[t, pl.ds(core * self.half, self.half)]
        return self.remote(
            part, part, self.send_sem.at[5], self.step_sem.at[5, t], self.partner
        )

    def copy(self, src, dst, k, t, device):
        return self.remote(src, dst, self.send_sem.at[k], self.step_sem.at[k, t], device)

    def one_copy(self, t, p):
        src = self.sum.at[t, self.coarse(p, 1 - self.bit[p])]
        return self.copy(src, self.one.at[t, p], 1, t, self.first[p])

    def two_copy(self, t, p):
        src = self.sums.at[t, p, self.fine(1 - self.other_bit[p])]
        return self.copy(src, self.two.at[t, p], 2, t, self.second[p])

    def three_copy(self, t, p):
        start = self.bit[p] * (self.plane // 2) + self.other_bit[p] * (self.plane // 4)
        part = self.placed(t, p, start, self.plane // 4)
        return self.copy(part, part, 3, t, self.second[p])

    def four_copy(self, t, p):
        part = self.placed(t, p, self.bit[p] * (self.plane // 2), self.plane // 2)
        return self.copy(part, part, 4, t, self.first[p])

    def both(self, buf, k, t):
        return self.copy(buf.at[t], buf.at[t], k, t, self.partner)

    def stage_pair(self, t):
        self.pair_copy(t).wait_recv()
        mine = self.gb[t, pl.ds(self.core * self.half, self.half)].astype(F32)
        self.sum[t] = (mine + self.pair[t].astype(F32)).astype(BF16)
        for p in range(2):
            self.one_copy(t, p).start()

    def stage_one(self, t):
        self.both(self.one, 1, t).wait_recv()
        for p in range(2):
            mine = self.sum[t, self.coarse(p, self.bit[p])].astype(F32)
            self.sums[t, p] = (mine + self.one[t, p].astype(F32)).astype(BF16)
        for p in range(2):
            self.two_copy(t, p).start()

    def stage_two(self, t):
        self.both(self.two, 2, t).wait_recv()
        for p in range(2):
            mine = self.sums[t, p, self.fine(self.other_bit[p])].astype(F32)
            total = (mine + self.two[t, p].astype(F32)).astype(BF16)
            start = self.bit[p] * (self.plane // 2) + self.other_bit[p] * (self.plane // 4)
            at = self.core * self.half + p * self.plane + start
            self.out[t, pl.ds(at, self.plane // 4)] = total
        for p in range(2):
            self.three_copy(t, p).start()

    def stage_three(self, t):
        self.both(self.two, 3, t).wait_recv()
        for p in range(2):
            self.four_copy(t, p).start()

    def stage_four(self, t):
        self.both(self.one, 4, t).wait_recv()
        self.fwd_copy(t, False).start()

    def store(self, t):
        return pltpu.make_async_copy(self.out.at[t], self.hbm.at[t], self.store_sem.at[0])

    def stages(self):
        return [
            self.stage_pair, self.stage_one, self.stage_two, self.stage_three,
            self.stage_four, self.stage_fwd,
        ]

    def drain(self):
        for k, buf in enumerate((self.pair, self.one, self.two, self.two, self.one, self.pair)):
            self.remote(
                buf, buf, self.send_sem.at[k], self.step_sem.at[k, 0], self.partner
            ).wait_send()
        pltpu.make_async_copy(self.out, self.hbm, self.store_sem.at[0]).wait()


class Halo:
    def __init__(self, n, lats, levels, level_windows, lat_windows, refs, sems):
        self.n, self.lats = n, lats
        self.levels, self.level_windows, self.lat_windows = levels, level_windows, lat_windows
        self.given, self.body, self.east, self.gl, self.gh, self.wh, self.nh, self.out = refs
        self.load_sem, self.east_sem, self.south_sem, self.wh_sem, self.nh_sem, self.out_sem = sems
        self.me, self.lat = lax.axis_index("lon"), lax.axis_index("lat")
        self.shift = WIN_LAT // 2
        self.height = lat_windows * WIN_LAT
        self.last = lat_windows - 1
        self.last_lat = self.lat == lats - 1
        self.strip = pl.ds(0, WIN_LON // 2)
        self.parts = ((1, WIN_Z), (1 + WIN_Z, levels - 1 - WIN_Z), (0, 1))

    def remote(self, src, dst, sems, at, lat, lon, send_at=None):
        device = {"lat": self.lat + lat, "lon": lax.rem(self.me + lon + self.n, self.n)}
        send = (0,) + (at if send_at is None else send_at)
        return pltpu.make_async_remote_copy(
            src_ref=src, dst_ref=dst, send_sem=sems.at[send], recv_sem=sems.at[(1,) + at],
            device_id=device, device_id_type=pl.DeviceIdType.MESH,
        )

    def count(self, bottom):
        return self.shift if bottom else WIN_LAT

    def load(self, i, b, bottom):
        rows = pl.ds(self.shift + b * WIN_LAT, self.count(bottom))
        return pltpu.make_async_copy(
            self.given[i].at[:, rows], self.body.at[i, :, rows], self.load_sem.at[i, b]
        )

    def east_copy(self, i, part, b, bottom):
        level = pl.ds(*self.parts[part])
        src = pl.ds(self.shift + b * WIN_LAT, self.count(bottom))
        dst = pl.ds(b * WIN_LAT, self.count(bottom))
        return self.remote(
            self.given[i].at[level, src, self.strip, :], self.east.at[i, level, dst, self.strip, :],
            self.east_sem, (i, b, part), 0, -1, (i, 0, 0),
        )

    def east_all(self, i):
        rows = pl.ds(self.shift, self.height - self.shift)
        src = self.given[i].at[:, rows, self.strip, :]
        dst = self.east.at[i, :, rows, self.strip, :]
        return self.remote(src, dst, self.east_sem, (i, 0, 0), 0, -1)

    def corner_copy(self, i):
        src, dst = pl.ds(0, self.shift), pl.ds(self.height - self.shift, self.shift)
        return self.remote(
            self.given[i].at[:, src, self.strip, :], self.east.at[i, :, dst, self.strip, :],
            self.east_sem, (i, self.lat_windows, 0), -1, -1,
        )

    def south_copy(self, i):
        src = self.given[i].at[:, pl.ds(0, self.shift)]
        dst = self.body.at[i, :, pl.ds(self.height, self.shift)]
        return self.remote(src, dst, self.south_sem, (i,), -1, 0)

    def begin(self):
        for b in range(self.lat_windows):
            for i in range(2):
                self.load(i, b, b == self.last).start()
        self.east[...] = jnp.zeros_like(self.east)
        self.wh[...] = jnp.zeros_like(self.wh)

        @pl.when(self.last_lat)
        def _():
            shape = self.body.shape
            blank = jnp.zeros(shape[:2] + (self.shift,) + shape[3:], BF16)
            self.body[:, :, pl.ds(self.height, self.shift)] = blank

        @pl.when(self.lat == 0)
        def _():
            self.nh[...] = jnp.zeros_like(self.nh)

    def send(self, b, bottom):
        for part in range(3):
            for i in range(2):
                self.east_copy(i, part, b, bottom).start()
        if bottom:
            @pl.when(self.lat > 0)
            def _():
                for i in range(2):
                    self.south_copy(i).start()
                    self.corner_copy(i).start()

    def send_next(self, b):
        pl.when(b + 1 < self.last)(lambda: self.send(b + 1, False))
        pl.when(b + 1 == self.last)(lambda: self.send(self.last, True))

    def pair(self, a):
        return [lax.rem(WIN_Z * a + 1 + u, self.levels) for u in range(WIN_Z)]

    def arrive_part(self, part, b, bottom):
        for i in range(2):
            if part == 0:
                self.load(i, b, bottom).wait()
            self.east_copy(i, part, b, bottom).wait_recv()
        if bottom and part == 0:
            @pl.when(jnp.logical_not(self.last_lat))
            def _():
                for i in range(2):
                    self.corner_copy(i).wait_recv()
                    self.south_copy(i).wait_recv()

    def arrive(self, a, b):
        at = (a == 0, a == 1, a == self.level_windows - 1)
        for part in range(3):
            pl.when(at[part] & (b < self.last))(
                functools.partial(self.arrive_part, part, b, False)
            )
            pl.when(at[part] & (b == self.last))(
                functools.partial(self.arrive_part, part, self.last, True)
            )

    def back_copy(self, b, bottom):
        src = pl.ds(b * WIN_LAT, self.count(bottom))
        dst = pl.ds(self.shift + b * WIN_LAT, self.count(bottom))
        return self.remote(
            self.gh.at[:, src, self.strip, :], self.wh.at[:, dst, self.strip, :],
            self.wh_sem, (b,), 0, 1,
        )

    def back_corner(self):
        src, dst = pl.ds(self.height - self.shift, self.shift), pl.ds(0, self.shift)
        return self.remote(
            self.gh.at[:, src, self.strip, :], self.wh.at[:, dst, self.strip, :],
            self.wh_sem, (self.lat_windows,), 1, 1,
        )

    def down_copy(self):
        src = self.gl.at[:, pl.ds(self.height, self.shift)]
        return self.remote(src, self.nh, self.nh_sem, (), 1, 0)

    def give_last(self):
        @pl.when(jnp.logical_not(self.last_lat))
        def _():
            self.back_corner().start()
            self.down_copy().start()

        self.back_copy(self.last, True).start()

    def store(self, b, bottom):
        rows = pl.ds(self.shift + b * WIN_LAT, self.count(bottom))
        return pltpu.make_async_copy(
            self.gl.at[:, rows], self.out.at[:, rows], self.out_sem.at[b]
        )

    def store_top(self):
        rows = pl.ds(0, self.shift)
        return pltpu.make_async_copy(
            self.nh, self.out.at[:, rows], self.out_sem.at[self.lat_windows]
        )

    def finish(self, b, bottom):
        self.back_copy(b, bottom).wait_recv()
        rows = pl.ds(self.shift + b * WIN_LAT, self.count(bottom))
        seam = self.gl[:, rows, :HALO].astype(F32) + self.wh[:, rows].astype(F32)
        self.gl[:, rows, :HALO] = seam.astype(BF16)
        self.store(b, bottom).start()

    def finish_top(self):
        @pl.when(self.lat > 0)
        def _():
            self.back_corner().wait_recv()
            self.down_copy().wait_recv()

        seam = self.nh[:, :, :HALO].astype(F32) + self.wh[:, : self.shift].astype(F32)
        self.nh[:, :, :HALO] = seam.astype(BF16)
        self.store_top().start()

    def end(self):
        for b in range(self.lat_windows):
            bottom = b == self.last
            self.back_copy(b, bottom).wait_send()
            self.store(b, bottom).wait()
        self.store_top().wait()
        for i in range(2):
            self.east_all(i).wait_send()

        @pl.when(self.lat > 0)
        def _():
            for i in range(2):
                self.south_copy(i).wait_send()
                self.corner_copy(i).wait_send()

        @pl.when(jnp.logical_not(self.last_lat))
        def _():
            self.back_corner().wait_send()
            self.down_copy().wait_send()


def enter(n, lats):
    me, lat = lax.axis_index("lon"), lax.axis_index("lat")
    barrier = pltpu.get_barrier_semaphore()
    for o in range(1, n):
        pl.semaphore_signal(
            barrier, inc=1, device_id={"lon": lax.rem(me + o, n)},
            device_id_type=pl.DeviceIdType.MESH,
        )
    for o in range(1, lats):
        pl.semaphore_signal(
            barrier, inc=1, device_id={"lat": lax.rem(lat + o, lats)},
            device_id_type=pl.DeviceIdType.MESH,
        )
    for o in (-1, 1):
        pl.semaphore_signal(
            barrier, inc=1,
            device_id={"lat": lax.rem(lat + o + lats, lats), "lon": lax.rem(me + o + n, n)},
            device_id_type=pl.DeviceIdType.MESH,
        )
    return lambda: pl.semaphore_wait(barrier, n + lats)


class WeightSum:
    def __init__(self, n, lats, wg, wp, wc, w1, w2, wout, sems):
        self.n, self.lats, self.chips = n, lats, n // 2
        self.wg, self.wp, self.wc = wg, wp, wc
        self.w1, self.w2, self.wout = w1, w2, wout
        self.sems = sems
        me, self.lat = lax.axis_index("lon"), lax.axis_index("lat")
        self.core, self.chip = lax.rem(me, 2), me // 2
        self.partner = me + 1 - 2 * self.core
        self.mine = pl.ds(self.core * self.chips, self.chips)
        self.theirs = pl.ds((1 - self.core) * self.chips, self.chips)

    def remote(self, src, dst, k, device):
        return pltpu.make_async_remote_copy(
            src_ref=src, dst_ref=dst, send_sem=self.sems.at[0, k], recv_sem=self.sems.at[1, k],
            device_id=device, device_id_type=pl.DeviceIdType.MESH,
        )

    def every(self, buf, count, k):
        part = buf.at[pl.ds(0, count)]
        return self.remote(part, part, k, {"lon": self.partner})

    def peers(self):
        return [lax.rem(self.chip + o, self.chips) for o in range(1, self.chips)]

    def start(self):
        self.remote(self.wg.at[self.theirs], self.wp, 0, {"lon": self.partner}).start()

    def step_zero(self):
        self.every(self.wp, self.chips, 0).wait_recv()
        total = self.wg[self.mine].astype(F32) + self.wp[...].astype(F32)
        self.wc[...] = total.astype(BF16)
        self.w1[pl.ds(self.chip, 1)] = self.wc[pl.ds(self.chip, 1)]
        for j in self.peers():
            device = {"lon": j * 2 + self.core}
            self.remote(self.wc.at[j], self.w1.at[self.chip], 1, device).start()

    def step_one(self):
        self.every(self.w1, self.chips - 1, 1).wait_recv()
        total = jnp.sum(self.w1[...].astype(F32), axis=0, keepdims=True)
        self.w2[pl.ds(self.lat, 1)] = total.astype(BF16)
        for o in range(1, self.lats):
            p = lax.rem(self.lat + o, self.lats)
            part = self.w2.at[self.lat]
            self.remote(part, part, 2, {"lat": p}).start()

    def step_two(self):
        self.every(self.w2, self.lats - 1, 2).wait_recv()
        total = jnp.sum(self.w2[...].astype(F32), axis=0, keepdims=True)
        at = self.core * self.chips + self.chip
        self.wout[pl.ds(at, 1)] = total.astype(BF16)
        for j in self.peers():
            part = self.wout.at[at]
            self.remote(part, part, 3, {"lon": j * 2 + self.core}).start()

    def step_three(self):
        self.every(self.w1, self.chips - 1, 3).wait_recv()
        part = self.wout.at[self.mine]
        self.remote(part, part, 4, {"lon": self.partner}).start()

    def finish(self):
        self.every(self.wp, self.chips, 4).wait_recv()
        self.every(self.wp, self.chips, 0).wait_send()
        self.every(self.w1, self.chips - 1, 1).wait_send()
        self.every(self.w2, self.lats - 1, 2).wait_send()
        self.every(self.w1, self.chips - 1, 3).wait_send()
        self.every(self.wp, self.chips, 4).wait_send()


class Pack:
    def __init__(self, table, rows, sems, bias, side, main, tail):
        self.table, self.rows, self.sems = table, rows, sems
        self.bias, self.side, self.main, self.tail = bias, side, main, tail
        self.kinds = bias.shape[0]

    def load(self, h):
        return pltpu.make_async_copy(self.table.at[h], self.rows.at[h], self.sems.at[h])

    def begin(self):
        for h in range(HEADS):
            self.load(h).start()

    def head(self, h, _):
        self.load(h).wait()
        group = LANES // TAIL
        kinds = self.kinds
        lane = lax.broadcasted_iota(jnp.int32, (kinds, LANES), 1)

        def body(m):
            tiles = []
            for r in range(group + 1):
                start = pl.multiple_of(m * (group * WTOK) + r * LANES, LANES)
                tiles.append(self.rows[h, :, pl.ds(start, LANES)].astype(F32))
            for r in range(group):
                turn = (LANES - TAIL * r) % LANES
                left = pltpu.roll(tiles[r], turn, 1) if r else tiles[r]
                right = pltpu.roll(tiles[r + 1], turn, 1) if r else tiles[r + 1]
                whole = jnp.where(lane < LANES - TAIL * r, left, right) if r else left
                at = pl.ds(m * group + r, kinds, stride=ODD)
                self.main[at, :] = whole
                self.tail[at, :] = right

        def several(i, _):
            for u in range(UNROLL):
                body(i * UNROLL + u)
            return 0

        lax.fori_loop(0, WTOK // group // UNROLL, several, 0)
        wide = lax.broadcasted_iota(jnp.int32, (WTOK, LANES), 1) // TAIL
        for t in range(kinds):
            at = slice(t * ODD, t * ODD + WTOK)
            self.bias[t, pl.ds(pl.multiple_of(h * WTOK, WTOK), WTOK)] = self.main[at, :].astype(BF16)
            turned = pltpu.roll(self.tail[at, :], h * TAIL, 1)
            before = jnp.where(h == 0, 0.0, self.side[t].astype(F32))
            self.side[t] = jnp.where(wide == h, turned, before).astype(BF16)
        return 0

    def heads(self, lo, hi):
        lax.fori_loop(lo, hi, self.head, 0)


def flip(mains, under, right, corner):
    lane = lax.broadcasted_iota(jnp.int32, (TAIL, LANES), 1) // TAIL
    spare = jnp.zeros((LANES - HEADS * TAIL, LANES), F32)
    mains_t = [block.T for block in mains]
    right_t = jnp.concatenate(under + [spare], axis=0).T
    turned = right.T
    under_t = [turned[h * TAIL : (h + 1) * TAIL] for h in range(HEADS)]
    pad = jnp.zeros((LANES - TAIL, LANES), F32)
    turned = jnp.concatenate([corner, pad], axis=0).T
    corner_t = jnp.zeros((TAIL, LANES), F32)
    for h in range(HEADS):
        piece = turned[h * TAIL : (h + 1) * TAIL]
        if h:
            piece = pltpu.roll(piece, h * TAIL, 1)
        corner_t = jnp.where(lane == h, piece, corner_t)
    return mains_t, under_t, right_t, corner_t


def kernel(
    n,
    lats,
    kinds,
    lat_windows,
    level_windows,
    lon_windows,
    perm_ref,
    back_ref,
    x_hbm,
    c_hbm,
    wqkv_ref,
    wproj_ref,
    table_hbm,
    gqkv_ref,
    gproj_ref,
    gbias_hbm,
    grad_hbm,
    q_s,
    m_s,
    qt_s,
    mt_s,
    kt_s,
    vt_s,
    p_s,
    ds_s,
    shift_s,
    mix_s,
    dqt_s,
    gqkv_s,
    gproj_s,
    gbias_s,
    pair_s,
    sum_s,
    cross_s,
    step_s,
    half_s,
    red_s,
    wg_s,
    wp_s,
    wc_s,
    w1_s,
    w2_s,
    w3_s,
    body_s,
    east_s,
    gl_s,
    gh_s,
    wh_s,
    nh_s,
    rows_s,
    bias_s,
    side_s,
    flat_s,
    flat_tail_s,
    wqkv_s,
    wback_s,
    wproj_s,
    rows_sem,
    pair_sem,
    cross_sem,
    back_sem,
    fwd_sem,
    store_sem,
    w_sem,
    load_sem,
    east_sem,
    south_sem,
    wh_sem,
    nh_sem,
    out_sem,
):
    step = pl.program_id(0)
    a = lax.rem(step, level_windows)
    b = step // level_windows
    channels = wqkv_ref.shape[0]
    head_dim = channels // HEADS
    scale = head_dim ** -0.5
    levels = x_hbm.shape[0]
    shift = WIN_LAT // 2
    breadth = x_hbm.shape[2]
    tails = HEADS * LANES
    stack = HEADS * WTOK

    @pl.when(step == 0)
    def _():
        for ref in (gqkv_s, gproj_s, q_s, m_s, qt_s, mt_s):
            ref[...] = jnp.zeros_like(ref)
        gbias_s[:, stack + WTOK :, :] = jnp.zeros((kinds, PACKED - stack - WTOK, LANES), BF16)

    halo = Halo(
        n, lats, levels, level_windows, lat_windows,
        ((x_hbm, c_hbm), body_s, east_s, gl_s, gh_s, wh_s, nh_s, grad_hbm),
        (load_sem, east_sem, south_sem, wh_sem, nh_sem, out_sem),
    )

    @pl.when(step == 0)
    def _():
        table = Pack(table_hbm, rows_s, rows_sem, bias_s, side_s, flat_s, flat_tail_s)
        table.begin()
        halo.begin()
        entered = enter(n, lats)
        for i in range(3):
            part = wqkv_ref[:, i * channels : (i + 1) * channels]
            wqkv_s[i] = part
            wback_s[i] = part.T
        wproj_s[...] = wproj_ref[...].T
        table.heads(0, HEADS // 3)
        entered()
        halo.send(0, lat_windows == 1)
        table.heads(HEADS // 3, HEADS)

    halo.arrive(a, b)

    perm = perm_ref[...]
    bottom = b == lat_windows - 1

    def raw(which):
        flat = lambda t: t.reshape(-1, channels)
        zs = halo.pair(a)
        parts = [flat(body_s[which, z, pl.ds(shift + b * WIN_LAT, WIN_LAT)]) for z in zs]
        parts += [flat(east_s[which, z, pl.ds(b * WIN_LAT, WIN_LAT)]) for z in zs]
        return jnp.concatenate(parts, axis=0)

    x_raw, c_raw = raw(0), raw(1)
    x = mm(perm, x_raw).astype(BF16)
    c = mm(perm, c_raw).astype(BF16)
    q = (mm(x, wqkv_s[0]) * (scale * LOG2E)).astype(BF16)
    k = mm(x, wqkv_s[1]).astype(BF16)
    v = mm(x, wqkv_s[2]).astype(BF16)
    m = mm(c, wproj_s[...]).astype(BF16)

    wrap_here = a == level_windows - 1
    dead_here = bottom & (lax.axis_index("lat") == lats - 1)
    per_level = WTOK // WIN_Z

    def classes(token):
        upper = token >= per_level
        inner = jnp.where(upper, token - per_level, token)
        wrapped = jnp.where(upper & wrap_here, 2, 0)
        dead = jnp.where((inner >= per_level // 2) & dead_here, 1, 0)
        return wrapped + dead

    lane = lax.broadcasted_iota(jnp.int32, (1, LANES), 1)
    key_class = classes(lax.broadcasted_iota(jnp.int32, (WTOK, LANES), 0))
    mask_main = jnp.where(key_class == classes(lane), 0.0, -1e30)
    mask_tail = jnp.where(key_class == classes(LANES + lax.rem(lane, TAIL)), 0.0, -1e30)

    table = lambda lo, rows: bias_s[step, lo : lo + rows, :].astype(F32) * LOG2E
    mains_t, under_t, right_t, corner_t = flip(
        [table(h * WTOK, LANES) for h in range(HEADS)],
        [table(h * WTOK + LANES, TAIL) for h in range(HEADS)],
        side_s[step, :LANES, :].astype(F32) * LOG2E,
        side_s[step, LANES:, :].astype(F32) * LOG2E,
    )
    for h in range(HEADS):
        cols = slice(h * LANES, (h + 1) * LANES)
        shift_s[:LANES, cols] = mains_t[h] + mask_main[:LANES]
        shift_s[LANES:, cols] = under_t[h] + mask_main[LANES:]
    shift_s[:LANES, tails:] = right_t + mask_tail[:LANES]
    shift_s[LANES:, tails:] = corner_t + mask_tail[LANES:]

    whole = lon_windows * LANES
    main = lambda w: slice(w * LANES, (w + 1) * LANES)
    tail = lambda w: slice(whole + w * TAIL, whole + (w + 1) * TAIL)
    window = lambda t, w: jnp.concatenate([t[main(w)], t[tail(w)]], axis=0)
    keys = [window(k, w) for w in range(lon_windows)]
    values = [window(v, w) for w in range(lon_windows)]
    for w in range(lon_windows):
        for flat, wide_s, turned_s in ((q, q_s, qt_s), (m, m_s, mt_s)):
            turned = flat[main(w)].T
            for h in range(HEADS):
                cs = slice(h * head_dim, (h + 1) * head_dim)
                wide_s[w, h * LANES : (h + 1) * LANES, cs] = flat[main(w), cs]
                wide_s[w, tails + h * TAIL : tails + (h + 1) * TAIL, cs] = flat[tail(w), cs]
                turned_s[w, cs, h * LANES : (h + 1) * LANES] = turned[cs]
            turned_s[w, :, tails:] = wide_s[w, tails:, :].T
        kt_s[w] = keys[w].T
        vt_s[w] = values[w].T

    tiles = HEADS + 1
    gb = []
    for j in range(0, tiles, 2):
        cols = slice(j * LANES, min(j + 2, tiles) * LANES)
        total = [None, None]
        for w in range(lon_windows):
            s2 = mm(keys[w], qt_s[w, :, cols])
            dp2 = mm(values[w], mt_s[w, :, cols])
            for i in range(min(2, tiles - j)):
                here = slice(i * LANES, (i + 1) * LANES)
                at = slice((j + i) * LANES, (j + i + 1) * LANES)
                s = s2[:, here] + shift_s[:, at]
                dp = dp2[:, here]
                e = jnp.exp2(s - jnp.max(s, axis=0, keepdims=True))
                r = 1.0 / jnp.sum(e, axis=0, keepdims=True)
                p = e * r
                delta = jnp.sum(p * dp, axis=0, keepdims=True)
                ds = p * (dp - delta)
                p_s[w, :, at] = p.astype(BF16)
                ds_s[w, :, at] = ds.astype(BF16)
                total[i] = ds if total[i] is None else total[i] + ds
        gb += total[: min(2, tiles - j)]

    tail_lane = lax.broadcasted_iota(jnp.int32, (head_dim, LANES), 1) // TAIL
    for turned_s, from_s, to_s, factor in ((vt_s, p_s, mix_s, None), (kt_s, ds_s, dqt_s, scale)):
        far = [None] * HEADS
        for w in range(lon_windows):
            for j in range(0, HEADS, 2):
                rows = slice(j * head_dim, (j + 2) * head_dim)
                out = mm(turned_s[w, rows, :], from_s[w, :, j * LANES : (j + 2) * LANES])
                if factor is not None:
                    out = out * factor
                for i in range(2):
                    cs = slice((j + i) * head_dim, (j + i + 1) * head_dim)
                    piece = out[i * head_dim : (i + 1) * head_dim, i * LANES : (i + 1) * LANES]
                    to_s[cs, main(w)] = piece.astype(BF16)
            out = mm(turned_s[w], from_s[w, :, tails:])
            if factor is not None:
                out = out * factor
            for h in range(HEADS):
                piece = out[h * head_dim : (h + 1) * head_dim]
                turn = (w - h) * TAIL % LANES
                if turn:
                    piece = pltpu.roll(piece, turn, 1)
                far[h] = jnp.where(tail_lane == w, piece, 0.0 if far[h] is None else far[h])
        for h in range(HEADS):
            cs = slice(h * head_dim, (h + 1) * head_dim)
            to_s[cs, whole:] = far[h].astype(BF16)

    dk, dv = [], []
    for w in range(lon_windows):
        dk.append((mm(ds_s[w], q_s[w]) * (1.0 / LOG2E)).astype(BF16))
        dv.append(mm(p_s[w], m_s[w]).astype(BF16))
    order = lambda ts: jnp.concatenate([t[:LANES] for t in ts] + [t[LANES:] for t in ts], axis=0)
    tokens = lon_windows * WTOK
    dq = dqt_s[...].T[:tokens]
    cols = [dq, order(dk), order(dv)]
    xt = x.T
    for i in range(3):
        gqkv_s[i] += mm(xt, cols[i])
    gproj_s[...] += mm(mix_s[:, :tokens], c)
    gin = mm(cols[0], wback_s[0]) + mm(cols[1], wback_s[1]) + mm(cols[2], wback_s[2])
    gout = mm(back_ref[...], gin.astype(BF16)).astype(BF16)
    near, far = WIN_LAT * breadth, WIN_LAT * HALO
    for u, z in enumerate(halo.pair(a)):
        rows = pl.ds(shift + b * WIN_LAT, WIN_LAT)
        own = gout[u * near : (u + 1) * near]
        gl_s[z, rows] = own.reshape(WIN_LAT, breadth, channels)
        strip = gout[WIN_Z * near + u * far : WIN_Z * near + (u + 1) * far]
        gh_s[z, pl.ds(b * WIN_LAT, WIN_LAT)] = strip.reshape(WIN_LAT, HALO, channels)

    ws = WeightSum(n, lats, wg_s, wp_s, wc_s, w1_s, w2_s, w3_s, w_sem)
    share = channels // n

    @pl.when(step == kinds - 1)
    def _():
        for i in range(n):
            rows = slice(i * share, (i + 1) * share)
            for j in range(3):
                wg_s[i, j * share : (j + 1) * share, :] = gqkv_s[j, rows].astype(BF16)
            wg_s[i, 3 * share :, :] = gproj_s[rows].astype(BF16)
        ws.start()

    @pl.when((a == level_windows - 1) & (b < lat_windows - 1))
    def _():
        halo.back_copy(b, False).start()

    @pl.when(a == 0)
    def _():
        halo.send_next(b)

    @pl.when((a == GRAD_LAG - 1) & (b > 0))
    def _():
        halo.finish(b - 1, False)

    mains_t, under_t, right_t, corner_t = flip(
        [gb[h][:LANES] for h in range(HEADS)],
        [gb[h][LANES:] for h in range(HEADS)],
        gb[HEADS][:LANES],
        gb[HEADS][LANES:],
    )
    for h in range(HEADS):
        gbias_s[step, h * WTOK : h * WTOK + LANES, :] = mains_t[h].astype(BF16)
        gbias_s[step, h * WTOK + LANES : (h + 1) * WTOK, :] = under_t[h].astype(BF16)
    gbias_s[step, stack : stack + LANES, :] = right_t.astype(BF16)
    gbias_s[step, stack + LANES : stack + WTOK, :] = corner_t.astype(BF16)

    ex = (Square if n == 8 else Exchange)(
        n, kinds,
        (gbias_s, pair_s, sum_s, (cross_s, step_s, half_s) if n == 8 else cross_s, red_s, gbias_hbm),
        (pair_sem, cross_sem, back_sem, fwd_sem, store_sem),
    )
    ex.behind(step)
    ex.pair_copy(step).start()

    @pl.when(step == kinds - 1)
    def _():
        halo.give_last()
        ws.step_zero()
        for turn, _ in enumerate(ex.rest()):
            if turn == 0:
                ws.step_one()
            if turn == 2:
                ws.step_two()
                halo.finish(lat_windows - 1, True)
                halo.finish_top()
            if turn == 3:
                ws.step_three()
        ws.finish()
        for p in range(n):
            rows = slice(p * share, (p + 1) * share)
            for j in range(3):
                cs = slice(j * channels, (j + 1) * channels)
                gqkv_ref[rows, cs] = w3_s[p, j * share : (j + 1) * share, :].astype(F32)
            gproj_ref[rows, :] = w3_s[p, 3 * share :, :].astype(F32)
        ex.drain()
        halo.end()


def unpack_kernel(main_ref, tail_ref, out_ref, main_s, tail_s):
    h = pl.program_id(0)
    kinds = main_ref.shape[0]
    for t in range(kinds):
        at = slice(t * ODD, t * ODD + WTOK)
        main_s[at, :] = main_ref[t].astype(F32)

    @pl.when(h == 0)
    def _():
        for t in range(kinds):
            tail_s[t * ODD : t * ODD + WTOK, :] = tail_ref[t].astype(F32)

    group = LANES // TAIL
    lane = lax.broadcasted_iota(jnp.int32, (kinds, LANES), 1)

    def body(m):
        before_main = before_tail = None
        for r in range(group + 1):
            tile = None
            if r < group:
                at = pl.ds(m * group + r, kinds, stride=ODD)
                here_main, here_tail = main_s[at, :], tail_s[at, :]
                if r:
                    here_main = pltpu.roll(here_main, TAIL * r, 1)
                here_tail = pltpu.roll(here_tail, lax.rem(LANES + TAIL * (r - h), LANES), 1)
                tile = here_main
            if r:
                ended = before_tail
                if r > 1:
                    ended = jnp.where(lane < TAIL * (r - 1), before_main, before_tail)
                tile = ended if r == group else jnp.where(lane < TAIL * r, ended, tile)
            start = pl.multiple_of(m * (group * WTOK) + r * LANES, LANES)
            out_ref[0, :, pl.ds(start, LANES)] = tile
            if r < group:
                before_main, before_tail = here_main, here_tail

    def several(i, _):
        for u in range(UNROLL):
            body(i * UNROLL + u)
        return 0

    lax.fori_loop(0, WTOK // group // UNROLL, several, 0)


def unpack(packed):
    kinds, _, lanes = packed.shape
    return pl.pallas_call(
        unpack_kernel,
        grid=(HEADS,),
        in_specs=[
            pl.BlockSpec((kinds, WTOK, lanes), lambda i: (0, i, 0)),
            pl.BlockSpec((kinds, WTOK, lanes), lambda i: (0, HEADS, 0)),
        ],
        out_specs=pl.BlockSpec((1, kinds, WTOK * WTOK), lambda i: (i, 0, 0)),
        out_shape=jax.ShapeDtypeStruct((HEADS, kinds, WTOK * WTOK), F32),
        scratch_shapes=[pltpu.VMEM((kinds * ODD, LANES), F32)] * 2,
        cost_estimate=pl.CostEstimate(
            flops=10_000_000_000, bytes_accessed=15_000_000, transcendentals=0
        ),
    )(packed, packed)


def window_call(perm, back, normed, cotangent, wqkv, wproj, table):
    levels, height, breadth, channels = normed.shape
    level_windows = levels // WIN_Z
    lat_windows = height // WIN_LAT
    lon_windows = perm.shape[0] // WTOK
    kinds = lat_windows * level_windows
    n, lats = lax.axis_size("lon"), lax.axis_size("lat")
    chips = n // 2
    shift = WIN_LAT // 2
    whole = lambda arr: pl.BlockSpec(arr.shape, lambda i: (0,) * arr.ndim)
    const = lambda shape: pl.BlockSpec(shape, lambda i: (0,) * len(shape))
    anywhere = pl.BlockSpec(memory_space=pl.ANY)
    stack = HEADS * WTOK
    padded = (HEADS + 1) * LANES
    turned = (lon_windows + 1) * LANES
    wgrad = (4 * channels // n, channels)
    sem = lambda *k: pltpu.SemaphoreType.DMA((2,) + k)
    dma = pltpu.SemaphoreType.DMA
    if n == 8:
        exchange_sems = [dma((6,)), dma((6, kinds)), dma((1,)), dma((1,)), dma((1,))]
    else:
        exchange_sems = [
            sem(kinds), sem(kinds, chips), sem(kinds, chips), sem(kinds), dma((kinds,))
        ]
    arriving = (2, PACKED // 8, LANES) if n == 8 else (chips, PACKED // n, LANES)
    return pl.pallas_call(
        functools.partial(kernel, n, lats, kinds, lat_windows, level_windows, lon_windows),
        grid=(kinds,),
        in_specs=[
            whole(perm),
            whole(back),
            anywhere,
            anywhere,
            whole(wqkv),
            whole(wproj),
            anywhere,
        ],
        out_specs=[
            const((channels, 3 * channels)),
            const((channels, channels)),
            anywhere,
            anywhere,
        ],
        out_shape=[
            jax.ShapeDtypeStruct((channels, 3 * channels), F32),
            jax.ShapeDtypeStruct((channels, channels), F32),
            jax.ShapeDtypeStruct((kinds, PACKED, LANES), BF16),
            jax.ShapeDtypeStruct(normed.shape, BF16),
        ],
        scratch_shapes=[
            pltpu.VMEM((lon_windows, padded, channels), BF16),
            pltpu.VMEM((lon_windows, padded, channels), BF16),
            pltpu.VMEM((lon_windows, channels, padded), BF16),
            pltpu.VMEM((lon_windows, channels, padded), BF16),
            pltpu.VMEM((lon_windows, channels, WTOK), BF16),
            pltpu.VMEM((lon_windows, channels, WTOK), BF16),
            pltpu.VMEM((lon_windows, WTOK, padded), BF16),
            pltpu.VMEM((lon_windows, WTOK, padded), BF16),
            pltpu.VMEM((WTOK, padded), F32),
            pltpu.VMEM((channels, turned), BF16),
            pltpu.VMEM((channels, turned), BF16),
            pltpu.VMEM((3, channels, channels), F32),
            pltpu.VMEM((channels, channels), F32),
            pltpu.VMEM((kinds, PACKED, LANES), BF16),
            pltpu.VMEM((kinds, PACKED // 2, LANES), BF16),
            pltpu.VMEM((kinds, PACKED // 2, LANES), BF16),
            pltpu.VMEM((kinds,) + arriving, BF16),
            pltpu.VMEM((kinds, 2, PACKED // 8, LANES), BF16),
            pltpu.VMEM((kinds, 2, PACKED // 16, LANES), BF16),
            pltpu.VMEM((kinds, PACKED, LANES), BF16),
            pltpu.VMEM((n,) + wgrad, BF16),
            pltpu.VMEM((chips,) + wgrad, BF16),
            pltpu.VMEM((chips,) + wgrad, BF16),
            pltpu.VMEM((chips,) + wgrad, BF16),
            pltpu.VMEM((lats,) + wgrad, BF16),
            pltpu.VMEM((n,) + wgrad, BF16),
            pltpu.VMEM((2, levels, height + shift, breadth, channels), BF16),
            pltpu.VMEM((2, levels, height, HALO, channels), BF16),
            pltpu.VMEM((levels, height + shift, breadth, channels), BF16),
            pltpu.VMEM((levels, height, HALO, channels), BF16),
            pltpu.VMEM((levels, height, HALO, channels), BF16),
            pltpu.VMEM((levels, shift, breadth, channels), BF16),
            pltpu.VMEM(table.shape, BF16),
            pltpu.VMEM((kinds, stack, LANES), BF16),
            pltpu.VMEM((kinds, WTOK, LANES), BF16),
            pltpu.VMEM((kinds * ODD, LANES), F32),
            pltpu.VMEM((kinds * ODD, LANES), F32),
            pltpu.VMEM((3, channels, channels), BF16),
            pltpu.VMEM((3, channels, channels), BF16),
            pltpu.VMEM((channels, channels), BF16),
            dma((HEADS,)),
            *exchange_sems,
            sem(5),
            pltpu.SemaphoreType.DMA((2, lat_windows)),
            sem(2, lat_windows + 1, 3),
            sem(2),
            sem(lat_windows + 1),
            sem(),
            pltpu.SemaphoreType.DMA((lat_windows + 1,)),
        ],
        compiler_params=pltpu.CompilerParams(
            dimension_semantics=("arbitrary",),
            vmem_limit_bytes=62 * 2**20,
            collective_id=0,
            has_side_effects=True,
        ),
        cost_estimate=pl.CostEstimate(
            flops=kinds * 1_500_000_000, bytes_accessed=kinds * 2_000_000, transcendentals=0
        ),
    )(
        perm, back, normed, cotangent, wqkv, wproj, table
    )


def frame_order(breadth, lon_windows):
    rows = np.arange(lon_windows * WTOK)
    mains = lon_windows * LANES
    is_main = rows < mains
    window = np.where(is_main, rows // LANES, (rows - mains) // TAIL)
    token = np.where(is_main, rows % LANES, LANES + (rows - mains) % TAIL)
    per_level = WIN_LAT * WIN_LON
    level = token // per_level
    row = token % per_level // WIN_LON
    place = window * WIN_LON + token % WIN_LON + WIN_LON // 2
    near, far = WIN_LAT * breadth, WIN_LAT * HALO
    source = np.where(
        place < breadth,
        level * near + row * breadth + place,
        WIN_Z * near + level * far + row * HALO + place - breadth,
    )
    columns = np.arange(WIN_Z * (near + far))
    return (source[:, None] == columns[None, :]).astype(np.float32)


def local(normed, cotangent, weight_qkv, weight_proj, bias_table):
    breadth = normed.shape[2]
    lon_windows = breadth // WIN_LON
    perm = frame_order(breadth, lon_windows)
    gqkv, gproj, packed, input_grad = window_call(
        jnp.asarray(perm, BF16), jnp.asarray(perm.T, BF16),
        normed, cotangent, weight_qkv, weight_proj, jnp.swapaxes(bias_table, 0, 1),
    )
    bias_grad = jnp.swapaxes(unpack(packed), 0, 1)
    return input_grad, gqkv, gproj, bias_grad


def solution(mesh):
    in_specs = (
        P(None, "lat", "lon", None),
        P(None, "lat", "lon", None),
        P(),
        P(),
        P("lat", None, None),
    )
    out_specs = (P(None, "lat", "lon", None), P(), P(), P("lat", None, None))
    return jax.shard_map(local, mesh=mesh, in_specs=in_specs, out_specs=out_specs, check_vma=False)
```

```python
import functools
import math

import jax
import jax.numpy as jnp
import numpy as np
from jax import lax
from jax.experimental import pallas as pl
from jax.experimental.pallas import tpu as pltpu
from jax.sharding import PartitionSpec as P

HEADS = 6
WIN_Z = 2
WIN_LAT = 6
WIN_LON = 12
WTOK = 144
LANES = 128
TAIL = WTOK - LANES
HALO = 8
PACKED = 1024
GRAD_LAG = 2
LAGS = (1, 3, 5, 7, 9, 10)
UNROLL = 9
ODD = WTOK + 1
LOG2E = math.log2(math.e)
F32 = jnp.float32
BF16 = jnp.bfloat16


def mm(a, b, ca=1, cb=0):
    return lax.dot_general(a, b, (((ca,), (cb,)), ((), ())), preferred_element_type=F32)


class Exchange:
    def __init__(self, n, kinds, bufs, sems):
        self.n, self.kinds = n, kinds
        self.chips = n // 2
        self.gb, self.pair, self.sum, self.cross, self.out, self.hbm = bufs
        self.pair_sem, self.cross_sem, self.back_sem, self.fwd_sem, self.store_sem = sems
        me = lax.axis_index("lon")
        self.me = me
        self.core = lax.rem(me, 2)
        self.chip = me // 2
        self.other = 1 - self.core
        self.partner = self.chip * 2 + self.other
        self.half = PACKED // 2
        self.part = self.half // self.chips

    def remote(self, src, dst, send, recv, device):
        return pltpu.make_async_remote_copy(
            src_ref=src, dst_ref=dst, send_sem=send, recv_sem=recv,
            device_id={"lon": device}, device_id_type=pl.DeviceIdType.MESH,
        )

    def peer(self, o):
        return lax.rem(self.chip + o, self.chips)

    def rows(self, core, chip):
        return pl.ds(core * self.half + chip * self.part, self.part)

    def pair_copy(self, t):
        src = self.gb.at[t, pl.ds(self.other * self.half, self.half)]
        return self.remote(
            src, self.pair.at[t], self.pair_sem.at[0, t], self.pair_sem.at[1, t], self.partner
        )

    def cross_copy(self, t, o, arriving):
        j = self.peer(o)
        src = self.sum.at[t, pl.ds(j * self.part, self.part)]
        slot = j if arriving else self.chip
        return self.remote(
            src, self.cross.at[t, slot], self.cross_sem.at[0, t, j],
            self.cross_sem.at[1, t, slot], j * 2 + self.core,
        )

    def back_copy(self, t, o, arriving):
        j = self.peer(o)
        slot = j if arriving else self.chip
        part = self.out.at[t, self.rows(self.core, slot)]
        return self.remote(
            part, part, self.back_sem.at[0, t, j], self.back_sem.at[1, t, slot],
            j * 2 + self.core,
        )

    def fwd_copy(self, t, arriving):
        core = self.other if arriving else self.core
        part = self.out.at[t, pl.ds(core * self.half, self.half)]
        return self.remote(
            part, part, self.fwd_sem.at[0, t], self.fwd_sem.at[1, t], self.partner
        )

    def store(self, t):
        return pltpu.make_async_copy(self.out.at[t], self.hbm.at[t], self.store_sem.at[t])

    def stage_pair(self, t):
        self.pair_copy(t).wait_recv()
        mine = self.gb[t, pl.ds(self.core * self.half, self.half)].astype(F32)
        total = (mine + self.pair[t].astype(F32)).astype(BF16)
        self.sum[t] = total
        for o in range(1, self.chips):
            self.cross_copy(t, o, False).start()

    def stage_cross(self, t):
        for o in range(1, self.chips):
            self.cross_copy(t, o, True).wait_recv()
        acc = self.sum[t, pl.ds(self.chip * self.part, self.part)].astype(F32)
        for o in range(1, self.chips):
            acc = acc + self.cross[t, self.peer(o)].astype(F32)
        self.out[t, self.rows(self.core, self.chip)] = acc.astype(BF16)
        for o in range(1, self.chips):
            self.back_copy(t, o, False).start()

    def stage_back(self, t):
        for o in range(1, self.chips):
            self.back_copy(t, o, True).wait_recv()
        self.fwd_copy(t, False).start()

    def stage_fwd(self, t):
        self.fwd_copy(t, True).wait_recv()
        self.store(t).start()

    def stages(self):
        return [self.stage_pair, self.stage_cross, self.stage_back, self.stage_fwd]

    def behind(self, step):
        for lag, stage in reversed(list(zip(LAGS, self.stages()))):
            t = step - lag
            if isinstance(t, int):
                if 0 <= t < self.kinds:
                    stage(t)
            else:
                pl.when(t >= 0)(functools.partial(stage, t))

    def rest(self):
        stages = self.stages()
        done = [self.kinds - lag for lag in LAGS[: len(stages)]]
        while done[-1] < self.kinds:
            limit = [self.kinds] + done[:-1]
            for k, stage in enumerate(stages):
                for t in range(done[k], min(done[k] + 2, limit[k])):
                    stage(t)
                done[k] = max(done[k], min(done[k] + 2, limit[k]))
            yield

    def drain(self):
        def body(t, _):
            self.pair_copy(t).wait_send()
            for o in range(1, self.chips):
                self.cross_copy(t, o, False).wait_send()
                self.back_copy(t, o, False).wait_send()
            self.fwd_copy(t, False).wait_send()
            self.store(t).wait()
            return 0

        lax.fori_loop(0, self.kinds, body, 0)


class Square(Exchange):
    def __init__(self, n, kinds, bufs, sems):
        pair_bufs, one, sums, two = bufs[:3] + bufs[4:], bufs[3][0], bufs[3][1], bufs[3][2]
        gb, pair, total, out, hbm = pair_bufs
        super().__init__(n, kinds, (gb, pair, total, None, out, hbm), sems)
        self.one, self.sums, self.two = one, sums, two
        bits = (lax.rem(self.chip, 2), self.chip // 2)
        flip_x = self.chip + 1 - 2 * bits[0]
        flip_y = lax.rem(self.chip + 2, self.chips)
        self.first = (flip_x * 2 + self.core, flip_y * 2 + self.core)
        self.second = self.first[::-1]
        self.bit = bits
        self.other_bit = bits[::-1]
        self.plane = self.half // 2
        self.send_sem, self.step_sem = sems[0], sems[1]

    def coarse(self, p, bit):
        return pl.ds(p * self.plane + bit * (self.plane // 2), self.plane // 2)

    def fine(self, bit):
        return pl.ds(bit * (self.plane // 4), self.plane // 4)

    def placed(self, t, p, start, rows):
        at = self.core * self.half + p * self.plane + start
        return self.out.at[t, pl.ds(at, rows)]

    def pair_copy(self, t):
        src = self.gb.at[t, pl.ds(self.other * self.half, self.half)]
        return self.remote(
            src, self.pair.at[t], self.send_sem.at[0], self.step_sem.at[0, t], self.partner
        )

    def fwd_copy(self, t, arriving):
        core = self.other if arriving else self.core
        part = self.out.at[t, pl.ds(core * self.half, self.half)]
        return self.remote(
            part, part, self.send_sem.at[5], self.step_sem.at[5, t], self.partner
        )

    def copy(self, src, dst, k, t, device):
        return self.remote(src, dst, self.send_sem.at[k], self.step_sem.at[k, t], device)

    def one_copy(self, t, p):
        src = self.sum.at[t, self.coarse(p, 1 - self.bit[p])]
        return self.copy(src, self.one.at[t, p], 1, t, self.first[p])

    def two_copy(self, t, p):
        src = self.sums.at[t, p, self.fine(1 - self.other_bit[p])]
        return self.copy(src, self.two.at[t, p], 2, t, self.second[p])

    def three_copy(self, t, p):
        start = self.bit[p] * (self.plane // 2) + self.other_bit[p] * (self.plane // 4)
        part = self.placed(t, p, start, self.plane // 4)
        return self.copy(part, part, 3, t, self.second[p])

    def four_copy(self, t, p):
        part = self.placed(t, p, self.bit[p] * (self.plane // 2), self.plane // 2)
        return self.copy(part, part, 4, t, self.first[p])

    def both(self, buf, k, t):
        return self.copy(buf.at[t], buf.at[t], k, t, self.partner)

    def stage_pair(self, t):
        self.pair_copy(t).wait_recv()
        mine = self.gb[t, pl.ds(self.core * self.half, self.half)].astype(F32)
        self.sum[t] = (mine + self.pair[t].astype(F32)).astype(BF16)
        for p in range(2):
            self.one_copy(t, p).start()

    def stage_one(self, t):
        self.both(self.one, 1, t).wait_recv()
        for p in range(2):
            mine = self.sum[t, self.coarse(p, self.bit[p])].astype(F32)
            self.sums[t, p] = (mine + self.one[t, p].astype(F32)).astype(BF16)
        for p in range(2):
            self.two_copy(t, p).start()

    def stage_two(self, t):
        self.both(self.two, 2, t).wait_recv()
        for p in range(2):
            mine = self.sums[t, p, self.fine(self.other_bit[p])].astype(F32)
            total = (mine + self.two[t, p].astype(F32)).astype(BF16)
            start = self.bit[p] * (self.plane // 2) + self.other_bit[p] * (self.plane // 4)
            at = self.core * self.half + p * self.plane + start
            self.out[t, pl.ds(at, self.plane // 4)] = total
        for p in range(2):
            self.three_copy(t, p).start()

    def stage_three(self, t):
        self.both(self.two, 3, t).wait_recv()
        for p in range(2):
            self.four_copy(t, p).start()

    def stage_four(self, t):
        self.both(self.one, 4, t).wait_recv()
        self.fwd_copy(t, False).start()

    def store(self, t):
        return pltpu.make_async_copy(self.out.at[t], self.hbm.at[t], self.store_sem.at[0])

    def stages(self):
        return [
            self.stage_pair, self.stage_one, self.stage_two, self.stage_three,
            self.stage_four, self.stage_fwd,
        ]

    def drain(self):
        for k, buf in enumerate((self.pair, self.one, self.two, self.two, self.one, self.pair)):
            self.remote(
                buf, buf, self.send_sem.at[k], self.step_sem.at[k, 0], self.partner
            ).wait_send()
        pltpu.make_async_copy(self.out, self.hbm, self.store_sem.at[0]).wait()


class Halo:
    def __init__(self, n, lats, levels, level_windows, lat_windows, refs, sems):
        self.n, self.lats = n, lats
        self.levels, self.level_windows, self.lat_windows = levels, level_windows, lat_windows
        self.given, self.body, self.east, self.gl, self.gh, self.wh, self.nh, self.out = refs
        self.load_sem, self.east_sem, self.south_sem, self.wh_sem, self.nh_sem, self.out_sem = sems
        self.me, self.lat = lax.axis_index("lon"), lax.axis_index("lat")
        self.shift = WIN_LAT // 2
        self.height = lat_windows * WIN_LAT
        self.last = lat_windows - 1
        self.last_lat = self.lat == lats - 1
        self.strip = pl.ds(0, WIN_LON // 2)
        self.parts = ((1, WIN_Z), (1 + WIN_Z, levels - 1 - WIN_Z), (0, 1))

    def remote(self, src, dst, sems, at, lat, lon, send_at=None):
        device = {"lat": self.lat + lat, "lon": lax.rem(self.me + lon + self.n, self.n)}
        send = (0,) + (at if send_at is None else send_at)
        return pltpu.make_async_remote_copy(
            src_ref=src, dst_ref=dst, send_sem=sems.at[send], recv_sem=sems.at[(1,) + at],
            device_id=device, device_id_type=pl.DeviceIdType.MESH,
        )

    def count(self, bottom):
        return self.shift if bottom else WIN_LAT

    def load(self, i, b, bottom):
        rows = pl.ds(self.shift + b * WIN_LAT, self.count(bottom))
        return pltpu.make_async_copy(
            self.given[i].at[:, rows], self.body.at[i, :, rows], self.load_sem.at[i, b]
        )

    def east_copy(self, i, part, b, bottom):
        level = pl.ds(*self.parts[part])
        src = pl.ds(self.shift + b * WIN_LAT, self.count(bottom))
        dst = pl.ds(b * WIN_LAT, self.count(bottom))
        return self.remote(
            self.given[i].at[level, src, self.strip, :], self.east.at[i, level, dst, self.strip, :],
            self.east_sem, (i, b, part), 0, -1, (i, 0, 0),
        )

    def east_all(self, i):
        rows = pl.ds(self.shift, self.height - self.shift)
        src = self.given[i].at[:, rows, self.strip, :]
        dst = self.east.at[i, :, rows, self.strip, :]
        return self.remote(src, dst, self.east_sem, (i, 0, 0), 0, -1)

    def corner_copy(self, i):
        src, dst = pl.ds(0, self.shift), pl.ds(self.height - self.shift, self.shift)
        return self.remote(
            self.given[i].at[:, src, self.strip, :], self.east.at[i, :, dst, self.strip, :],
            self.east_sem, (i, self.lat_windows, 0), -1, -1,
        )

    def south_copy(self, i):
        src = self.given[i].at[:, pl.ds(0, self.shift)]
        dst = self.body.at[i, :, pl.ds(self.height, self.shift)]
        return self.remote(src, dst, self.south_sem, (i,), -1, 0)

    def begin(self):
        for b in range(self.lat_windows):
            for i in range(2):
                self.load(i, b, b == self.last).start()
        self.east[...] = jnp.zeros_like(self.east)
        self.wh[...] = jnp.zeros_like(self.wh)

        @pl.when(self.last_lat)
        def _():
            shape = self.body.shape
            blank = jnp.zeros(shape[:2] + (self.shift,) + shape[3:], BF16)
            self.body[:, :, pl.ds(self.height, self.shift)] = blank

        @pl.when(self.lat == 0)
        def _():
            self.nh[...] = jnp.zeros_like(self.nh)

    def send(self, b, bottom):
        for part in range(3):
            for i in range(2):
                self.east_copy(i, part, b, bottom).start()
        if bottom:
            @pl.when(self.lat > 0)
            def _():
                for i in range(2):
                    self.south_copy(i).start()
                    self.corner_copy(i).start()

    def send_next(self, b):
        pl.when(b + 1 < self.last)(lambda: self.send(b + 1, False))
        pl.when(b + 1 == self.last)(lambda: self.send(self.last, True))

    def pair(self, a):
        return [lax.rem(WIN_Z * a + 1 + u, self.levels) for u in range(WIN_Z)]

    def arrive_part(self, part, b, bottom):
        for i in range(2):
            if part == 0:
                self.load(i, b, bottom).wait()
            self.east_copy(i, part, b, bottom).wait_recv()
        if bottom and part == 0:
            @pl.when(jnp.logical_not(self.last_lat))
            def _():
                for i in range(2):
                    self.corner_copy(i).wait_recv()
                    self.south_copy(i).wait_recv()

    def arrive(self, a, b):
        at = (a == 0, a == 1, a == self.level_windows - 1)
        for part in range(3):
            pl.when(at[part] & (b < self.last))(
                functools.partial(self.arrive_part, part, b, False)
            )
            pl.when(at[part] & (b == self.last))(
                functools.partial(self.arrive_part, part, self.last, True)
            )

    def back_copy(self, b, bottom):
        src = pl.ds(b * WIN_LAT, self.count(bottom))
        dst = pl.ds(self.shift + b * WIN_LAT, self.count(bottom))
        return self.remote(
            self.gh.at[:, src, self.strip, :], self.wh.at[:, dst, self.strip, :],
            self.wh_sem, (b,), 0, 1,
        )

    def back_corner(self):
        src, dst = pl.ds(self.height - self.shift, self.shift), pl.ds(0, self.shift)
        return self.remote(
            self.gh.at[:, src, self.strip, :], self.wh.at[:, dst, self.strip, :],
            self.wh_sem, (self.lat_windows,), 1, 1,
        )

    def down_copy(self):
        src = self.gl.at[:, pl.ds(self.height, self.shift)]
        return self.remote(src, self.nh, self.nh_sem, (), 1, 0)

    def give_last(self):
        @pl.when(jnp.logical_not(self.last_lat))
        def _():
            self.back_corner().start()
            self.down_copy().start()

        self.back_copy(self.last, True).start()

    def store(self, b, bottom):
        rows = pl.ds(self.shift + b * WIN_LAT, self.count(bottom))
        return pltpu.make_async_copy(
            self.gl.at[:, rows], self.out.at[:, rows], self.out_sem.at[b]
        )

    def store_top(self):
        rows = pl.ds(0, self.shift)
        return pltpu.make_async_copy(
            self.nh, self.out.at[:, rows], self.out_sem.at[self.lat_windows]
        )

    def finish(self, b, bottom):
        self.back_copy(b, bottom).wait_recv()
        rows = pl.ds(self.shift + b * WIN_LAT, self.count(bottom))
        seam = self.gl[:, rows, :HALO].astype(F32) + self.wh[:, rows].astype(F32)
        self.gl[:, rows, :HALO] = seam.astype(BF16)
        self.store(b, bottom).start()

    def finish_top(self):
        @pl.when(self.lat > 0)
        def _():
            self.back_corner().wait_recv()
            self.down_copy().wait_recv()

        seam = self.nh[:, :, :HALO].astype(F32) + self.wh[:, : self.shift].astype(F32)
        self.nh[:, :, :HALO] = seam.astype(BF16)
        self.store_top().start()

    def end(self):
        for b in range(self.lat_windows):
            bottom = b == self.last
            self.back_copy(b, bottom).wait_send()
            self.store(b, bottom).wait()
        self.store_top().wait()
        for i in range(2):
            self.east_all(i).wait_send()

        @pl.when(self.lat > 0)
        def _():
            for i in range(2):
                self.south_copy(i).wait_send()
                self.corner_copy(i).wait_send()

        @pl.when(jnp.logical_not(self.last_lat))
        def _():
            self.back_corner().wait_send()
            self.down_copy().wait_send()


def enter(n, lats):
    me, lat = lax.axis_index("lon"), lax.axis_index("lat")
    barrier = pltpu.get_barrier_semaphore()
    for o in range(1, n):
        pl.semaphore_signal(
            barrier, inc=1, device_id={"lon": lax.rem(me + o, n)},
            device_id_type=pl.DeviceIdType.MESH,
        )
    for o in range(1, lats):
        pl.semaphore_signal(
            barrier, inc=1, device_id={"lat": lax.rem(lat + o, lats)},
            device_id_type=pl.DeviceIdType.MESH,
        )
    for o in (-1, 1):
        pl.semaphore_signal(
            barrier, inc=1,
            device_id={"lat": lax.rem(lat + o + lats, lats), "lon": lax.rem(me + o + n, n)},
            device_id_type=pl.DeviceIdType.MESH,
        )
    return lambda: pl.semaphore_wait(barrier, n + lats)


class WeightSum:
    def __init__(self, n, lats, wg, wp, wc, w1, w2, wout, sems):
        self.n, self.lats, self.chips = n, lats, n // 2
        self.wg, self.wp, self.wc = wg, wp, wc
        self.w1, self.w2, self.wout = w1, w2, wout
        self.sems = sems
        me, self.lat = lax.axis_index("lon"), lax.axis_index("lat")
        self.core, self.chip = lax.rem(me, 2), me // 2
        self.partner = me + 1 - 2 * self.core
        self.mine = pl.ds(self.core * self.chips, self.chips)
        self.theirs = pl.ds((1 - self.core) * self.chips, self.chips)

    def remote(self, src, dst, k, device):
        return pltpu.make_async_remote_copy(
            src_ref=src, dst_ref=dst, send_sem=self.sems.at[0, k], recv_sem=self.sems.at[1, k],
            device_id=device, device_id_type=pl.DeviceIdType.MESH,
        )

    def every(self, buf, count, k):
        part = buf.at[pl.ds(0, count)]
        return self.remote(part, part, k, {"lon": self.partner})

    def peers(self):
        return [lax.rem(self.chip + o, self.chips) for o in range(1, self.chips)]

    def start(self):
        self.remote(self.wg.at[self.theirs], self.wp, 0, {"lon": self.partner}).start()

    def step_zero(self):
        self.every(self.wp, self.chips, 0).wait_recv()
        total = self.wg[self.mine].astype(F32) + self.wp[...].astype(F32)
        self.wc[...] = total.astype(BF16)
        self.w1[pl.ds(self.chip, 1)] = self.wc[pl.ds(self.chip, 1)]
        for j in self.peers():
            device = {"lon": j * 2 + self.core}
            self.remote(self.wc.at[j], self.w1.at[self.chip], 1, device).start()

    def step_one(self):
        self.every(self.w1, self.chips - 1, 1).wait_recv()
        total = jnp.sum(self.w1[...].astype(F32), axis=0, keepdims=True)
        self.w2[pl.ds(self.lat, 1)] = total.astype(BF16)
        for o in range(1, self.lats):
            p = lax.rem(self.lat + o, self.lats)
            part = self.w2.at[self.lat]
            self.remote(part, part, 2, {"lat": p}).start()

    def step_two(self):
        self.every(self.w2, self.lats - 1, 2).wait_recv()
        total = jnp.sum(self.w2[...].astype(F32), axis=0, keepdims=True)
        at = self.core * self.chips + self.chip
        self.wout[pl.ds(at, 1)] = total.astype(BF16)
        for j in self.peers():
            part = self.wout.at[at]
            self.remote(part, part, 3, {"lon": j * 2 + self.core}).start()

    def step_three(self):
        self.every(self.w1, self.chips - 1, 3).wait_recv()
        part = self.wout.at[self.mine]
        self.remote(part, part, 4, {"lon": self.partner}).start()

    def finish(self):
        self.every(self.wp, self.chips, 4).wait_recv()
        self.every(self.wp, self.chips, 0).wait_send()
        self.every(self.w1, self.chips - 1, 1).wait_send()
        self.every(self.w2, self.lats - 1, 2).wait_send()
        self.every(self.w1, self.chips - 1, 3).wait_send()
        self.every(self.wp, self.chips, 4).wait_send()


class Pack:
    def __init__(self, table, rows, sems, bias, side, main, tail):
        self.table, self.rows, self.sems = table, rows, sems
        self.bias, self.side, self.main, self.tail = bias, side, main, tail
        self.kinds = bias.shape[0]

    def load(self, h):
        return pltpu.make_async_copy(self.table.at[h], self.rows.at[h], self.sems.at[h])

    def begin(self):
        for h in range(HEADS):
            self.load(h).start()

    def head(self, h, _):
        self.load(h).wait()
        group = LANES // TAIL
        kinds = self.kinds
        lane = lax.broadcasted_iota(jnp.int32, (kinds, LANES), 1)

        def body(m):
            tiles = []
            for r in range(group + 1):
                start = pl.multiple_of(m * (group * WTOK) + r * LANES, LANES)
                tiles.append(self.rows[h, :, pl.ds(start, LANES)].astype(F32))
            for r in range(group):
                turn = (LANES - TAIL * r) % LANES
                left = pltpu.roll(tiles[r], turn, 1) if r else tiles[r]
                right = pltpu.roll(tiles[r + 1], turn, 1) if r else tiles[r + 1]
                whole = jnp.where(lane < LANES - TAIL * r, left, right) if r else left
                at = pl.ds(m * group + r, kinds, stride=ODD)
                self.main[at, :] = whole
                self.tail[at, :] = right

        def several(i, _):
            for u in range(UNROLL):
                body(i * UNROLL + u)
            return 0

        lax.fori_loop(0, WTOK // group // UNROLL, several, 0)
        wide = lax.broadcasted_iota(jnp.int32, (WTOK, LANES), 1) // TAIL
        for t in range(kinds):
            at = slice(t * ODD, t * ODD + WTOK)
            self.bias[t, pl.ds(pl.multiple_of(h * WTOK, WTOK), WTOK)] = self.main[at, :].astype(BF16)
            turned = pltpu.roll(self.tail[at, :], h * TAIL, 1)
            before = jnp.where(h == 0, 0.0, self.side[t].astype(F32))
            self.side[t] = jnp.where(wide == h, turned, before).astype(BF16)
        return 0

    def heads(self, lo, hi):
        lax.fori_loop(lo, hi, self.head, 0)


def flip(mains, under, right, corner):
    lane = lax.broadcasted_iota(jnp.int32, (TAIL, LANES), 1) // TAIL
    spare = jnp.zeros((LANES - HEADS * TAIL, LANES), right.dtype)
    mains_t = [block.T for block in mains]
    right_t = jnp.concatenate(under + [spare], axis=0).T
    turned = right.T
    under_t = [turned[h * TAIL : (h + 1) * TAIL] for h in range(HEADS)]
    pad = jnp.zeros((LANES - TAIL, LANES), F32)
    turned = jnp.concatenate([corner, pad], axis=0).T
    corner_t = jnp.zeros((TAIL, LANES), F32)
    for h in range(HEADS):
        piece = turned[h * TAIL : (h + 1) * TAIL]
        if h:
            piece = pltpu.roll(piece, h * TAIL, 1)
        corner_t = jnp.where(lane == h, piece, corner_t)
    return mains_t, under_t, right_t, corner_t


def kernel(
    n,
    lats,
    kinds,
    lat_windows,
    level_windows,
    lon_windows,
    perm_ref,
    back_ref,
    x_hbm,
    c_hbm,
    wqkv_ref,
    wproj_ref,
    table_hbm,
    gqkv_ref,
    gproj_ref,
    gbias_hbm,
    grad_hbm,
    q_s,
    m_s,
    qt_s,
    mt_s,
    kt_s,
    vt_s,
    p_s,
    ds_s,
    shift_s,
    mix_s,
    dqt_s,
    gqkv_s,
    gproj_s,
    gbias_s,
    pair_s,
    sum_s,
    cross_s,
    step_s,
    half_s,
    red_s,
    wg_s,
    wp_s,
    wc_s,
    w1_s,
    w2_s,
    w3_s,
    body_s,
    east_s,
    gl_s,
    gh_s,
    wh_s,
    nh_s,
    rows_s,
    bias_s,
    side_s,
    flat_s,
    flat_tail_s,
    wqkv_s,
    wback_s,
    wproj_s,
    rows_sem,
    pair_sem,
    cross_sem,
    back_sem,
    fwd_sem,
    store_sem,
    w_sem,
    load_sem,
    east_sem,
    south_sem,
    wh_sem,
    nh_sem,
    out_sem,
):
    step = pl.program_id(0)
    a = lax.rem(step, level_windows)
    b = step // level_windows
    channels = wqkv_ref.shape[0]
    head_dim = channels // HEADS
    scale = head_dim ** -0.5
    levels = x_hbm.shape[0]
    shift = WIN_LAT // 2
    breadth = x_hbm.shape[2]
    tails = HEADS * LANES
    stack = HEADS * WTOK

    @pl.when(step == 0)
    def _():
        for ref in (gqkv_s, gproj_s, q_s, m_s, qt_s, mt_s):
            ref[...] = jnp.zeros_like(ref)
        gbias_s[:, stack + WTOK :, :] = jnp.zeros((kinds, PACKED - stack - WTOK, LANES), BF16)

    halo = Halo(
        n, lats, levels, level_windows, lat_windows,
        ((x_hbm, c_hbm), body_s, east_s, gl_s, gh_s, wh_s, nh_s, grad_hbm),
        (load_sem, east_sem, south_sem, wh_sem, nh_sem, out_sem),
    )

    @pl.when(step == 0)
    def _():
        table = Pack(table_hbm, rows_s, rows_sem, bias_s, side_s, flat_s, flat_tail_s)
        table.begin()
        halo.begin()
        entered = enter(n, lats)
        for i in range(3):
            part = wqkv_ref[:, i * channels : (i + 1) * channels]
            wqkv_s[i] = part
            wback_s[i] = part.T
        wproj_s[...] = wproj_ref[...].T
        table.heads(0, HEADS // 3)
        entered()
        halo.send(0, lat_windows == 1)
        table.heads(HEADS // 3, HEADS)

    halo.arrive(a, b)

    perm = perm_ref[...]
    bottom = b == lat_windows - 1

    def raw(which):
        flat = lambda t: t.reshape(-1, channels)
        zs = halo.pair(a)
        parts = [flat(body_s[which, z, pl.ds(shift + b * WIN_LAT, WIN_LAT)]) for z in zs]
        parts += [flat(east_s[which, z, pl.ds(b * WIN_LAT, WIN_LAT)]) for z in zs]
        return jnp.concatenate(parts, axis=0)

    x_raw, c_raw = raw(0), raw(1)
    x = mm(perm, x_raw).astype(BF16)
    c = mm(perm, c_raw).astype(BF16)
    q = (mm(x, wqkv_s[0]) * (scale * LOG2E)).astype(BF16)
    k = mm(x, wqkv_s[1]).astype(BF16)
    v = mm(x, wqkv_s[2]).astype(BF16)
    m = mm(c, wproj_s[...]).astype(BF16)

    wrap_here = a == level_windows - 1
    dead_here = bottom & (lax.axis_index("lat") == lats - 1)
    per_level = WTOK // WIN_Z

    def classes(token):
        upper = token >= per_level
        inner = jnp.where(upper, token - per_level, token)
        wrapped = jnp.where(upper & wrap_here, 2, 0)
        dead = jnp.where((inner >= per_level // 2) & dead_here, 1, 0)
        return wrapped + dead

    lane = lax.broadcasted_iota(jnp.int32, (1, LANES), 1)
    key_class = classes(lax.broadcasted_iota(jnp.int32, (WTOK, LANES), 0))
    mask_main = jnp.where(key_class == classes(lane), 0.0, -1e30)
    mask_tail = jnp.where(key_class == classes(LANES + lax.rem(lane, TAIL)), 0.0, -1e30)

    table = lambda lo, rows: bias_s[step, lo : lo + rows, :].astype(F32) * LOG2E
    mains_t, under_t, right_t, corner_t = flip(
        [table(h * WTOK, LANES) for h in range(HEADS)],
        [table(h * WTOK + LANES, TAIL) for h in range(HEADS)],
        side_s[step, :LANES, :].astype(F32) * LOG2E,
        side_s[step, LANES:, :].astype(F32) * LOG2E,
    )
    for h in range(HEADS):
        cols = slice(h * LANES, (h + 1) * LANES)
        shift_s[:LANES, cols] = mains_t[h] + mask_main[:LANES]
        shift_s[LANES:, cols] = under_t[h] + mask_main[LANES:]
    shift_s[:LANES, tails:] = right_t + mask_tail[:LANES]
    shift_s[LANES:, tails:] = corner_t + mask_tail[LANES:]

    whole = lon_windows * LANES
    main = lambda w: slice(w * LANES, (w + 1) * LANES)
    tail = lambda w: slice(whole + w * TAIL, whole + (w + 1) * TAIL)
    window = lambda t, w: jnp.concatenate([t[main(w)], t[tail(w)]], axis=0)
    keys = [window(k, w) for w in range(lon_windows)]
    values = [window(v, w) for w in range(lon_windows)]
    for w in range(lon_windows):
        for flat, wide_s, turned_s in ((q, q_s, qt_s), (m, m_s, mt_s)):
            turned = flat[main(w)].T
            for h in range(HEADS):
                cs = slice(h * head_dim, (h + 1) * head_dim)
                wide_s[w, h * LANES : (h + 1) * LANES, cs] = flat[main(w), cs]
                wide_s[w, tails + h * TAIL : tails + (h + 1) * TAIL, cs] = flat[tail(w), cs]
                turned_s[w, cs, h * LANES : (h + 1) * LANES] = turned[cs]
            turned_s[w, :, tails:] = wide_s[w, tails:, :].T
        kt_s[w] = keys[w].T
        vt_s[w] = values[w].T

    tiles = HEADS + 1
    gb = []
    for j in range(0, tiles, 2):
        cols = slice(j * LANES, min(j + 2, tiles) * LANES)
        total = [None, None]
        for w in range(lon_windows):
            s2 = mm(keys[w], qt_s[w, :, cols])
            dp2 = mm(values[w], mt_s[w, :, cols])
            for i in range(min(2, tiles - j)):
                here = slice(i * LANES, (i + 1) * LANES)
                at = slice((j + i) * LANES, (j + i + 1) * LANES)
                s = s2[:, here] + shift_s[:, at]
                dp = dp2[:, here]
                e = jnp.exp2(s - jnp.max(s, axis=0, keepdims=True))
                r = 1.0 / jnp.sum(e, axis=0, keepdims=True)
                p = e * r
                delta = jnp.sum(p * dp, axis=0, keepdims=True)
                ds = p * (dp - delta)
                p_s[w, :, at] = p.astype(BF16)
                ds_s[w, :, at] = ds.astype(BF16)
                total[i] = ds if total[i] is None else total[i] + ds
        gb += total[: min(2, tiles - j)]

    tail_lane = lax.broadcasted_iota(jnp.int32, (head_dim, LANES), 1) // TAIL
    for turned_s, from_s, to_s, factor in ((vt_s, p_s, mix_s, None), (kt_s, ds_s, dqt_s, scale)):
        far = [None] * HEADS
        for w in range(lon_windows):
            for j in range(0, HEADS, 2):
                rows = slice(j * head_dim, (j + 2) * head_dim)
                out = mm(turned_s[w, rows, :], from_s[w, :, j * LANES : (j + 2) * LANES])
                if factor is not None:
                    out = out * factor
                for i in range(2):
                    cs = slice((j + i) * head_dim, (j + i + 1) * head_dim)
                    piece = out[i * head_dim : (i + 1) * head_dim, i * LANES : (i + 1) * LANES]
                    to_s[cs, main(w)] = piece.astype(BF16)
            out = mm(turned_s[w], from_s[w, :, tails:])
            if factor is not None:
                out = out * factor
            for h in range(HEADS):
                piece = out[h * head_dim : (h + 1) * head_dim]
                turn = (w - h) * TAIL % LANES
                if turn:
                    piece = pltpu.roll(piece, turn, 1)
                far[h] = jnp.where(tail_lane == w, piece, 0.0 if far[h] is None else far[h])
        for h in range(HEADS):
            cs = slice(h * head_dim, (h + 1) * head_dim)
            to_s[cs, whole:] = far[h].astype(BF16)

    dk, dv = [], []
    for w in range(lon_windows):
        dk.append((mm(ds_s[w], q_s[w]) * (1.0 / LOG2E)).astype(BF16))
        dv.append(mm(p_s[w], m_s[w]).astype(BF16))
    order = lambda ts: jnp.concatenate([t[:LANES] for t in ts] + [t[LANES:] for t in ts], axis=0)
    tokens = lon_windows * WTOK
    dq = dqt_s[...].T[:tokens]
    cols = [dq, order(dk), order(dv)]
    xt = x.T
    for i in range(3):
        gqkv_s[i] += mm(xt, cols[i])
    gproj_s[...] += mm(mix_s[:, :tokens], c)
    gin = mm(cols[0], wback_s[0]) + mm(cols[1], wback_s[1]) + mm(cols[2], wback_s[2])
    gout = mm(back_ref[...], gin.astype(BF16)).astype(BF16)
    near, far = WIN_LAT * breadth, WIN_LAT * HALO
    for u, z in enumerate(halo.pair(a)):
        rows = pl.ds(shift + b * WIN_LAT, WIN_LAT)
        own = gout[u * near : (u + 1) * near]
        gl_s[z, rows] = own.reshape(WIN_LAT, breadth, channels)
        strip = gout[WIN_Z * near + u * far : WIN_Z * near + (u + 1) * far]
        gh_s[z, pl.ds(b * WIN_LAT, WIN_LAT)] = strip.reshape(WIN_LAT, HALO, channels)

    ws = WeightSum(n, lats, wg_s, wp_s, wc_s, w1_s, w2_s, w3_s, w_sem)
    share = channels // n

    @pl.when(step == kinds - 1)
    def _():
        for i in range(n):
            rows = slice(i * share, (i + 1) * share)
            for j in range(3):
                wg_s[i, j * share : (j + 1) * share, :] = gqkv_s[j, rows].astype(BF16)
            wg_s[i, 3 * share :, :] = gproj_s[rows].astype(BF16)
        ws.start()

    @pl.when((a == level_windows - 1) & (b < lat_windows - 1))
    def _():
        halo.back_copy(b, False).start()

    @pl.when(a == 0)
    def _():
        halo.send_next(b)

    @pl.when((a == GRAD_LAG - 1) & (b > 0))
    def _():
        halo.finish(b - 1, False)

    mains_t, under_t, right_t, corner_t = flip(
        [gb[h][:LANES].astype(BF16) for h in range(HEADS)],
        [gb[h][LANES:].astype(BF16) for h in range(HEADS)],
        gb[HEADS][:LANES].astype(BF16),
        gb[HEADS][LANES:],
    )
    for h in range(HEADS):
        gbias_s[step, h * WTOK : h * WTOK + LANES, :] = mains_t[h].astype(BF16)
        gbias_s[step, h * WTOK + LANES : (h + 1) * WTOK, :] = under_t[h].astype(BF16)
    gbias_s[step, stack : stack + LANES, :] = right_t.astype(BF16)
    gbias_s[step, stack + LANES : stack + WTOK, :] = corner_t.astype(BF16)

    ex = (Square if n == 8 else Exchange)(
        n, kinds,
        (gbias_s, pair_s, sum_s, (cross_s, step_s, half_s) if n == 8 else cross_s, red_s, gbias_hbm),
        (pair_sem, cross_sem, back_sem, fwd_sem, store_sem),
    )
    ex.behind(step)
    ex.pair_copy(step).start()

    @pl.when(step == kinds - 1)
    def _():
        halo.give_last()
        ws.step_zero()
        for turn, _ in enumerate(ex.rest()):
            if turn == 0:
                ws.step_one()
            if turn == 2:
                ws.step_two()
                halo.finish(lat_windows - 1, True)
                halo.finish_top()
            if turn == 3:
                ws.step_three()
        ws.finish()
        for p in range(n):
            rows = slice(p * share, (p + 1) * share)
            for j in range(3):
                cs = slice(j * channels, (j + 1) * channels)
                gqkv_ref[rows, cs] = w3_s[p, j * share : (j + 1) * share, :].astype(F32)
            gproj_ref[rows, :] = w3_s[p, 3 * share :, :].astype(F32)
        ex.drain()
        halo.end()


def unpack_kernel(main_ref, tail_ref, out_ref, main_s, tail_s):
    h = pl.program_id(0)
    kinds = main_ref.shape[0]
    for t in range(kinds):
        at = slice(t * ODD, t * ODD + WTOK)
        main_s[at, :] = main_ref[t].astype(F32)

    @pl.when(h == 0)
    def _():
        for t in range(kinds):
            tail_s[t * ODD : t * ODD + WTOK, :] = tail_ref[t].astype(F32)

    group = LANES // TAIL
    lane = lax.broadcasted_iota(jnp.int32, (kinds, LANES), 1)

    def body(m):
        before_main = before_tail = None
        for r in range(group + 1):
            tile = None
            if r < group:
                at = pl.ds(m * group + r, kinds, stride=ODD)
                here_main, here_tail = main_s[at, :], tail_s[at, :]
                if r:
                    here_main = pltpu.roll(here_main, TAIL * r, 1)
                here_tail = pltpu.roll(here_tail, lax.rem(LANES + TAIL * (r - h), LANES), 1)
                tile = here_main
            if r:
                ended = before_tail
                if r > 1:
                    ended = jnp.where(lane < TAIL * (r - 1), before_main, before_tail)
                tile = ended if r == group else jnp.where(lane < TAIL * r, ended, tile)
            start = pl.multiple_of(m * (group * WTOK) + r * LANES, LANES)
            out_ref[0, :, pl.ds(start, LANES)] = tile
            if r < group:
                before_main, before_tail = here_main, here_tail

    def several(i, _):
        for u in range(UNROLL):
            body(i * UNROLL + u)
        return 0

    lax.fori_loop(0, WTOK // group // UNROLL, several, 0)


def unpack(packed):
    kinds, _, lanes = packed.shape
    return pl.pallas_call(
        unpack_kernel,
        grid=(HEADS,),
        in_specs=[
            pl.BlockSpec((kinds, WTOK, lanes), lambda i: (0, i, 0)),
            pl.BlockSpec((kinds, WTOK, lanes), lambda i: (0, HEADS, 0)),
        ],
        out_specs=pl.BlockSpec((1, kinds, WTOK * WTOK), lambda i: (i, 0, 0)),
        out_shape=jax.ShapeDtypeStruct((HEADS, kinds, WTOK * WTOK), F32),
        scratch_shapes=[pltpu.VMEM((kinds * ODD, LANES), F32)] * 2,
        cost_estimate=pl.CostEstimate(
            flops=10_000_000_000, bytes_accessed=15_000_000, transcendentals=0
        ),
    )(packed, packed)


def window_call(perm, back, normed, cotangent, wqkv, wproj, table):
    levels, height, breadth, channels = normed.shape
    level_windows = levels // WIN_Z
    lat_windows = height // WIN_LAT
    lon_windows = perm.shape[0] // WTOK
    kinds = lat_windows * level_windows
    n, lats = lax.axis_size("lon"), lax.axis_size("lat")
    chips = n // 2
    shift = WIN_LAT // 2
    whole = lambda arr: pl.BlockSpec(arr.shape, lambda i: (0,) * arr.ndim)
    const = lambda shape: pl.BlockSpec(shape, lambda i: (0,) * len(shape))
    anywhere = pl.BlockSpec(memory_space=pl.ANY)
    stack = HEADS * WTOK
    padded = (HEADS + 1) * LANES
    turned = (lon_windows + 1) * LANES
    wgrad = (4 * channels // n, channels)
    sem = lambda *k: pltpu.SemaphoreType.DMA((2,) + k)
    dma = pltpu.SemaphoreType.DMA
    if n == 8:
        exchange_sems = [dma((6,)), dma((6, kinds)), dma((1,)), dma((1,)), dma((1,))]
    else:
        exchange_sems = [
            sem(kinds), sem(kinds, chips), sem(kinds, chips), sem(kinds), dma((kinds,))
        ]
    arriving = (2, PACKED // 8, LANES) if n == 8 else (chips, PACKED // n, LANES)
    return pl.pallas_call(
        functools.partial(kernel, n, lats, kinds, lat_windows, level_windows, lon_windows),
        grid=(kinds,),
        in_specs=[
            whole(perm),
            whole(back),
            anywhere,
            anywhere,
            whole(wqkv),
            whole(wproj),
            anywhere,
        ],
        out_specs=[
            const((channels, 3 * channels)),
            const((channels, channels)),
            anywhere,
            anywhere,
        ],
        out_shape=[
            jax.ShapeDtypeStruct((channels, 3 * channels), F32),
            jax.ShapeDtypeStruct((channels, channels), F32),
            jax.ShapeDtypeStruct((kinds, PACKED, LANES), BF16),
            jax.ShapeDtypeStruct(normed.shape, BF16),
        ],
        scratch_shapes=[
            pltpu.VMEM((lon_windows, padded, channels), BF16),
            pltpu.VMEM((lon_windows, padded, channels), BF16),
            pltpu.VMEM((lon_windows, channels, padded), BF16),
            pltpu.VMEM((lon_windows, channels, padded), BF16),
            pltpu.VMEM((lon_windows, channels, WTOK), BF16),
            pltpu.VMEM((lon_windows, channels, WTOK), BF16),
            pltpu.VMEM((lon_windows, WTOK, padded), BF16),
            pltpu.VMEM((lon_windows, WTOK, padded), BF16),
            pltpu.VMEM((WTOK, padded), F32),
            pltpu.VMEM((channels, turned), BF16),
            pltpu.VMEM((channels, turned), BF16),
            pltpu.VMEM((3, channels, channels), F32),
            pltpu.VMEM((channels, channels), F32),
            pltpu.VMEM((kinds, PACKED, LANES), BF16),
            pltpu.VMEM((kinds, PACKED // 2, LANES), BF16),
            pltpu.VMEM((kinds, PACKED // 2, LANES), BF16),
            pltpu.VMEM((kinds,) + arriving, BF16),
            pltpu.VMEM((kinds, 2, PACKED // 8, LANES), BF16),
            pltpu.VMEM((kinds, 2, PACKED // 16, LANES), BF16),
            pltpu.VMEM((kinds, PACKED, LANES), BF16),
            pltpu.VMEM((n,) + wgrad, BF16),
            pltpu.VMEM((chips,) + wgrad, BF16),
            pltpu.VMEM((chips,) + wgrad, BF16),
            pltpu.VMEM((chips,) + wgrad, BF16),
            pltpu.VMEM((lats,) + wgrad, BF16),
            pltpu.VMEM((n,) + wgrad, BF16),
            pltpu.VMEM((2, levels, height + shift, breadth, channels), BF16),
            pltpu.VMEM((2, levels, height, HALO, channels), BF16),
            pltpu.VMEM((levels, height + shift, breadth, channels), BF16),
            pltpu.VMEM((levels, height, HALO, channels), BF16),
            pltpu.VMEM((levels, height, HALO, channels), BF16),
            pltpu.VMEM((levels, shift, breadth, channels), BF16),
            pltpu.VMEM(table.shape, BF16),
            pltpu.VMEM((kinds, stack, LANES), BF16),
            pltpu.VMEM((kinds, WTOK, LANES), BF16),
            pltpu.VMEM((kinds * ODD, LANES), F32),
            pltpu.VMEM((kinds * ODD, LANES), F32),
            pltpu.VMEM((3, channels, channels), BF16),
            pltpu.VMEM((3, channels, channels), BF16),
            pltpu.VMEM((channels, channels), BF16),
            dma((HEADS,)),
            *exchange_sems,
            sem(5),
            pltpu.SemaphoreType.DMA((2, lat_windows)),
            sem(2, lat_windows + 1, 3),
            sem(2),
            sem(lat_windows + 1),
            sem(),
            pltpu.SemaphoreType.DMA((lat_windows + 1,)),
        ],
        compiler_params=pltpu.CompilerParams(
            dimension_semantics=("arbitrary",),
            vmem_limit_bytes=62 * 2**20,
            collective_id=0,
            has_side_effects=True,
        ),
        cost_estimate=pl.CostEstimate(
            flops=kinds * 1_500_000_000, bytes_accessed=kinds * 2_000_000, transcendentals=0
        ),
    )(
        perm, back, normed, cotangent, wqkv, wproj, table
    )


def frame_order(breadth, lon_windows):
    rows = np.arange(lon_windows * WTOK)
    mains = lon_windows * LANES
    is_main = rows < mains
    window = np.where(is_main, rows // LANES, (rows - mains) // TAIL)
    token = np.where(is_main, rows % LANES, LANES + (rows - mains) % TAIL)
    per_level = WIN_LAT * WIN_LON
    level = token // per_level
    row = token % per_level // WIN_LON
    place = window * WIN_LON + token % WIN_LON + WIN_LON // 2
    near, far = WIN_LAT * breadth, WIN_LAT * HALO
    source = np.where(
        place < breadth,
        level * near + row * breadth + place,
        WIN_Z * near + level * far + row * HALO + place - breadth,
    )
    columns = np.arange(WIN_Z * (near + far))
    return (source[:, None] == columns[None, :]).astype(np.float32)


def local(normed, cotangent, weight_qkv, weight_proj, bias_table):
    breadth = normed.shape[2]
    lon_windows = breadth // WIN_LON
    perm = frame_order(breadth, lon_windows)
    gqkv, gproj, packed, input_grad = window_call(
        jnp.asarray(perm, BF16), jnp.asarray(perm.T, BF16),
        normed, cotangent, weight_qkv, weight_proj, jnp.swapaxes(bias_table, 0, 1),
    )
    bias_grad = jnp.swapaxes(unpack(packed), 0, 1)
    return input_grad, gqkv, gproj, bias_grad


def solution(mesh):
    in_specs = (
        P(None, "lat", "lon", None),
        P(None, "lat", "lon", None),
        P(),
        P(),
        P("lat", None, None),
    )
    out_specs = (P(None, "lat", "lon", None), P(), P(), P("lat", None, None))
    return jax.shard_map(local, mesh=mesh, in_specs=in_specs, out_specs=out_specs, check_vma=False)
```
